128 devices in a mesh: gx: 8 (over y, core), gy: 16 (over z, x).
Axes of the slice: x: 4, y: 4, z: 4, core: 2. Of those that a mesh axis runs over, the one named last changes fastest.
Arguments:
- forcing: float32 [16, 512, 2048], P(None, 'gy', 'gx'), may hold values from -6 to 6
- damping: float32 [16, 512, 2048], P(None, 'gy', 'gx'), may hold values from 0.5 to 4
- coupling: float32 [16, 16], replicated, may hold values from -1.5 to 1.5
- wind_lon: float32 [512, 2048], P('gy', 'gx'), may hold values from -0.5 to 0.5
- wind_lat: float32 [512, 2048], P('gy', 'gx'), may hold values from -0.5 to 0.5
Outputs:
- solution: float32 [16, 512, 2048], P(None, 'gy', 'gx')
- residual: float32 [16, 512, 2048], P(None, 'gy', 'gx')
The draws below stay inside these ranges and needn't reach their ends.
All inputs are finite; a program needn't handle non-finite values.
Results may differ from the reference program's by a relative error of at most 0.0003.
Values sent between devices are 32-bit elements; how exact they have to be, the bound alone decides.
A program may use at most 64 MiB of HBM per device.

```python
import math
import jax
import jax.numpy as jnp
from jax import lax

CH = 16
ITERS = 8
NLAT = 512
NLON = 2048


def block_scale(stream_key, dims, cuts, smallest, high):
    def one(position, parts):
        steps = jax.random.uniform(jax.random.fold_in(jax.random.fold_in(stream_key, 6), position), (parts,), jnp.float32, smallest / len(cuts), high / len(cuts))
        return jnp.repeat(jnp.exp(steps), dims[position] // parts).reshape((-1,) + (1,) * (len(dims) - position - 1))

    factor_of = one(*cuts[0])
    for cut in cuts[1:]:
        factor_of = factor_of * one(*cut)
    return factor_of


def scatter_about(own_key, extent, scale, limit, pieces=(), held_as=jnp.bfloat16):
    factor_of = block_scale(own_key, extent, pieces, -0.22, 0.18) if pieces else 1.0
    drawn = jax.random.normal(own_key, extent, jnp.float32) * scale * factor_of
    return jnp.minimum(jnp.maximum(drawn, -limit), limit).astype(held_as)


def setup_inputs(seed: int = 0) -> dict:
    seeds = jax.random.split(jax.random.key(seed), 6)
    return {
        "forcing": scatter_about(seeds[0], (CH, NLAT, NLON), 1.0, 6.0, ((1, 16), (2, 8)), jnp.float32),
        "damping": jnp.clip(jnp.exp(math.log(4.0) - 2.0794415 * jax.random.uniform(seeds[1], (CH, NLAT, NLON), jnp.float32) ** block_scale(seeds[1], (CH, NLAT, NLON), ((1, 16), (2, 8)), -0.2, 0.2)), 0.5, 4.0),
        "coupling": scatter_about(seeds[2], (CH, CH), CH ** -0.5, 1.5, (), jnp.float32),
        "wind_lon": jnp.clip(jax.random.uniform(seeds[3], (NLAT, NLON), jnp.float32, -0.5, 0.5) * block_scale(seeds[3], (NLAT, NLON), ((0, 16), (1, 8)), -0.4, 0.0), -0.5, 0.5),
        "wind_lat": jnp.clip(jax.random.uniform(seeds[4], (NLAT, NLON), jnp.float32, -0.5, 0.5) * block_scale(seeds[4], (NLAT, NLON), ((0, 16), (1, 8)), -0.4, 0.0), -0.5, 0.5),
    }


COUPLE = 0.25
DIFF_LAT = 0.5
DIFF_LON = 0.5
GUARD = 1.0

def apply_core(padded, damping, coupling, wind_lon, wind_lat, diffuse_lon):
    centre = padded[:, 2:-2, 2:-2]
    east_one = padded[:, 2:-2, 3:-1]
    west_one = padded[:, 2:-2, 1:-3]
    east_two = padded[:, 2:-2, 4:]
    west_two = padded[:, 2:-2, :-4]
    north_one = padded[:, 3:-1, 2:-2]
    south_one = padded[:, 1:-3, 2:-2]
    north_two = padded[:, 4:, 2:-2]
    south_two = padded[:, :-4, 2:-2]
    slope_lon = (8.0 * (east_one - west_one) - (east_two - west_two)) / 12.0
    slope_lat = (8.0 * (north_one - south_one) - (north_two - south_two)) / 12.0
    coupled = COUPLE * jnp.einsum('ij,jab->iab', coupling, centre, precision=lax.Precision.HIGHEST)
    return (1.0 + damping) * centre + coupled + diffuse_lon * (2.0 * centre - east_one - west_one) + DIFF_LAT * (2.0 * centre - north_one - south_one) + wind_lon * slope_lon + wind_lat * slope_lat

def lon_diffusion(row_pos, lat_total):
    phi = -math.pi / 2 + (row_pos + 0.5) * (math.pi / lat_total)
    return DIFF_LON / (jnp.cos(phi) ** 2 + 0.1)

def operate(source, damping, coupling, wind_lon, wind_lat):
    padded = jnp.pad(source, ((0, 0), (2, 2), (0, 0)))
    padded = jnp.concatenate([padded[:, :, -2:], padded, padded[:, :, :2]], axis=2)
    row_pos = jnp.arange(NLAT).astype(jnp.float32)
    diffuse = lon_diffusion(row_pos, NLAT)[:, None]
    return apply_core(padded, damping, coupling, wind_lon, wind_lat, diffuse)

def least_squares(heights, first):
    num_steps = heights.shape[1]
    target = jnp.zeros((num_steps + 1,), jnp.float32).at[0].set(first)
    rotated = heights
    cosines = []
    sines = []
    for column in range(num_steps):
        column_vec = rotated[:, column]
        for earlier in range(column):
            upper_val = column_vec[earlier]
            lower_val = column_vec[earlier + 1]
            column_vec = column_vec.at[earlier].set(cosines[earlier] * upper_val + sines[earlier] * lower_val)
            column_vec = column_vec.at[earlier + 1].set(-sines[earlier] * upper_val + cosines[earlier] * lower_val)
        upper_val = column_vec[column]
        lower_val = column_vec[column + 1]
        radius = jnp.sqrt(upper_val * upper_val + lower_val * lower_val)
        cosine = upper_val / radius
        sine_val = lower_val / radius
        column_vec = column_vec.at[column].set(radius).at[column + 1].set(0.0)
        rotated = rotated.at[:, column].set(column_vec)
        upper_val = target[column]
        lower_val = target[column + 1]
        target = target.at[column].set(cosine * upper_val + sine_val * lower_val)
        target = target.at[column + 1].set(-sine_val * upper_val + cosine * lower_val)
        cosines.append(cosine)
        sines.append(sine_val)
    weights = [None] * num_steps
    for column in reversed(range(num_steps)):
        partial_value = target[column]
        for later_col in range(column + 1, num_steps):
            partial_value = partial_value - rotated[column, later_col] * weights[later_col]
        weights[column] = partial_value / rotated[column, column]
    return weights

def reference(forcing, damping, coupling, wind_lon, wind_lat):
    scale_first = jnp.sqrt(jnp.sum(forcing * forcing) + GUARD)
    krylov = [forcing / scale_first]
    heights = jnp.zeros((ITERS + 1, ITERS), jnp.float32)
    for column in range(ITERS):
        applied = operate(krylov[column], damping, coupling, wind_lon, wind_lat)
        coeffs = jnp.stack([jnp.sum(vector * applied) for vector in krylov])
        for earlier in range(len(krylov)):
            applied = applied - coeffs[earlier] * krylov[earlier]
        subdiag = jnp.sqrt(jnp.sum(applied * applied) + GUARD)
        heights = heights.at[:column + 1, column].set(coeffs).at[column + 1, column].set(subdiag)
        if column + 1 < ITERS:
            krylov.append(applied / subdiag)
    weights = least_squares(heights, scale_first)
    solution = weights[0] * krylov[0]
    for column in range(1, ITERS):
        solution = solution + weights[column] * krylov[column]
    residual = forcing - operate(solution, damping, coupling, wind_lon, wind_lat)
    return (solution, residual)
```

```python
import functools
import math

import jax
import jax.numpy as jnp
import numpy as np
from jax import lax
from jax.experimental import pallas as pl
from jax.experimental.pallas import tpu as pltpu
from jax.sharding import PartitionSpec as P

ITERS = 8
CH = 16
RIM = 8
LOW, HIGH = 1.0, 16.0
MID, HALF = (LOW + HIGH) / 2, (HIGH - LOW) / 2
BLOCK = 4
NOISE = 1.2e-7
TRUST = 1.0e-4
MESH = pl.DeviceIdType.MESH
F32 = jnp.float32


def trial_table():
    rng = np.random.default_rng(7)
    draw = rng.choice([-1.0, 1.0], size=(9, 16, 128)) * NOISE
    table = np.zeros((9, 16, 128), np.float32)
    for i in range(9):
        for k in range(i, 9):
            table[i, k] = draw[i, k]
            table[k, i] = draw[i, k]
    table[:, :, 0] = 0.0
    return table


def kx_table(lat_total):
    row = np.arange(lat_total) + 0.5
    phi = -math.pi / 2 + row * (math.pi / lat_total)
    table = np.zeros((lat_total + 2 * RIM, 128), np.float32)
    table[RIM : RIM + lat_total] = (0.5 / (np.cos(phi) ** 2 + 0.1))[:, None]
    return table


def lanes(shape):
    return lax.broadcasted_iota(jnp.int32, shape, len(shape) - 1)


def apply_a(vec):
    sub = lax.broadcasted_iota(jnp.int32, vec.shape, 0)
    up = pltpu.roll(vec, 1, 0)
    kept = jnp.where((sub == 0) | (sub == BLOCK), 0.0, vec)
    down = pltpu.roll(kept, 15, 0)
    return MID * vec + (HALF / 2) * (up + down)


def mat_vec(cols, vec, count):
    total = cols[0] * vec[0:1, :]
    for k in range(1, count):
        total = total + cols[k] * vec[k : k + 1, :]
    return total


def dot(a, b):
    return jnp.sum(a * b, axis=0, keepdims=True)


def gmres(cols):
    sub = lax.broadcasted_iota(jnp.int32, (16, 128), 0)
    first = jnp.sqrt(cols[0][0:1, :] + 1.0)
    basis = [jnp.where(sub == 0, 1.0, 0.0) / first]
    target = first
    targets = []
    columns = []
    turns = []
    for j in range(ITERS):
        w = apply_a(basis[j])
        u = mat_vec(cols, w, j + 2)
        h = [dot(v, u) for v in basis]
        for i in range(j + 1):
            w = w - h[i] * basis[i]
        norm = dot(w, mat_vec(cols, w, j + 2))
        below = jnp.sqrt(jnp.maximum(norm, 0.0) + 1.0)
        if j + 1 < ITERS:
            basis.append(w / below)
        col = list(h)
        for i, (c, s) in enumerate(turns):
            if i + 1 <= j:
                col[i], col[i + 1] = c * col[i] + s * col[i + 1], c * col[i + 1] - s * col[i]
        radius = jnp.sqrt(col[j] * col[j] + below * below)
        inv = 1.0 / radius
        c, s = col[j] * inv, below * inv
        turns.append((c, s))
        col[j] = radius
        columns.append((col, inv))
        targets.append(c * target)
        target = -s * target
    y = [None] * ITERS
    for j in reversed(range(ITERS)):
        y[j] = targets[j] * columns[j][1]
        for i in range(j):
            targets[i] = targets[i] - columns[j][0][i] * y[j]
    q = basis[0] * y[0]
    for j in range(1, ITERS):
        q = q + basis[j] * y[j]
    return q


def kernel(
    nx, ny, stk, coup, trial, kxs, sol, res, flag,
    ext, pwr, coef, lon, pack, kxv, gx_slots, gy_slots,
    in_sem, kx_sem, lon_send, lon_recv, lat_send, lat_recv, cor_send, cor_recv,
    mid_send, mid_recv, gxs_send, gxs_recv, gys_send, gys_recv,
):
    gx, gy = lax.axis_index("gx"), lax.axis_index("gy")
    rows = stk.shape[0]
    top = RIM + rows
    total = rows + 2 * RIM
    east, west = lax.rem(gx + 1, nx), lax.rem(gx + nx - 1, nx)
    north, south = gy + 1, gy - 1
    has_n, has_s = gy < ny - 1, gy > 0

    own = pltpu.make_async_copy(stk, ext.at[pl.ds(RIM, rows), :, pl.ds(0, 256)], in_sem)
    own.start()
    start = pl.multiple_of(gy * rows, 8)
    kcopy = pltpu.make_async_copy(kxs.at[pl.ds(start, total), :], kxv, kx_sem)
    kcopy.start()

    barrier = pltpu.get_barrier_semaphore()
    for k in range(1, nx):
        pl.semaphore_signal(barrier, 1, device_id=(lax.rem(gx + k, nx), gy), device_id_type=MESH)
    for k in range(1, ny):
        pl.semaphore_signal(barrier, 1, device_id=(gx, lax.rem(gy + k, ny)), device_id_type=MESH)
    own.wait()
    lane = lanes((rows // 8, 40, 128))
    to_west = jnp.zeros((rows // 8, 40, 128), F32)
    to_east = jnp.zeros((rows // 8, 40, 128), F32)
    for j in range(8):
        here = (lane >= 16 * j) & (lane < 16 * j + 16)
        left = jnp.stack([ext[RIM + 8 * g + j, :, 0:128] for g in range(rows // 8)])
        right = jnp.stack([ext[RIM + 8 * g + j, :, 128:256] for g in range(rows // 8)])
        if j:
            left = pltpu.roll(left, 16 * j, 2)
        to_west = jnp.where(here, left, to_west)
        if j < 7:
            right = pltpu.roll(right, 16 * j + 16, 2)
        to_east = jnp.where(here, right, to_east)
    pack[0] = to_west
    pack[1] = to_east
    pl.semaphore_wait(barrier, nx + ny - 2)

    groups = rows // 8
    go_west = pltpu.make_async_remote_copy(
        pack.at[0], lon.at[0, pl.ds(1, groups)], lon_send.at[0], lon_recv.at[0],
        device_id=(west, gy), device_id_type=MESH)
    go_east = pltpu.make_async_remote_copy(
        pack.at[1], lon.at[1, pl.ds(1, groups)], lon_send.at[1], lon_recv.at[1],
        device_id=(east, gy), device_id_type=MESH)
    go_west.start()
    go_east.start()

    def strip(src, dst, size, chan, sem, peer):
        return pltpu.make_async_remote_copy(
            ext.at[pl.ds(src, size), chan, pl.ds(0, 256)],
            ext.at[pl.ds(dst, size), chan, pl.ds(0, 256)],
            lat_send.at[sem], lat_recv.at[sem], device_id=(gx, peer), device_id_type=MESH)

    vec, par = pl.ds(0, CH), pl.ds(CH, 24)
    to_s = [strip(RIM, top, RIM, vec, 0, south), strip(RIM, top, RIM - 2, par, 1, south)]
    to_n = [strip(rows, 0, RIM, vec, 2, north), strip(rows + 2, 2, RIM - 2, par, 3, north)]

    @pl.when(has_s)
    def _():
        for copy in to_s:
            copy.start()

    @pl.when(has_n)
    def _():
        for copy in to_n:
            copy.start()

    @pl.when(jnp.logical_not(has_s))
    def _():
        ext[0:RIM, :, 0:256] = jnp.zeros((RIM, 40, 256), F32)
        lon[:, 0] = jnp.zeros((2, 40, 128), F32)

    @pl.when(jnp.logical_not(has_n))
    def _():
        ext[top : top + RIM, :, 0:256] = jnp.zeros((RIM, 40, 256), F32)
        lon[:, groups + 1] = jnp.zeros((2, 40, 128), F32)

    go_west.wait_recv()
    go_east.wait_recv()
    cor_s = pltpu.make_async_remote_copy(
        lon.at[:, 1], lon.at[:, groups + 1], cor_send.at[0], cor_recv.at[0],
        device_id=(gx, south), device_id_type=MESH)
    cor_n = pltpu.make_async_remote_copy(
        lon.at[:, groups], lon.at[:, 0], cor_send.at[1], cor_recv.at[1],
        device_id=(gx, north), device_id_type=MESH)

    @pl.when(has_s)
    def _():
        cor_s.start()

    @pl.when(has_n)
    def _():
        cor_n.start()

    kcopy.wait()

    def unpack(g):
        from_e, from_w = lon[0, g], lon[1, g]
        lane2 = lanes((40, 128))
        for j in range(8):
            a = pltpu.roll(from_e, (128 - 16 * j) % 128, 1) if j else from_e
            b = pltpu.roll(from_w, 112 - 16 * j, 1) if j < 7 else from_w
            ext[g * 8 + j, :, 256:384] = jnp.where(
                lane2 < 16, a, jnp.where(lane2 >= 112, b, 0.0))

    @pl.loop(1, groups + 1)
    def _(g):
        unpack(g)

    @pl.when(has_s)
    def _():
        to_s[0].wait_send()
        to_s[1].wait_send()
        cor_s.wait_send()
        for copy in to_n:
            copy.wait_recv()
        cor_n.wait_recv()

    @pl.when(has_n)
    def _():
        to_n[0].wait_send()
        to_n[1].wait_send()
        cor_n.wait_send()
        for copy in to_s:
            copy.wait_recv()
        cor_s.wait_recv()

    unpack(0)
    unpack(groups + 1)

    two = 2.0 / HALF
    kind = lax.broadcasted_iota(jnp.int32, (8, 384), 0)
    by_kx = jnp.where(kind < 2, -two, 0.0)
    by_one = jnp.where((kind == 3) | (kind == 4), -0.5 * two, 0.0)
    eight = two * 8.0 / 12.0
    by_lon = jnp.where(kind == 0, eight, 0.0) + jnp.where(kind == 1, -eight, 0.0)
    by_lon = by_lon + jnp.where(kind == 2, -two / 12.0, 0.0)
    by_lat = jnp.where(kind == 3, eight, 0.0) + jnp.where(kind == 4, -eight, 0.0)
    by_lat = by_lat + jnp.where(kind == 5, -two / 12.0, 0.0)

    @pl.loop(2, total - 2)
    def _(r):
        kx = jnp.concatenate([kxv[pl.ds(r, 1), :]] * 3, axis=1)
        inside = jnp.where(kx > 0.0, 1.0, 0.0)
        wind = ext[r, 32:40, :]
        coef[r] = (kx * by_kx + inside * by_one + by_lon * wind[0:1, :] + by_lat * wind[1:2, :])
        diag = ext[r, CH : 2 * CH, :]
        ext[r, CH : 2 * CH, :] = (two * inside) * (diag + (2.0 - MID)) + (2.0 * two) * kx

    cm = coup[...] * (0.25 * two)
    cm = jnp.concatenate([jnp.concatenate([cm] * 4, axis=1)] * 4, axis=0)
    r4 = lax.broadcasted_iota(jnp.int32, (64, 64), 0) // 16
    c4 = lax.broadcasted_iota(jnp.int32, (64, 64), 1) // 16
    cm = jnp.where(r4 == c4, cm, 0.0)
    cm_hi = cm.astype(jnp.bfloat16)
    cm_lo = (cm - cm_hi.astype(F32)).astype(jnp.bfloat16)
    weights = jnp.concatenate([cm_hi, cm_hi, cm_lo], axis=1)

    def power(k):
        return ext.at[:, pl.ds(0, CH), :] if k == 0 else pwr.at[k - 1]

    lane4 = lanes((4, CH, 128))

    def advance(k):
        src, dst = power(k), power(k + 1)
        depth = k % BLOCK
        low = 2 * (depth + 1)
        count = (total - 2 * low) // 4
        prev = power(k - 1) if depth else None

        def body(g, carry):
            r0 = low + 4 * g
            mids = [src[pl.ds(r0, 4), :, 128 * t : 128 * t + 128] for t in range(3)]
            flat = jnp.concatenate([m.reshape(64, 128) for m in mids], axis=1)
            hi = flat.astype(jnp.bfloat16)
            lo = (flat - hi.astype(F32)).astype(jnp.bfloat16)
            mixed = jnp.dot(weights, jnp.concatenate([hi, lo, hi], axis=0),
                            preferred_element_type=F32)
            for t in range(3):
                cut = pl.ds(128 * t, 128)
                mid, nxt, prv = mids[t], mids[(t + 1) % 3], mids[(t + 2) % 3]
                e1 = pltpu.roll(jnp.where(lane4 < 1, nxt, mid), 127, 2)
                e2 = pltpu.roll(jnp.where(lane4 < 2, nxt, mid), 126, 2)
                w1 = pltpu.roll(jnp.where(lane4 >= 127, prv, mid), 1, 2)
                w2 = pltpu.roll(jnp.where(lane4 >= 126, prv, mid), 2, 2)
                n1 = src[pl.ds(r0 + 1, 4), :, cut]
                n2 = src[pl.ds(r0 + 2, 4), :, cut]
                s1 = src[pl.ds(r0 - 1, 4), :, cut]
                s2 = src[pl.ds(r0 - 2, 4), :, cut]
                cs = [coef[pl.ds(r0, 4), i : i + 1, cut] for i in range(6)]
                out = ext[pl.ds(r0, 4), CH : 2 * CH, cut] * mid
                out = out + mixed[:, 128 * t : 128 * t + 128].reshape(4, CH, 128)
                out = out + cs[0] * e1 + cs[1] * w1 + cs[2] * (e2 - w2)
                out = out + cs[3] * n1 + cs[4] * s1 + cs[5] * (n2 - s2)
                if prev is not None:
                    out = out - prev[pl.ds(r0, 4), :, cut]
                dst[pl.ds(r0, 4), :, cut] = out
            return carry

        lax.fori_loop(0, count, body, 0)

    for k in range(BLOCK):
        advance(k)

    half = power(BLOCK)

    def again(src, dst, sem, peer):
        return pltpu.make_async_remote_copy(
            half.at[pl.ds(src, RIM)], half.at[pl.ds(dst, RIM)],
            mid_send.at[sem], mid_recv.at[sem], device_id=(gx, peer), device_id_type=MESH)

    mid_s, mid_n = again(RIM, top, 0, south), again(rows, 0, 1, north)

    @pl.when(has_s)
    def _():
        mid_s.start()

    @pl.when(has_n)
    def _():
        mid_n.start()

    @pl.when(jnp.logical_not(has_s))
    def _():
        half[0:RIM] = jnp.zeros((RIM, CH, 384), F32)

    @pl.when(jnp.logical_not(has_n))
    def _():
        half[top : top + RIM] = jnp.zeros((RIM, CH, 384), F32)

    @pl.when(has_s)
    def _():
        mid_s.wait_send()
        mid_n.wait_recv()

    @pl.when(has_n)
    def _():
        mid_n.wait_send()
        mid_s.wait_recv()

    for k in range(BLOCK, ITERS):
        advance(k)

    pairs = [(i, k) for i in range(9) for k in range(i, 9)]

    def gram(r, sums):
        for o in range(2):
            for t in range(2):
                at = (r, pl.ds(8 * o, 8), pl.ds(128 * t, 128))
                vals = [power(k)[at] for k in range(9)]
                sums = [s + vals[i] * vals[k] for s, (i, k) in zip(sums, pairs)]
        return tuple(sums)

    sums = lax.fori_loop(RIM, top, gram, tuple(jnp.zeros((8, 128), F32) for _ in pairs))
    sums = dict(zip(pairs, sums))
    sub = lax.broadcasted_iota(jnp.int32, (16, 128), 0)
    lane16 = lanes((16, 128))
    folded = {p: jnp.sum(s, axis=0, keepdims=True) for p, s in sums.items()}
    mine = jnp.zeros((16, 128), F32)
    for k in range(9):
        col = jnp.zeros((16, 128), F32)
        for i in range(9):
            col = jnp.where(sub == i, folded[min(i, k), max(i, k)], col)
        mine = jnp.where(lane16 == k, jnp.sum(col, axis=1, keepdims=True), mine)

    def reduce_over(value, slots, send, recv, me, count, device):
        slots[me] = value
        copies = []
        for k in range(1, count):
            peer = lax.rem(me + k, count)
            copy = pltpu.make_async_remote_copy(
                slots.at[me], slots.at[me], send.at[k - 1], recv.at[me],
                device_id=device(peer), device_id_type=MESH)
            copy.start()
            copies.append(copy)
        for k in range(1, count):
            src = lax.rem(me + count - k, count)
            pltpu.make_async_remote_copy(
                slots.at[src], slots.at[src], send.at[k - 1], recv.at[src],
                device_id=device(src), device_id_type=MESH).wait_recv()
        value = slots[0]
        for k in range(1, count):
            value = value + slots[k]
        return value, copies

    value, sent = reduce_over(mine, gx_slots, gxs_send, gxs_recv, gx, nx, lambda p: (p, gy))
    value, more = reduce_over(value, gy_slots, gys_send, gys_recv, gy, ny, lambda p: (gx, p))

    plain = [jnp.broadcast_to(value[:, k : k + 1], (16, 128)) for k in range(9)]
    diag = jnp.zeros((16, 128), F32)
    for k in range(9):
        diag = jnp.where(sub == k, plain[k], diag)
    size = jnp.sqrt(diag)
    cols = [plain[k] + trial[k] * size * size[k : k + 1, :] for k in range(9)]
    q = gmres(cols)
    d = apply_a(q)
    q0 = jnp.broadcast_to(q[:, 0:1], (16, 128))
    d0 = jnp.broadcast_to(d[:, 0:1], (16, 128))
    left0 = jnp.where(sub == 0, 1.0, 0.0) - d0
    dq, dd = q - q0, d - d0
    bad_q = dot(dq, mat_vec(plain, dq, 8)) - TRUST**2 * dot(q0, mat_vec(plain, q0, 8))
    bad_d = dot(dd, mat_vec(plain, dd, 9)) - TRUST**2 * dot(left0, mat_vec(plain, left0, 9))
    fine = (bad_q <= 0.0) & (bad_d <= 0.0)
    flag[...] = jnp.broadcast_to(jnp.where(fine, 0.0, 1.0), (8, 128))

    qs = [q0[k : k + 1, :] for k in range(8)]
    ds = [left0[k : k + 1, :] for k in range(9)]

    @pl.loop(0, rows)
    def _(r):
        for t in range(2):
            cut = pl.ds(128 * t, 128)
            vals = [power(k)[r + RIM, :, cut] for k in range(9)]
            s = qs[0] * vals[0]
            e = ds[0] * vals[0]
            for k in range(1, 8):
                s = s + qs[k] * vals[k]
            for k in range(1, 9):
                e = e + ds[k] * vals[k]
            sol[r, :, cut] = s
            res[r, :, cut] = e

    go_west.wait_send()
    go_east.wait_send()
    for copy in sent + more:
        copy.wait_send()


def fused(nx, ny, stk, coup, lat_total):
    rows = stk.shape[0]
    total = rows + 2 * RIM
    vm = pl.BlockSpec(memory_space=pltpu.VMEM)
    hbm = pl.BlockSpec(memory_space=pl.ANY)
    dma = pltpu.SemaphoreType.DMA
    out = jax.ShapeDtypeStruct((rows, CH, 256), F32)
    return pl.pallas_call(
        functools.partial(kernel, nx, ny),
        out_shape=(out, out, jax.ShapeDtypeStruct((8, 128), F32)),
        in_specs=[hbm, vm, vm, hbm],
        out_specs=(vm, vm, vm),
        scratch_shapes=[
            pltpu.VMEM((total, 40, 384), F32),
            pltpu.VMEM((8, total, CH, 384), F32),
            pltpu.VMEM((total, 8, 384), F32),
            pltpu.VMEM((2, total // 8, 40, 128), F32),
            pltpu.VMEM((2, rows // 8, 40, 128), F32),
            pltpu.VMEM((total, 128), F32),
            pltpu.VMEM((nx, 16, 128), F32),
            pltpu.VMEM((ny, 16, 128), F32),
            dma, dma, dma((2,)), dma((2,)), dma((4,)), dma((4,)), dma((2,)), dma((2,)),
            dma((2,)), dma((2,)), dma((nx,)), dma((nx,)), dma((ny,)), dma((ny,)),
        ],
        compiler_params=pltpu.CompilerParams(
            collective_id=0, has_side_effects=True, vmem_limit_bytes=48 * 1024 * 1024),
        name="krylov",
    )(stk, coup, jnp.asarray(trial_table()), jnp.asarray(kx_table(lat_total)))


def shifted(cells, axis, dim, closed, width):
    count = lax.axis_size(axis)
    ends = count if closed else count - 1
    head = lax.slice_in_dim(cells, 0, width, axis=dim)
    tail = lax.slice_in_dim(cells, cells.shape[dim] - width, cells.shape[dim], axis=dim)
    return jnp.concatenate(
        [
            lax.ppermute(tail, axis, [(i, (i + 1) % count) for i in range(ends)]),
            cells,
            lax.ppermute(head, axis, [((i + 1) % count, i) for i in range(ends)]),
        ],
        axis=dim,
    )


def apply_plain(vec, damping, coupling, wind_lon, wind_lat, kx):
    wide = shifted(vec, "gx", 2, True, 2)
    tall = shifted(vec, "gy", 1, False, 2)
    e1, w1, e2, w2 = wide[:, :, 3:-1], wide[:, :, 1:-3], wide[:, :, 4:], wide[:, :, :-4]
    n1, s1, n2, s2 = tall[:, 3:-1], tall[:, 1:-3], tall[:, 4:], tall[:, :-4]
    mixed = jnp.einsum("ij,jab->iab", coupling, vec, precision=lax.Precision.HIGHEST)
    return (
        (1.0 + damping) * vec + 0.25 * mixed
        + kx * (2.0 * vec - e1 - w1) + 0.5 * (2.0 * vec - n1 - s1)
        + wind_lon * ((8.0 * (e1 - w1) - (e2 - w2)) / 12.0)
        + wind_lat * ((8.0 * (n1 - s1) - (n2 - s2)) / 12.0)
    )


def careful(forcing, damping, coupling, wind_lon, wind_lat):
    rows = forcing.shape[1]
    pos = (lax.axis_index("gy") * rows + jnp.arange(rows)).astype(F32)
    phi = -math.pi / 2 + (pos + 0.5) * (math.pi / (rows * lax.axis_size("gy")))
    kx = (0.5 / (jnp.cos(phi) ** 2 + 0.1))[:, None]
    operate = lambda v: apply_plain(v, damping, coupling, wind_lon, wind_lat, kx)
    every = ("gx", "gy")
    first = jnp.sqrt(lax.psum(jnp.sum(forcing * forcing), every) + 1.0)
    basis = jnp.zeros((ITERS,) + forcing.shape, F32).at[0].set(forcing / first)
    heights = jnp.zeros((ITERS + 1, ITERS), F32)

    def body(j, state):
        basis, heights = state
        w = operate(lax.dynamic_index_in_dim(basis, j, 0, keepdims=False))
        h = lax.psum(jnp.sum(basis * w[None], axis=(1, 2, 3)), every)
        w = w - jnp.sum(h[:, None, None, None] * basis, axis=0)
        below = jnp.sqrt(lax.psum(jnp.sum(w * w), every) + 1.0)
        col = jnp.concatenate([h, jnp.zeros((1,), F32)])
        col = jnp.where(jnp.arange(ITERS + 1) == j + 1, below, col)
        heights = lax.dynamic_update_slice(heights, col[:, None], (0, j))
        old = lax.dynamic_index_in_dim(basis, jnp.minimum(j + 1, ITERS - 1), 0, keepdims=False)
        new = jnp.where(j + 1 < ITERS, w / below, old)
        basis = lax.dynamic_update_index_in_dim(basis, new, jnp.minimum(j + 1, ITERS - 1), 0)
        return basis, heights

    basis, heights = lax.fori_loop(0, ITERS, body, (basis, heights))
    h = [[heights[i, j] for j in range(ITERS)] for i in range(ITERS + 1)]
    target = [first] + [jnp.zeros((), F32)] * ITERS
    turns = []
    for j in range(ITERS):
        for i in range(j):
            c, s = turns[i]
            h[i][j], h[i + 1][j] = c * h[i][j] + s * h[i + 1][j], c * h[i + 1][j] - s * h[i][j]
        radius = jnp.sqrt(h[j][j] * h[j][j] + h[j + 1][j] * h[j + 1][j])
        c, s = h[j][j] / radius, h[j + 1][j] / radius
        turns.append((c, s))
        h[j][j] = radius
        target[j], target[j + 1] = c * target[j] + s * target[j + 1], c * target[j + 1] - s * target[j]
    y = [None] * ITERS
    for j in reversed(range(ITERS)):
        part = target[j]
        for i in range(j + 1, ITERS):
            part = part - h[j][i] * y[i]
        y[j] = part / h[j][j]
    weights = jnp.stack(y)
    answer = jnp.sum(weights[:, None, None, None] * basis, axis=0)
    return answer, forcing - operate(answer)


def per_device(nx, ny, forcing, damping, coupling, wind_lon, wind_lat):
    channels, rows, cols = forcing.shape
    pad = jnp.zeros((6, rows, cols), F32)
    stk = jnp.concatenate([forcing, damping, wind_lon[None], wind_lat[None], pad], axis=0)
    stk = jnp.transpose(stk, (1, 0, 2))
    sol, res, flag = fused(nx, ny, stk, coupling, rows * ny)
    trusted = jnp.max(flag) == 0.0
    back = lambda: (jnp.transpose(sol, (1, 0, 2)), jnp.transpose(res, (1, 0, 2)))
    slow = lambda: careful(forcing, damping, coupling, wind_lon, wind_lat)
    return lax.cond(trusted, back, slow)


def solution(mesh):
    nx, ny = mesh.shape["gx"], mesh.shape["gy"]
    in_specs = (P(None, "gy", "gx"), P(None, "gy", "gx"), P(), P("gy", "gx"), P("gy", "gx"))
    out_specs = (P(None, "gy", "gx"), P(None, "gy", "gx"))
    return jax.shard_map(
        functools.partial(per_device, nx, ny),
        mesh=mesh, in_specs=in_specs, out_specs=out_specs, check_vma=False,
    )
```

```python
import functools
import math

import jax
import jax.numpy as jnp
import numpy as np
from jax import lax
from jax.experimental import pallas as pl
from jax.experimental.pallas import tpu as pltpu
from jax.experimental.layout import Layout, with_layout_constraint
from jax.sharding import PartitionSpec as P

ITERS = 8
CH = 16
RIM = 8
LOW, HIGH = 1.0, 16.0
MID, HALF = (LOW + HIGH) / 2, (HIGH - LOW) / 2
BLOCK = 4
NOISE = 1.2e-7
TRUST = 1.0e-4
MESH = pl.DeviceIdType.MESH
F32 = jnp.float32


def trial_table():
    rng = np.random.default_rng(7)
    draw = rng.choice([-1.0, 1.0], size=(9, 16, 128)) * NOISE
    table = np.zeros((9, 16, 128), np.float32)
    for i in range(9):
        for k in range(i, 9):
            table[i, k] = draw[i, k]
            table[k, i] = draw[i, k]
    table[:, :, 0] = 0.0
    return table


def kx_table(lat_total):
    row = np.arange(lat_total) + 0.5
    phi = -math.pi / 2 + row * (math.pi / lat_total)
    table = np.zeros((lat_total + 2 * RIM, 128), np.float32)
    table[RIM : RIM + lat_total] = (0.5 / (np.cos(phi) ** 2 + 0.1))[:, None]
    return table


def lanes(shape):
    return lax.broadcasted_iota(jnp.int32, shape, len(shape) - 1)


def apply_a(vec):
    sub = lax.broadcasted_iota(jnp.int32, vec.shape, 0)
    up = pltpu.roll(vec, 1, 0)
    kept = jnp.where((sub == 0) | (sub == BLOCK), 0.0, vec)
    down = pltpu.roll(kept, 15, 0)
    return MID * vec + (HALF / 2) * (up + down)


def mat_vec(cols, vec, count):
    total = cols[0] * vec[0:1, :]
    for k in range(1, count):
        total = total + cols[k] * vec[k : k + 1, :]
    return total


def dot(a, b):
    return jnp.sum(a * b, axis=0, keepdims=True)


def gmres(cols):
    sub = lax.broadcasted_iota(jnp.int32, (16, 128), 0)
    first = jnp.sqrt(cols[0][0:1, :] + 1.0)
    basis = [jnp.where(sub == 0, 1.0, 0.0) / first]
    target = first
    targets = []
    columns = []
    turns = []
    for j in range(ITERS):
        w = apply_a(basis[j])
        u = mat_vec(cols, w, j + 2)
        h = [dot(v, u) for v in basis]
        for i in range(j + 1):
            w = w - h[i] * basis[i]
        norm = dot(w, mat_vec(cols, w, j + 2))
        below = jnp.sqrt(jnp.maximum(norm, 0.0) + 1.0)
        if j + 1 < ITERS:
            basis.append(w / below)
        col = list(h)
        for i, (c, s) in enumerate(turns):
            if i + 1 <= j:
                col[i], col[i + 1] = c * col[i] + s * col[i + 1], c * col[i + 1] - s * col[i]
        radius = jnp.sqrt(col[j] * col[j] + below * below)
        inv = 1.0 / radius
        c, s = col[j] * inv, below * inv
        turns.append((c, s))
        col[j] = radius
        columns.append((col, inv))
        targets.append(c * target)
        target = -s * target
    y = [None] * ITERS
    for j in reversed(range(ITERS)):
        y[j] = targets[j] * columns[j][1]
        for i in range(j):
            targets[i] = targets[i] - columns[j][0][i] * y[j]
    q = basis[0] * y[0]
    for j in range(1, ITERS):
        q = q + basis[j] * y[j]
    return q


def kernel(
    nx, ny, forc, damp, wlon, wlat, coup, trial, kxs, sol, res, flag,
    *scratch,
):
    pwr, scratch = scratch[:ITERS], scratch[ITERS:]
    (ext, coef, main, wind, lon, pack, kxv, mix, made, rims, gx_slots, gy_slots, outs,
     in_sem, kx_sem, lon_send, lon_recv, lat_send, lat_recv, cor_send, cor_recv,
     mid_send, mid_recv, gxs_send, gxs_recv, gys_send, gys_recv, out_sem) = scratch
    gx, gy = lax.axis_index("gx"), lax.axis_index("gy")
    rows = forc.shape[1]
    top = RIM + rows
    total = rows + 2 * RIM
    groups = rows // 8
    east, west = lax.rem(gx + 1, nx), lax.rem(gx + nx - 1, nx)
    north, south = gy + 1, gy - 1
    has_n, has_s = gy < ny - 1, gy > 0
    no_n, no_s = jnp.logical_not(has_n), jnp.logical_not(has_s)

    loads = []
    for c in range(CH):
        for n, src in enumerate((forc, damp)):
            loads.append(pltpu.make_async_copy(
                src.at[c], ext.at[pl.ds(RIM, rows), CH * n + c, pl.ds(0, 256)],
                in_sem.at[CH * n + c]))
    for n, src in enumerate((wlon, wlat)):
        loads.append(pltpu.make_async_copy(
            src, wind.at[n, pl.ds(RIM, rows), pl.ds(0, 256)], in_sem.at[2 * CH + n]))
    start = pl.multiple_of(gy * rows, 8)
    loads.append(pltpu.make_async_copy(kxs.at[pl.ds(start, total), :], kxv, kx_sem))
    for copy in loads:
        copy.start()

    barrier = pltpu.get_barrier_semaphore()
    for k in range(1, nx):
        pl.semaphore_signal(barrier, 1, device_id=(lax.rem(gx + k, nx), gy), device_id_type=MESH)
    for k in range(1, ny):
        pl.semaphore_signal(barrier, 1, device_id=(gx, lax.rem(gy + k, ny)), device_id_type=MESH)
    for copy in loads:
        copy.wait()

    def turn(value, by):
        by = by % 128
        return pltpu.roll(value, by, value.ndim - 1) if by else value

    lane32, lane8 = lanes((2 * CH, 128)), lanes((8, 128))

    @pl.loop(0, groups)
    def _(g):
        for side in range(2):
            shift, cut = (0, pl.ds(0, 128)) if side == 0 else (16, pl.ds(128, 128))
            out = jnp.zeros((2 * CH, 128), F32)
            for j in range(8):
                here = (lane32 >= 16 * j) & (lane32 < 16 * j + 16)
                out = jnp.where(here, turn(ext[RIM + 8 * g + j, :, cut], 16 * j + shift), out)
            pack[side, g, 0 : 2 * CH, :] = out
            at = pl.ds(pl.multiple_of(RIM + 8 * g, 8), 8)
            a = turn(wind[0, at, cut], shift)
            b = turn(wind[1, at, cut], 16 + shift)
            pack[side, g, 2 * CH :, :] = jnp.where(lane8 < 16, a, b)

    pl.semaphore_wait(barrier, nx + ny - 2)

    go_west = pltpu.make_async_remote_copy(
        pack.at[0], lon.at[0, pl.ds(1, groups)], lon_send.at[0], lon_recv.at[0],
        device_id=(west, gy), device_id_type=MESH)
    go_east = pltpu.make_async_remote_copy(
        pack.at[1], lon.at[1, pl.ds(1, groups)], lon_send.at[1], lon_recv.at[1],
        device_id=(east, gy), device_id_type=MESH)
    go_west.start()
    go_east.start()

    def strip(ref, src, dst, size, chan, sem, peer):
        return pltpu.make_async_remote_copy(
            ref.at[pl.ds(src, size), chan, pl.ds(0, 256)],
            ref.at[pl.ds(dst, size), chan, pl.ds(0, 256)],
            lat_send.at[sem], lat_recv.at[sem], device_id=(gx, peer), device_id_type=MESH)

    def breeze(src, dst, sem, peer):
        return pltpu.make_async_remote_copy(
            wind.at[:, pl.ds(src, 8), pl.ds(0, 256)], wind.at[:, pl.ds(dst, 8), pl.ds(0, 256)],
            lat_send.at[sem], lat_recv.at[sem], device_id=(gx, peer), device_id_type=MESH)

    vec, par = pl.ds(0, CH), pl.ds(CH, CH)
    to_s = [breeze(RIM, top, 4, south), strip(ext, RIM, top, RIM, vec, 0, south),
            strip(ext, RIM, top, RIM - 2, par, 1, south)]
    to_n = [breeze(rows, 0, 5, north), strip(ext, rows, 0, RIM, vec, 2, north),
            strip(ext, rows + 2, 2, RIM - 2, par, 3, north)]

    @pl.when(has_s)
    def _():
        for copy in to_s:
            copy.start()

    @pl.when(has_n)
    def _():
        for copy in to_n:
            copy.start()

    for missing, row, slot in ((no_s, 0, 0), (no_n, top, groups + 1)):
        @pl.when(missing)
        def _():
            ext[row : row + RIM, 0 : 2 * CH, 0:256] = jnp.zeros((RIM, 2 * CH, 256), F32)
            wind[:, row : row + RIM, 0:256] = jnp.zeros((2, RIM, 256), F32)
            lon[:, slot] = jnp.zeros((2, 40, 128), F32)

    go_west.wait_recv()
    go_east.wait_recv()
    cor_s = pltpu.make_async_remote_copy(
        lon.at[:, 1], lon.at[:, groups + 1], cor_send.at[0], cor_recv.at[0],
        device_id=(gx, south), device_id_type=MESH)
    cor_n = pltpu.make_async_remote_copy(
        lon.at[:, groups], lon.at[:, 0], cor_send.at[1], cor_recv.at[1],
        device_id=(gx, north), device_id_type=MESH)

    @pl.when(has_s)
    def _():
        cor_s.start()

    @pl.when(has_n)
    def _():
        cor_n.start()

    two = 2.0 / HALF
    kind = lax.broadcasted_iota(jnp.int32, (8, 128), 0)
    by_kx = jnp.where(kind < 2, -two, 0.0)
    by_one = jnp.where((kind == 3) | (kind == 4), -0.5 * two, 0.0)
    eight = two * 8.0 / 12.0
    by_lon = jnp.where(kind == 0, eight, 0.0) + jnp.where(kind == 1, -eight, 0.0)
    by_lon = by_lon + jnp.where(kind == 2, -two / 12.0, 0.0)
    by_lat = jnp.where(kind == 3, eight, 0.0) + jnp.where(kind == 4, -eight, 0.0)
    by_lat = by_lat + jnp.where(kind == 5, -two / 12.0, 0.0)

    def merge(from_e, from_w):
        at = lanes(from_e.shape)
        return jnp.where(at < 16, from_e, jnp.where(at >= 112, from_w, 0.0))

    def prepare(g):
        at = pl.ds(pl.multiple_of(8 * g, 8), 8)
        for j in range(8):
            ext[8 * g + j, 0 : 2 * CH, 256:384] = merge(
                turn(lon[0, g, 0 : 2 * CH, :], -16 * j), turn(lon[1, g, 0 : 2 * CH, :], 112 - 16 * j))
        for n in range(2):
            wind[n, at, 256:384] = merge(
                turn(lon[0, g, 2 * CH :, :], -16 * n), turn(lon[1, g, 2 * CH :, :], 112 - 16 * n))
        kx8 = kxv[at, :]
        in8 = jnp.where(kx8 > 0.0, 1.0, 0.0)
        for t in range(3):
            cut = pl.ds(128 * t, 128)
            lon8, lat8 = wind[0, at, cut], wind[1, at, cut]
            for j in range(8):
                one = slice(j, j + 1)
                coef[8 * g + j, :, cut] = (
                    kx8[one] * by_kx + in8[one] * by_one + by_lon * lon8[one] + by_lat * lat8[one])
                diag = ext[8 * g + j, CH : 2 * CH, cut]
                gain, base = two * in8[one], (two * (2.0 - MID)) * in8[one] + (2.0 * two) * kx8[one]
                main[8 * g + j, :, cut] = diag * gain + base

    @pl.loop(1, groups + 1)
    def _(g):
        prepare(g)

    cm = coup[...] * (0.25 * two)
    cm = jnp.concatenate([jnp.concatenate([cm] * 4, axis=1)] * 4, axis=0)
    r4 = lax.broadcasted_iota(jnp.int32, (64, 64), 0) // 16
    c4 = lax.broadcasted_iota(jnp.int32, (64, 64), 1) // 16
    cm = jnp.where(r4 == c4, cm, 0.0)
    cm_hi = cm.astype(jnp.bfloat16)
    cm_lo = (cm - cm_hi.astype(F32)).astype(jnp.bfloat16)
    weights = jnp.concatenate([cm_hi, cm_hi, cm_lo], axis=1)

    def power(k):
        return ext.at[:, pl.ds(0, CH), :] if k == 0 else pwr[k - 1]

    lane4 = lanes((4, CH, 128))

    def couple(src, r0):
        mids = [src[pl.ds(r0, 4), :, 128 * t : 128 * t + 128] for t in range(3)]
        flat = jnp.concatenate([m.reshape(64, 128) for m in mids], axis=1)
        hi = flat.astype(jnp.bfloat16)
        lo = (flat - hi.astype(F32)).astype(jnp.bfloat16)
        return jnp.dot(weights, jnp.concatenate([hi, lo, hi], axis=0), preferred_element_type=F32)

    def stencil(k, r0, mixed):
        src, dst = power(k), power(k + 1)
        prev = power(k - 1) if k % BLOCK else None
        mids = [src[pl.ds(r0, 4), :, 128 * t : 128 * t + 128] for t in range(3)]
        for t in range(3):
            cut = pl.ds(128 * t, 128)
            mid, nxt, prv = mids[t], mids[(t + 1) % 3], mids[(t + 2) % 3]
            e1 = pltpu.roll(jnp.where(lane4 < 1, nxt, mid), 127, 2)
            e2 = pltpu.roll(jnp.where(lane4 < 2, nxt, mid), 126, 2)
            w1 = pltpu.roll(jnp.where(lane4 >= 127, prv, mid), 1, 2)
            w2 = pltpu.roll(jnp.where(lane4 >= 126, prv, mid), 2, 2)
            n1 = src[pl.ds(r0 + 1, 4), :, cut]
            n2 = src[pl.ds(r0 + 2, 4), :, cut]
            s1 = src[pl.ds(r0 - 1, 4), :, cut]
            s2 = src[pl.ds(r0 - 2, 4), :, cut]
            cs = [coef[pl.ds(r0, 4), i : i + 1, cut] for i in range(6)]
            out = main[pl.ds(r0, 4), :, cut] * mid
            out = out + mixed[:, 128 * t : 128 * t + 128].reshape(4, CH, 128)
            out = out + cs[0] * e1 + cs[1] * w1 + cs[2] * (e2 - w2)
            out = out + cs[3] * n1 + cs[4] * s1 + cs[5] * (n2 - s2)
            if prev is not None:
                out = out - prev[pl.ds(r0, 4), :, cut]
            dst[pl.ds(r0, 4), :, cut] = out

    def inner(k):
        m = k % BLOCK + 1
        low, count = RIM + 2 * m, (rows - 4 * m) // 4
        mix[0] = couple(power(k), low)

        def body(g, carry):
            r0 = low + 4 * g
            ahead = couple(power(k), jnp.minimum(r0 + 4, low + 4 * (count - 1)))
            stencil(k, r0, mix[g % 2])
            mix[(g + 1) % 2] = ahead
            return carry

        lax.fori_loop(0, count, body, 0)

    def outer(k):
        m = k % BLOCK + 1
        for r0 in (2 * m, 2 * m + 4, top - 2 * m, top - 2 * m + 4):
            stencil(k, r0, couple(power(k), r0))

    for k in range(BLOCK):
        inner(k)

    @pl.when(has_s)
    def _():
        for copy in to_s:
            copy.wait_send()
        cor_s.wait_send()
        for copy in to_n:
            copy.wait_recv()
        cor_n.wait_recv()

    @pl.when(has_n)
    def _():
        for copy in to_n:
            copy.wait_send()
        cor_n.wait_send()
        for copy in to_s:
            copy.wait_recv()
        cor_s.wait_recv()

    prepare(0)
    prepare(groups + 1)
    for k in range(BLOCK):
        outer(k)

    half = power(BLOCK)
    lane16 = lanes((CH, 128))
    for side, row in ((0, RIM), (1, rows)):
        out = jnp.zeros((CH, 128), F32)
        for j in range(8):
            here = (lane16 >= 16 * j) & (lane16 < 16 * j + 16)
            out = jnp.where(here, turn(half[row + j, :, 256:384], 16 * j + 8), out)
        made[side] = out

    def again(src, dst, sem, peer):
        return pltpu.make_async_remote_copy(
            half.at[pl.ds(src, RIM), :, pl.ds(0, 256)], half.at[pl.ds(dst, RIM), :, pl.ds(0, 256)],
            mid_send.at[sem], mid_recv.at[sem], device_id=(gx, peer), device_id_type=MESH)

    def also(src, dst, sem, peer):
        return pltpu.make_async_remote_copy(
            made.at[src], rims.at[dst], mid_send.at[sem], mid_recv.at[sem],
            device_id=(gx, peer), device_id_type=MESH)

    mid_s = [also(0, 1, 2, south), again(RIM, top, 0, south)]
    mid_n = [also(1, 0, 3, north), again(rows, 0, 1, north)]

    @pl.when(has_s)
    def _():
        for copy in mid_s:
            copy.start()

    @pl.when(has_n)
    def _():
        for copy in mid_n:
            copy.start()

    for missing, row, slot in ((no_s, 0, 0), (no_n, top, 1)):
        @pl.when(missing)
        def _():
            half[row : row + RIM, :, 0:256] = jnp.zeros((RIM, CH, 256), F32)
            rims[slot] = jnp.zeros((CH, 128), F32)

    for k in range(BLOCK, ITERS):
        inner(k)

    pairs = [(i, k) for i in range(9) for k in range(i, 9)]

    def gram(r, sums):
        for o in range(2):
            for t in range(2):
                at = (r, pl.ds(8 * o, 8), pl.ds(128 * t, 128))
                vals = [power(k)[at] for k in range(9)]
                sums = [s + vals[i] * vals[k] for s, (i, k) in zip(sums, pairs)]
        return tuple(sums)

    sums = tuple(jnp.zeros((8, 128), F32) for _ in pairs)
    sums = lax.fori_loop(2 * RIM, top - RIM, gram, sums)

    @pl.when(has_s)
    def _():
        for copy in mid_s:
            copy.wait_send()
        for copy in mid_n:
            copy.wait_recv()

    @pl.when(has_n)
    def _():
        for copy in mid_n:
            copy.wait_send()
        for copy in mid_s:
            copy.wait_recv()

    for side, row in ((0, 0), (1, top)):
        for j in range(8):
            half[row + j, :, 256:384] = turn(rims[side], -16 * j - 8)
    for k in range(BLOCK, ITERS):
        outer(k)
    sums = lax.fori_loop(RIM, 2 * RIM, gram, sums)
    sums = lax.fori_loop(top - RIM, top, gram, sums)

    sums = dict(zip(pairs, sums))
    folded = {p: jnp.sum(s, axis=0, keepdims=True) for p, s in sums.items()}
    sub8 = lax.broadcasted_iota(jnp.int32, (8, 128), 0)
    mine = jnp.zeros((8, 128), F32)
    for k in range(10):
        col = jnp.zeros((8, 128), F32)
        if k < 9:
            for i in range(8):
                col = jnp.where(sub8 == i, folded[min(i, k), max(i, k)], col)
        else:
            col = jnp.where(sub8 == 0, folded[8, 8], col)
        mine = jnp.where(lane8 == k, jnp.sum(col, axis=1, keepdims=True), mine)

    def reduce_over(value, slots, send, recv, me, count, device):
        slots[me] = value
        copies = []
        for k in range(1, count):
            peer = lax.rem(me + k, count)
            copy = pltpu.make_async_remote_copy(
                slots.at[me], slots.at[me], send.at[k - 1], recv.at[me],
                device_id=device(peer), device_id_type=MESH)
            copy.start()
            copies.append(copy)
        for k in range(1, count):
            src = lax.rem(me + count - k, count)
            pltpu.make_async_remote_copy(
                slots.at[src], slots.at[src], send.at[k - 1], recv.at[src],
                device_id=device(src), device_id_type=MESH).wait_recv()
        parts = [slots[k] for k in range(count)]
        while len(parts) > 1:
            parts = [sum(parts[i : i + 2][1:], parts[i]) for i in range(0, len(parts), 2)]
        return parts[0], copies

    value, sent = reduce_over(mine, gx_slots, gxs_send, gxs_recv, gx, nx, lambda p: (p, gy))
    value, more = reduce_over(value, gy_slots, gys_send, gys_recv, gy, ny, lambda p: (gx, p))

    upper = [jnp.broadcast_to(value[:, k : k + 1], (8, 128)) for k in range(10)]
    lower = [upper[8][k : k + 1, :] for k in range(8)] + [upper[9][0:1, :]]
    plain = [jnp.concatenate([u, jnp.where(sub8 == 0, w, 0.0)]) for u, w in zip(upper, lower)]
    sub = lax.broadcasted_iota(jnp.int32, (16, 128), 0)
    diag = jnp.zeros((16, 128), F32)
    for k in range(9):
        diag = jnp.where(sub == k, plain[k], diag)
    size = jnp.sqrt(diag)
    cols = [plain[k] + trial[k] * size * size[k : k + 1, :] for k in range(9)]
    q = gmres(cols)
    d = apply_a(q)
    q0 = jnp.broadcast_to(q[:, 0:1], (16, 128))
    d0 = jnp.broadcast_to(d[:, 0:1], (16, 128))
    left0 = jnp.where(sub == 0, 1.0, 0.0) - d0
    dq, dd = q - q0, d - d0
    bad_q = dot(dq, mat_vec(plain, dq, 8)) - TRUST**2 * dot(q0, mat_vec(plain, q0, 8))
    bad_d = dot(dd, mat_vec(plain, dd, 9)) - TRUST**2 * dot(left0, mat_vec(plain, left0, 9))
    fine = (bad_q <= 0.0) & (bad_d <= 0.0)
    flag[0, 0] = jnp.max(jnp.where(fine, 0.0, 1.0))

    qs = [q0[k : k + 1, :] for k in range(8)]
    ds = [left0[k : k + 1, :] for k in range(9)]
    stores = []
    part = rows // 2
    for h in range(2):
        @pl.loop(h * part, (h + 1) * part)
        def _(r):
            for t in range(2):
                cut = pl.ds(128 * t, 128)
                vals = [power(k)[r + RIM, :, cut] for k in range(9)]
                s = qs[0] * vals[0]
                e = ds[0] * vals[0]
                for k in range(1, 8):
                    s = s + qs[k] * vals[k]
                for k in range(1, 9):
                    e = e + ds[k] * vals[k]
                outs[0, r, :, cut] = s
                outs[1, r, :, cut] = e

        for c in range(CH):
            for n, dst in enumerate((sol, res)):
                copy = pltpu.make_async_copy(
                    outs.at[n, pl.ds(h * part, part), c, :],
                    dst.at[c, pl.ds(h * part, part), :], out_sem.at[h, n, c])
                copy.start()
                stores.append(copy)

    go_west.wait_send()
    go_east.wait_send()
    for copy in sent + more:
        copy.wait_send()
    for copy in stores:
        copy.wait()


def fused(nx, ny, forcing, damping, wind_lon, wind_lat, coup):
    rows = forcing.shape[1]
    total = rows + 2 * RIM
    vm = pl.BlockSpec(memory_space=pltpu.VMEM)
    hbm = pl.BlockSpec(memory_space=pltpu.HBM)
    dma = pltpu.SemaphoreType.DMA
    out = jax.ShapeDtypeStruct(forcing.shape, F32)
    return pl.pallas_call(
        functools.partial(kernel, nx, ny),
        out_shape=(out, out, jax.ShapeDtypeStruct((1, 1), F32)),
        in_specs=[hbm, hbm, hbm, hbm, vm, vm, hbm],
        out_specs=(hbm, hbm, pl.BlockSpec(memory_space=pltpu.SMEM)),
        scratch_shapes=[pltpu.VMEM((total, CH, 384), F32)] * ITERS + [
            pltpu.VMEM((total, 2 * CH, 384), F32),
            pltpu.VMEM((total, 8, 384), F32),
            pltpu.VMEM((total, CH, 384), F32),
            pltpu.VMEM((2, total, 384), F32),
            pltpu.VMEM((2, total // 8, 40, 128), F32),
            pltpu.VMEM((2, rows // 8, 40, 128), F32),
            pltpu.VMEM((total, 128), F32),
            pltpu.VMEM((2, 64, 384), F32),
            pltpu.VMEM((2, CH, 128), F32),
            pltpu.VMEM((2, CH, 128), F32),
            pltpu.VMEM((nx, 8, 128), F32),
            pltpu.VMEM((ny, 8, 128), F32),
            pltpu.VMEM((2, rows, CH, 256), F32),
            dma((2 * CH + 2,)), dma, dma((2,)), dma((2,)), dma((6,)), dma((6,)),
            dma((2,)), dma((2,)), dma((4,)), dma((4,)),
            dma((nx,)), dma((nx,)), dma((ny,)), dma((ny,)), dma((2, 2, CH)),
        ],
        compiler_params=pltpu.CompilerParams(
            collective_id=0, has_side_effects=True, vmem_limit_bytes=48 * 1024 * 1024),
        name="krylov",
    )(forcing, damping, wind_lon, wind_lat, coup,
      jnp.asarray(trial_table()), jnp.asarray(kx_table(rows * ny)))


def shifted(cells, axis, dim, closed, width):
    count = lax.axis_size(axis)
    ends = count if closed else count - 1
    head = lax.slice_in_dim(cells, 0, width, axis=dim)
    tail = lax.slice_in_dim(cells, cells.shape[dim] - width, cells.shape[dim], axis=dim)
    return jnp.concatenate(
        [
            lax.ppermute(tail, axis, [(i, (i + 1) % count) for i in range(ends)]),
            cells,
            lax.ppermute(head, axis, [((i + 1) % count, i) for i in range(ends)]),
        ],
        axis=dim,
    )


def apply_plain(vec, damping, coupling, wind_lon, wind_lat, kx):
    wide = shifted(vec, "gx", 2, True, 2)
    tall = shifted(vec, "gy", 1, False, 2)
    e1, w1, e2, w2 = wide[:, :, 3:-1], wide[:, :, 1:-3], wide[:, :, 4:], wide[:, :, :-4]
    n1, s1, n2, s2 = tall[:, 3:-1], tall[:, 1:-3], tall[:, 4:], tall[:, :-4]
    mixed = jnp.einsum("ij,jab->iab", coupling, vec, precision=lax.Precision.HIGHEST)
    return (
        (1.0 + damping) * vec + 0.25 * mixed
        + kx * (2.0 * vec - e1 - w1) + 0.5 * (2.0 * vec - n1 - s1)
        + wind_lon * ((8.0 * (e1 - w1) - (e2 - w2)) / 12.0)
        + wind_lat * ((8.0 * (n1 - s1) - (n2 - s2)) / 12.0)
    )


def careful(forcing, damping, coupling, wind_lon, wind_lat):
    rows = forcing.shape[1]
    pos = (lax.axis_index("gy") * rows + jnp.arange(rows)).astype(F32)
    phi = -math.pi / 2 + (pos + 0.5) * (math.pi / (rows * lax.axis_size("gy")))
    kx = (0.5 / (jnp.cos(phi) ** 2 + 0.1))[:, None]
    operate = lambda v: apply_plain(v, damping, coupling, wind_lon, wind_lat, kx)
    every = ("gx", "gy")
    first = jnp.sqrt(lax.psum(jnp.sum(forcing * forcing), every) + 1.0)
    basis = jnp.zeros((ITERS,) + forcing.shape, F32).at[0].set(forcing / first)
    heights = jnp.zeros((ITERS + 1, ITERS), F32)

    def body(j, state):
        basis, heights = state
        w = operate(lax.dynamic_index_in_dim(basis, j, 0, keepdims=False))
        h = lax.psum(jnp.sum(basis * w[None], axis=(1, 2, 3)), every)
        w = w - jnp.sum(h[:, None, None, None] * basis, axis=0)
        below = jnp.sqrt(lax.psum(jnp.sum(w * w), every) + 1.0)
        col = jnp.concatenate([h, jnp.zeros((1,), F32)])
        col = jnp.where(jnp.arange(ITERS + 1) == j + 1, below, col)
        heights = lax.dynamic_update_slice(heights, col[:, None], (0, j))
        old = lax.dynamic_index_in_dim(basis, jnp.minimum(j + 1, ITERS - 1), 0, keepdims=False)
        new = jnp.where(j + 1 < ITERS, w / below, old)
        basis = lax.dynamic_update_index_in_dim(basis, new, jnp.minimum(j + 1, ITERS - 1), 0)
        return basis, heights

    basis, heights = lax.fori_loop(0, ITERS, body, (basis, heights))
    h = [[heights[i, j] for j in range(ITERS)] for i in range(ITERS + 1)]
    target = [first] + [jnp.zeros((), F32)] * ITERS
    turns = []
    for j in range(ITERS):
        for i in range(j):
            c, s = turns[i]
            h[i][j], h[i + 1][j] = c * h[i][j] + s * h[i + 1][j], c * h[i + 1][j] - s * h[i][j]
        radius = jnp.sqrt(h[j][j] * h[j][j] + h[j + 1][j] * h[j + 1][j])
        c, s = h[j][j] / radius, h[j + 1][j] / radius
        turns.append((c, s))
        h[j][j] = radius
        target[j], target[j + 1] = c * target[j] + s * target[j + 1], c * target[j + 1] - s * target[j]
    y = [None] * ITERS
    for j in reversed(range(ITERS)):
        part = target[j]
        for i in range(j + 1, ITERS):
            part = part - h[j][i] * y[i]
        y[j] = part / h[j][j]
    weights = jnp.stack(y)
    answer = jnp.sum(weights[:, None, None, None] * basis, axis=0)
    return answer, forcing - operate(answer)


def per_device(nx, ny, forcing, damping, coupling, wind_lon, wind_lat):
    sol, res, flag = fused(nx, ny, forcing, damping, wind_lon, wind_lat, coupling)

    pin = lambda x: with_layout_constraint(x, Layout(tuple(range(x.ndim))))

    def again(state):
        sol, res = careful(pin(forcing), pin(damping), coupling, wind_lon, wind_lat)
        return pin(sol), pin(res), jnp.zeros((), F32)

    done = lax.while_loop(lambda state: state[2] > 0.5, again, (sol, res, flag[0, 0]))
    return pin(done[0]), pin(done[1])


def solution(mesh):
    nx, ny = mesh.shape["gx"], mesh.shape["gy"]
    in_specs = (P(None, "gy", "gx"), P(None, "gy", "gx"), P(), P("gy", "gx"), P("gy", "gx"))
    out_specs = (P(None, "gy", "gx"), P(None, "gy", "gx"))
    return jax.shard_map(
        functools.partial(per_device, nx, ny),
        mesh=mesh, in_specs=in_specs, out_specs=out_specs, check_vma=False,
    )
```

```python
import functools
import math

import jax
import jax.numpy as jnp
import numpy as np
from jax import lax
from jax.experimental import pallas as pl
from jax.experimental.pallas import tpu as pltpu
from jax.experimental.layout import Layout, with_layout_constraint
from jax.sharding import PartitionSpec as P

ITERS = 8
CH = 16
RIM = 8
LOW, HIGH = 1.0, 16.0
MID, HALF = (LOW + HIGH) / 2, (HIGH - LOW) / 2
BLOCK = 4
NOISE = 1.2e-7
TRUST = 1.0e-4
MESH = pl.DeviceIdType.MESH
F32 = jnp.float32


def trials():
    sub = lax.broadcasted_iota(jnp.int32, (16, 128), 0)
    lane = lanes((16, 128))
    tables = []
    for k in range(9):
        pair = jnp.minimum(sub, k) * 16 + jnp.maximum(sub, k)
        bits = pair * 1640531527 + lane * 668265263
        bits = (bits ^ lax.shift_right_logical(bits, 15)) * 739982445
        bits = bits ^ lax.shift_right_logical(bits, 13)
        sign = jnp.where((bits & 64) == 0, NOISE, -NOISE)
        tables.append(jnp.where((lane == 0) | (sub > 8), 0.0, sign))
    return tables


def row_kx(first, count, lat_total):
    row = (first + lax.broadcasted_iota(jnp.int32, (count, 128), 0)).astype(F32)
    phi = -math.pi / 2 + (row + 0.5) * (math.pi / lat_total)
    inside = (row >= 0.0) & (row < lat_total)
    cos = jnp.cos(phi)
    return jnp.where(inside, 0.5 / (cos * cos + 0.1), 0.0)


def lanes(shape):
    return lax.broadcasted_iota(jnp.int32, shape, len(shape) - 1)


def apply_a(vec):
    sub = lax.broadcasted_iota(jnp.int32, vec.shape, 0)
    up = pltpu.roll(vec, 1, 0)
    kept = jnp.where((sub == 0) | (sub == BLOCK), 0.0, vec)
    down = pltpu.roll(kept, 15, 0)
    return MID * vec + (HALF / 2) * (up + down)


def mat_vec(cols, vec, count):
    total = cols[0] * vec[0:1, :]
    for k in range(1, count):
        total = total + cols[k] * vec[k : k + 1, :]
    return total


def dot(a, b):
    return jnp.sum(a * b, axis=0, keepdims=True)


def gmres(cols):
    sub = lax.broadcasted_iota(jnp.int32, (16, 128), 0)
    first = jnp.sqrt(cols[0][0:1, :] + 1.0)
    basis = [jnp.where(sub == 0, 1.0, 0.0) / first]
    target = first
    targets = []
    columns = []
    turns = []
    for j in range(ITERS):
        w = apply_a(basis[j])
        u = mat_vec(cols, w, j + 2)
        h = [dot(v, u) for v in basis]
        for i in range(j + 1):
            w = w - h[i] * basis[i]
        norm = dot(w, mat_vec(cols, w, j + 2))
        below = jnp.sqrt(jnp.maximum(norm, 0.0) + 1.0)
        if j + 1 < ITERS:
            basis.append(w / below)
        col = list(h)
        for i, (c, s) in enumerate(turns):
            if i + 1 <= j:
                col[i], col[i + 1] = c * col[i] + s * col[i + 1], c * col[i + 1] - s * col[i]
        radius = jnp.sqrt(col[j] * col[j] + below * below)
        inv = 1.0 / radius
        c, s = col[j] * inv, below * inv
        turns.append((c, s))
        col[j] = radius
        columns.append((col, inv))
        targets.append(c * target)
        target = -s * target
    y = [None] * ITERS
    for j in reversed(range(ITERS)):
        y[j] = targets[j] * columns[j][1]
        for i in range(j):
            targets[i] = targets[i] - columns[j][0][i] * y[j]
    q = basis[0] * y[0]
    for j in range(1, ITERS):
        q = q + basis[j] * y[j]
    return q


def kernel(
    nx, ny, forc, damp, wlon, wlat, coup_hbm, outs, flag,
    *scratch,
):
    pwr, scratch = scratch[:ITERS], scratch[ITERS:]
    (ext, coef, main, wind, lon, pack, kxv, coup, made, rims, gx_slots, gy_slots,
     in_sem, lon_send, lon_recv, lat_send, lat_recv, cor_send, cor_recv,
     mid_send, mid_recv, gxs_send, gxs_recv, gys_send, gys_recv) = scratch
    gx, gy = lax.axis_index("gx"), lax.axis_index("gy")
    rows = forc.shape[1]
    top = RIM + rows
    total = rows + 2 * RIM
    groups = rows // 8
    east, west = lax.rem(gx + 1, nx), lax.rem(gx + nx - 1, nx)
    north, south = gy + 1, gy - 1
    has_n, has_s = gy < ny - 1, gy > 0
    no_n, no_s = jnp.logical_not(has_n), jnp.logical_not(has_s)

    loads = []
    for c in range(CH):
        for n, src in enumerate((forc, damp)):
            loads.append(pltpu.make_async_copy(
                src.at[c], ext.at[pl.ds(RIM, rows), CH * n + c, pl.ds(0, 256)],
                in_sem.at[CH * n + c]))
    for n, src in enumerate((wlon, wlat)):
        loads.append(pltpu.make_async_copy(
            src, wind.at[n, pl.ds(RIM, rows), pl.ds(0, 256)], in_sem.at[2 * CH + n]))
    loads.append(pltpu.make_async_copy(coup_hbm, coup, in_sem.at[2 * CH + 2]))
    for copy in loads:
        copy.start()

    barrier = pltpu.get_barrier_semaphore()
    for k in range(1, nx):
        pl.semaphore_signal(barrier, 1, device_id=(lax.rem(gx + k, nx), gy), device_id_type=MESH)
    for k in range(1, ny):
        pl.semaphore_signal(barrier, 1, device_id=(gx, lax.rem(gy + k, ny)), device_id_type=MESH)
    kxv[...] = row_kx(gy * rows - RIM, total, rows * ny)
    for copy in loads:
        copy.wait()

    pl.semaphore_wait(barrier, nx + ny - 2)

    def strip(ref, src, dst, size, chan, sem, peer):
        return pltpu.make_async_remote_copy(
            ref.at[pl.ds(src, size), chan, pl.ds(0, 256)],
            ref.at[pl.ds(dst, size), chan, pl.ds(0, 256)],
            lat_send.at[sem], lat_recv.at[sem], device_id=(gx, peer), device_id_type=MESH)

    def breeze(src, dst, sem, peer):
        return pltpu.make_async_remote_copy(
            wind.at[:, pl.ds(src, 8), pl.ds(0, 256)], wind.at[:, pl.ds(dst, 8), pl.ds(0, 256)],
            lat_send.at[sem], lat_recv.at[sem], device_id=(gx, peer), device_id_type=MESH)

    vec, par = pl.ds(0, CH), pl.ds(CH, CH)
    to_s = [breeze(RIM, top, 4, south), strip(ext, RIM, top, RIM, vec, 0, south),
            strip(ext, RIM, top, RIM - 2, par, 1, south)]
    to_n = [breeze(rows, 0, 5, north), strip(ext, rows, 0, RIM, vec, 2, north),
            strip(ext, rows + 2, 2, RIM - 2, par, 3, north)]

    @pl.when(has_s)
    def _():
        for copy in to_s:
            copy.start()

    @pl.when(has_n)
    def _():
        for copy in to_n:
            copy.start()

    for missing, row, slot in ((no_s, 0, 0), (no_n, top, groups + 1)):
        @pl.when(missing)
        def _():
            ext[row : row + RIM, 0 : 2 * CH, 0:256] = jnp.zeros((RIM, 2 * CH, 256), F32)
            wind[:, row : row + RIM, 0:256] = jnp.zeros((2, RIM, 256), F32)
            lon[:, slot] = jnp.zeros((2, 40, 128), F32)

    def turn(value, by):
        by = by % 128
        return pltpu.roll(value, by, value.ndim - 1) if by else value

    lane32, lane8 = lanes((2 * CH, 128)), lanes((8, 128))

    @pl.loop(0, groups)
    def _(g):
        for side in range(2):
            shift, cut = (0, pl.ds(0, 128)) if side == 0 else (16, pl.ds(128, 128))
            out = jnp.zeros((2 * CH, 128), F32)
            for j in range(8):
                here = (lane32 >= 16 * j) & (lane32 < 16 * j + 16)
                out = jnp.where(here, turn(ext[RIM + 8 * g + j, :, cut], 16 * j + shift), out)
            pack[side, g, 0 : 2 * CH, :] = out
            at = pl.ds(pl.multiple_of(RIM + 8 * g, 8), 8)
            a = turn(wind[0, at, cut], shift)
            b = turn(wind[1, at, cut], 16 + shift)
            pack[side, g, 2 * CH :, :] = jnp.where(lane8 < 16, a, b)

    go_west = pltpu.make_async_remote_copy(
        pack.at[0], lon.at[0, pl.ds(1, groups)], lon_send.at[0], lon_recv.at[0],
        device_id=(west, gy), device_id_type=MESH)
    go_east = pltpu.make_async_remote_copy(
        pack.at[1], lon.at[1, pl.ds(1, groups)], lon_send.at[1], lon_recv.at[1],
        device_id=(east, gy), device_id_type=MESH)
    go_west.start()
    go_east.start()

    go_west.wait_recv()
    go_east.wait_recv()
    cor_s = pltpu.make_async_remote_copy(
        lon.at[:, 1], lon.at[:, groups + 1], cor_send.at[0], cor_recv.at[0],
        device_id=(gx, south), device_id_type=MESH)
    cor_n = pltpu.make_async_remote_copy(
        lon.at[:, groups], lon.at[:, 0], cor_send.at[1], cor_recv.at[1],
        device_id=(gx, north), device_id_type=MESH)

    @pl.when(has_s)
    def _():
        cor_s.start()

    @pl.when(has_n)
    def _():
        cor_n.start()

    two = 2.0 / HALF
    kind = lax.broadcasted_iota(jnp.int32, (8, 128), 0)
    by_kx = jnp.where(kind < 2, -two, 0.0)
    by_one = jnp.where((kind == 3) | (kind == 4), -0.5 * two, 0.0)
    eight = two * 8.0 / 12.0
    by_lon = jnp.where(kind == 0, eight, 0.0) + jnp.where(kind == 1, -eight, 0.0)
    by_lon = by_lon + jnp.where(kind == 2, -two / 12.0, 0.0)
    by_lat = jnp.where(kind == 3, eight, 0.0) + jnp.where(kind == 4, -eight, 0.0)
    by_lat = by_lat + jnp.where(kind == 5, -two / 12.0, 0.0)

    def merge(from_e, from_w):
        at = lanes(from_e.shape)
        return jnp.where(at < 16, from_e, jnp.where(at >= 112, from_w, 0.0))

    def prepare(g):
        at = pl.ds(pl.multiple_of(8 * g, 8), 8)
        for j in range(8):
            ext[8 * g + j, 0 : 2 * CH, 256:384] = merge(
                turn(lon[0, g, 0 : 2 * CH, :], -16 * j), turn(lon[1, g, 0 : 2 * CH, :], 112 - 16 * j))
        for n in range(2):
            wind[n, at, 256:384] = merge(
                turn(lon[0, g, 2 * CH :, :], -16 * n), turn(lon[1, g, 2 * CH :, :], 112 - 16 * n))
        kx8 = kxv[at, :]
        in8 = jnp.where(kx8 > 0.0, 1.0, 0.0)
        for t in range(3):
            cut = pl.ds(128 * t, 128)
            lon8, lat8 = wind[0, at, cut], wind[1, at, cut]
            for j in range(8):
                one = slice(j, j + 1)
                coef[8 * g + j, :, cut] = (
                    kx8[one] * by_kx + in8[one] * by_one + by_lon * lon8[one] + by_lat * lat8[one])
                diag = ext[8 * g + j, CH : 2 * CH, cut]
                gain, base = two * in8[one], (two * (2.0 - MID)) * in8[one] + (2.0 * two) * kx8[one]
                main[8 * g + j, :, cut] = diag * gain + base

    @pl.loop(1, groups + 1)
    def _(g):
        prepare(g)

    cm = coup[...] * (0.25 * two)
    cm = jnp.concatenate([jnp.concatenate([cm] * 4, axis=1)] * 4, axis=0)
    r4 = lax.broadcasted_iota(jnp.int32, (64, 64), 0) // 16
    c4 = lax.broadcasted_iota(jnp.int32, (64, 64), 1) // 16
    cm = jnp.where(r4 == c4, cm, 0.0)
    cm_hi = cm.astype(jnp.bfloat16)
    cm_lo = (cm - cm_hi.astype(F32)).astype(jnp.bfloat16)
    weights = jnp.concatenate([cm_hi, cm_hi, cm_lo], axis=1)

    def power(k):
        return ext.at[:, pl.ds(0, CH), :] if k == 0 else pwr[k - 1]

    lane4 = lanes((4, CH, 128))

    def couple(src, r0):
        mids = [src[pl.ds(r0, 4), :, 128 * t : 128 * t + 128] for t in range(3)]
        flat = jnp.concatenate([m.reshape(64, 128) for m in mids], axis=1)
        hi = flat.astype(jnp.bfloat16)
        lo = (flat - hi.astype(F32)).astype(jnp.bfloat16)
        return jnp.dot(weights, jnp.concatenate([hi, lo, hi], axis=0), preferred_element_type=F32)

    def stencil(k, r0, mixed):
        src, dst = power(k), power(k + 1)
        prev = power(k - 1) if k % BLOCK else None
        mids = [src[pl.ds(r0, 4), :, 128 * t : 128 * t + 128] for t in range(3)]
        for t in range(3):
            cut = pl.ds(128 * t, 128)
            mid, nxt, prv = mids[t], mids[(t + 1) % 3], mids[(t + 2) % 3]
            e1 = pltpu.roll(jnp.where(lane4 < 1, nxt, mid), 127, 2)
            e2 = pltpu.roll(jnp.where(lane4 < 2, nxt, mid), 126, 2)
            w1 = pltpu.roll(jnp.where(lane4 >= 127, prv, mid), 1, 2)
            w2 = pltpu.roll(jnp.where(lane4 >= 126, prv, mid), 2, 2)
            n1 = src[pl.ds(r0 + 1, 4), :, cut]
            n2 = src[pl.ds(r0 + 2, 4), :, cut]
            s1 = src[pl.ds(r0 - 1, 4), :, cut]
            s2 = src[pl.ds(r0 - 2, 4), :, cut]
            cs = [coef[pl.ds(r0, 4), i : i + 1, cut] for i in range(6)]
            out = main[pl.ds(r0, 4), :, cut] * mid
            out = out + mixed[:, 128 * t : 128 * t + 128].reshape(4, CH, 128)
            out = out + cs[0] * e1 + cs[1] * w1 + cs[2] * (e2 - w2)
            out = out + cs[3] * n1 + cs[4] * s1 + cs[5] * (n2 - s2)
            if prev is not None:
                out = out - prev[pl.ds(r0, 4), :, cut]
            dst[pl.ds(r0, 4), :, cut] = out

    def inner(k):
        m = k % BLOCK + 1
        for r0 in range(RIM + 2 * m, top - 2 * m, 4):
            stencil(k, r0, couple(power(k), r0))

    def outer(k):
        m = k % BLOCK + 1
        for r0 in (2 * m, 2 * m + 4, top - 2 * m, top - 2 * m + 4):
            stencil(k, r0, couple(power(k), r0))

    for k in range(BLOCK):
        inner(k)

    @pl.when(has_s)
    def _():
        for copy in to_s:
            copy.wait_send()
        cor_s.wait_send()
        for copy in to_n:
            copy.wait_recv()
        cor_n.wait_recv()

    @pl.when(has_n)
    def _():
        for copy in to_n:
            copy.wait_send()
        cor_n.wait_send()
        for copy in to_s:
            copy.wait_recv()
        cor_s.wait_recv()

    prepare(0)
    prepare(groups + 1)
    for k in range(BLOCK):
        outer(k)

    half = power(BLOCK)
    lane16 = lanes((CH, 128))
    for side, row in ((0, RIM), (1, rows)):
        out = jnp.zeros((CH, 128), F32)
        for j in range(8):
            here = (lane16 >= 16 * j) & (lane16 < 16 * j + 16)
            out = jnp.where(here, turn(half[row + j, :, 256:384], 16 * j + 8), out)
        made[side] = out

    def again(src, dst, sem, peer):
        return pltpu.make_async_remote_copy(
            half.at[pl.ds(src, RIM), :, pl.ds(0, 256)], half.at[pl.ds(dst, RIM), :, pl.ds(0, 256)],
            mid_send.at[sem], mid_recv.at[sem], device_id=(gx, peer), device_id_type=MESH)

    def also(src, dst, sem, peer):
        return pltpu.make_async_remote_copy(
            made.at[src], rims.at[dst], mid_send.at[sem], mid_recv.at[sem],
            device_id=(gx, peer), device_id_type=MESH)

    mid_s = [also(0, 1, 2, south), again(RIM, top, 0, south)]
    mid_n = [also(1, 0, 3, north), again(rows, 0, 1, north)]

    @pl.when(has_s)
    def _():
        for copy in mid_s:
            copy.start()

    @pl.when(has_n)
    def _():
        for copy in mid_n:
            copy.start()

    for missing, row, slot in ((no_s, 0, 0), (no_n, top, 1)):
        @pl.when(missing)
        def _():
            half[row : row + RIM, :, 0:256] = jnp.zeros((RIM, CH, 256), F32)
            rims[slot] = jnp.zeros((CH, 128), F32)

    for k in range(BLOCK, ITERS):
        inner(k)

    pairs = [(i, k) for i in range(9) for k in range(i, 9)]

    def gram(r, sums):
        for o in range(2):
            for t in range(2):
                at = (r, pl.ds(8 * o, 8), pl.ds(128 * t, 128))
                vals = [power(k)[at] for k in range(9)]
                sums = [s + vals[i] * vals[k] for s, (i, k) in zip(sums, pairs)]
        return tuple(sums)

    sums = tuple(jnp.zeros((8, 128), F32) for _ in pairs)
    sums = lax.fori_loop(2 * RIM, top - RIM, gram, sums)

    @pl.when(has_s)
    def _():
        for copy in mid_s:
            copy.wait_send()
        for copy in mid_n:
            copy.wait_recv()

    @pl.when(has_n)
    def _():
        for copy in mid_n:
            copy.wait_send()
        for copy in mid_s:
            copy.wait_recv()

    for side, row in ((0, 0), (1, top)):
        for j in range(8):
            half[row + j, :, 256:384] = turn(rims[side], -16 * j - 8)
    for k in range(BLOCK, ITERS):
        outer(k)
    sums = lax.fori_loop(RIM, 2 * RIM, gram, sums)
    sums = lax.fori_loop(top - RIM, top, gram, sums)

    sums = dict(zip(pairs, sums))
    folded = {p: jnp.sum(s, axis=0, keepdims=True) for p, s in sums.items()}
    sub8 = lax.broadcasted_iota(jnp.int32, (8, 128), 0)
    spread = jnp.zeros((8, 128), F32)
    for k in range(10):
        col = jnp.zeros((8, 128), F32)
        if k < 9:
            for i in range(8):
                col = jnp.where(sub8 == i, folded[min(i, k), max(i, k)], col)
        else:
            col = jnp.where(sub8 == 0, folded[8, 8], col)
        total_k = jnp.sum(col, axis=1, keepdims=True)
        spread = jnp.where(lane8 == 8 * k + sub8, total_k, spread)
    mine = jnp.sum(spread, axis=0, keepdims=True)

    def reduce_over(value, slots, send, recv, me, count, device):
        slots[me] = value
        copies = []
        for k in range(1, count):
            peer = lax.rem(me + k, count)
            copy = pltpu.make_async_remote_copy(
                slots.at[me], slots.at[me], send.at[k - 1], recv.at[me],
                device_id=device(peer), device_id_type=MESH)
            copy.start()
            copies.append(copy)
        for k in range(1, count):
            src = lax.rem(me + count - k, count)
            pltpu.make_async_remote_copy(
                slots.at[src], slots.at[src], send.at[k - 1], recv.at[src],
                device_id=device(src), device_id_type=MESH).wait_recv()
        parts = [slots[k] for k in range(count)]
        while len(parts) > 1:
            parts = [sum(parts[i : i + 2][1:], parts[i]) for i in range(0, len(parts), 2)]
        return parts[0], copies

    value, sent = reduce_over(mine, gx_slots, gxs_send, gxs_recv, gx, nx, lambda p: (p, gy))
    value, more = reduce_over(value, gy_slots, gys_send, gys_recv, gy, ny, lambda p: (gx, p))

    value = jnp.broadcast_to(value, (8, 128))
    picked = [jnp.where(lane8 == 8 * k + sub8, value, 0.0) for k in range(10)]
    upper = [jnp.broadcast_to(jnp.sum(p, axis=1, keepdims=True), (8, 128)) for p in picked]
    lower = [upper[8][k : k + 1, :] for k in range(8)] + [upper[9][0:1, :]]
    plain = [jnp.concatenate([u, jnp.where(sub8 == 0, w, 0.0)]) for u, w in zip(upper, lower)]
    sub = lax.broadcasted_iota(jnp.int32, (16, 128), 0)
    diag = jnp.zeros((16, 128), F32)
    for k in range(9):
        diag = jnp.where(sub == k, plain[k], diag)
    size = jnp.sqrt(diag)
    trial = trials()
    cols = [plain[k] + trial[k] * size * size[k : k + 1, :] for k in range(9)]
    q = gmres(cols)
    d = apply_a(q)
    q0 = jnp.broadcast_to(q[:, 0:1], (16, 128))
    d0 = jnp.broadcast_to(d[:, 0:1], (16, 128))
    left0 = jnp.where(sub == 0, 1.0, 0.0) - d0
    dq, dd = q - q0, d - d0
    bad_q = dot(dq, mat_vec(plain, dq, 8)) - TRUST**2 * dot(q0, mat_vec(plain, q0, 8))
    bad_d = dot(dd, mat_vec(plain, dd, 9)) - TRUST**2 * dot(left0, mat_vec(plain, left0, 9))
    fine = (bad_q <= 0.0) & (bad_d <= 0.0)
    flag[0, 0] = jnp.max(jnp.where(fine, 0.0, 1.0))

    qs = [q0[k : k + 1, :] for k in range(8)]
    ds = [left0[k : k + 1, :] for k in range(9)]

    @pl.loop(0, rows)
    def _(r):
        for t in range(2):
            cut = pl.ds(128 * t, 128)
            vals = [power(k)[r + RIM, :, cut] for k in range(9)]
            s = qs[0] * vals[0]
            e = ds[0] * vals[0]
            for k in range(1, 8):
                s = s + qs[k] * vals[k]
            for k in range(1, 9):
                e = e + ds[k] * vals[k]
            outs[0, r, :, cut] = s
            outs[1, r, :, cut] = e

    go_west.wait_send()
    go_east.wait_send()
    for copy in sent + more:
        copy.wait_send()


def unfold(outs, sol, res, sem):
    copies = []
    for c in range(CH):
        for n, dst in enumerate((sol, res)):
            copies.append(pltpu.make_async_copy(outs.at[n, :, c, :], dst.at[c], sem.at[n, c]))
    for copy in copies:
        copy.start()
    for copy in copies:
        copy.wait()


def fused(nx, ny, forcing, damping, wind_lon, wind_lat, coup):
    rows = forcing.shape[1]
    total = rows + 2 * RIM
    vm = pl.BlockSpec(memory_space=pltpu.VMEM)
    hbm = pl.BlockSpec(memory_space=pltpu.HBM)
    dma = pltpu.SemaphoreType.DMA
    outs, flag = pl.pallas_call(
        functools.partial(kernel, nx, ny),
        out_shape=(jax.ShapeDtypeStruct((2, rows, CH, 256), F32), jax.ShapeDtypeStruct((1, 1), F32)),
        in_specs=[hbm] * 5,
        out_specs=(vm, pl.BlockSpec(memory_space=pltpu.SMEM)),
        scratch_shapes=[pltpu.VMEM((total, CH, 384), F32)] * ITERS + [
            pltpu.VMEM((total, 2 * CH, 384), F32),
            pltpu.VMEM((total, 8, 384), F32),
            pltpu.VMEM((total, CH, 384), F32),
            pltpu.VMEM((2, total, 384), F32),
            pltpu.VMEM((2, total // 8, 40, 128), F32),
            pltpu.VMEM((2, rows // 8, 40, 128), F32),
            pltpu.VMEM((total, 128), F32),
            pltpu.VMEM((CH, CH), F32),
            pltpu.VMEM((2, CH, 128), F32),
            pltpu.VMEM((2, CH, 128), F32),
            pltpu.VMEM((nx, 1, 128), F32),
            pltpu.VMEM((ny, 1, 128), F32),
            dma((2 * CH + 3,)), dma((2,)), dma((2,)), dma((6,)), dma((6,)),
            dma((2,)), dma((2,)), dma((4,)), dma((4,)),
            dma((nx,)), dma((nx,)), dma((ny,)), dma((ny,)),
        ],
        compiler_params=pltpu.CompilerParams(
            collective_id=0, has_side_effects=True, vmem_limit_bytes=48 * 1024 * 1024),
        name="krylov",
    )(forcing, damping, wind_lon, wind_lat, coup)
    field = jax.ShapeDtypeStruct(forcing.shape, F32)
    sol, res = pl.pallas_call(
        unfold,
        out_shape=(field, field),
        in_specs=[vm],
        out_specs=(hbm, hbm),
        scratch_shapes=[dma((2, CH))],
        compiler_params=pltpu.CompilerParams(vmem_limit_bytes=8 * 1024 * 1024),
        name="unfold",
    )(outs)
    return sol, res, flag


def shifted(cells, axis, dim, closed, width):
    count = lax.axis_size(axis)
    ends = count if closed else count - 1
    head = lax.slice_in_dim(cells, 0, width, axis=dim)
    tail = lax.slice_in_dim(cells, cells.shape[dim] - width, cells.shape[dim], axis=dim)
    return jnp.concatenate(
        [
            lax.ppermute(tail, axis, [(i, (i + 1) % count) for i in range(ends)]),
            cells,
            lax.ppermute(head, axis, [((i + 1) % count, i) for i in range(ends)]),
        ],
        axis=dim,
    )


def apply_plain(vec, damping, coupling, wind_lon, wind_lat, kx):
    wide = shifted(vec, "gx", 2, True, 2)
    tall = shifted(vec, "gy", 1, False, 2)
    e1, w1, e2, w2 = wide[:, :, 3:-1], wide[:, :, 1:-3], wide[:, :, 4:], wide[:, :, :-4]
    n1, s1, n2, s2 = tall[:, 3:-1], tall[:, 1:-3], tall[:, 4:], tall[:, :-4]
    mixed = jnp.einsum("ij,jab->iab", coupling, vec, precision=lax.Precision.HIGHEST)
    return (
        (1.0 + damping) * vec + 0.25 * mixed
        + kx * (2.0 * vec - e1 - w1) + 0.5 * (2.0 * vec - n1 - s1)
        + wind_lon * ((8.0 * (e1 - w1) - (e2 - w2)) / 12.0)
        + wind_lat * ((8.0 * (n1 - s1) - (n2 - s2)) / 12.0)
    )


def careful(forcing, damping, coupling, wind_lon, wind_lat):
    rows = forcing.shape[1]
    pos = (lax.axis_index("gy") * rows + jnp.arange(rows)).astype(F32)
    phi = -math.pi / 2 + (pos + 0.5) * (math.pi / (rows * lax.axis_size("gy")))
    kx = (0.5 / (jnp.cos(phi) ** 2 + 0.1))[:, None]
    operate = lambda v: apply_plain(v, damping, coupling, wind_lon, wind_lat, kx)
    every = ("gx", "gy")
    first = jnp.sqrt(lax.psum(jnp.sum(forcing * forcing), every) + 1.0)
    basis = jnp.zeros((ITERS,) + forcing.shape, F32).at[0].set(forcing / first)
    heights = jnp.zeros((ITERS + 1, ITERS), F32)

    def body(j, state):
        basis, heights = state
        w = operate(lax.dynamic_index_in_dim(basis, j, 0, keepdims=False))
        h = lax.psum(jnp.sum(basis * w[None], axis=(1, 2, 3)), every)
        w = w - jnp.sum(h[:, None, None, None] * basis, axis=0)
        below = jnp.sqrt(lax.psum(jnp.sum(w * w), every) + 1.0)
        col = jnp.concatenate([h, jnp.zeros((1,), F32)])
        col = jnp.where(jnp.arange(ITERS + 1) == j + 1, below, col)
        heights = lax.dynamic_update_slice(heights, col[:, None], (0, j))
        old = lax.dynamic_index_in_dim(basis, jnp.minimum(j + 1, ITERS - 1), 0, keepdims=False)
        new = jnp.where(j + 1 < ITERS, w / below, old)
        basis = lax.dynamic_update_index_in_dim(basis, new, jnp.minimum(j + 1, ITERS - 1), 0)
        return basis, heights

    basis, heights = lax.fori_loop(0, ITERS, body, (basis, heights))
    h = [[heights[i, j] for j in range(ITERS)] for i in range(ITERS + 1)]
    target = [first] + [jnp.zeros((), F32)] * ITERS
    turns = []
    for j in range(ITERS):
        for i in range(j):
            c, s = turns[i]
            h[i][j], h[i + 1][j] = c * h[i][j] + s * h[i + 1][j], c * h[i + 1][j] - s * h[i][j]
        radius = jnp.sqrt(h[j][j] * h[j][j] + h[j + 1][j] * h[j + 1][j])
        c, s = h[j][j] / radius, h[j + 1][j] / radius
        turns.append((c, s))
        h[j][j] = radius
        target[j], target[j + 1] = c * target[j] + s * target[j + 1], c * target[j + 1] - s * target[j]
    y = [None] * ITERS
    for j in reversed(range(ITERS)):
        part = target[j]
        for i in range(j + 1, ITERS):
            part = part - h[j][i] * y[i]
        y[j] = part / h[j][j]
    weights = jnp.stack(y)
    answer = jnp.sum(weights[:, None, None, None] * basis, axis=0)
    return answer, forcing - operate(answer)


def per_device(nx, ny, forcing, damping, coupling, wind_lon, wind_lat):
    sol, res, flag = fused(nx, ny, forcing, damping, wind_lon, wind_lat, coupling)

    pin = lambda x: with_layout_constraint(x, Layout(tuple(range(x.ndim))))

    def again(state):
        sol, res = careful(pin(forcing), pin(damping), coupling, wind_lon, wind_lat)
        return pin(sol), pin(res), jnp.zeros((), F32)

    done = lax.while_loop(lambda state: state[2] > 0.5, again, (sol, res, flag[0, 0]))
    return pin(done[0]), pin(done[1])


def solution(mesh):
    nx, ny = mesh.shape["gx"], mesh.shape["gy"]
    in_specs = (P(None, "gy", "gx"), P(None, "gy", "gx"), P(), P("gy", "gx"), P("gy", "gx"))
    out_specs = (P(None, "gy", "gx"), P(None, "gy", "gx"))
    return jax.shard_map(
        functools.partial(per_device, nx, ny),
        mesh=mesh, in_specs=in_specs, out_specs=out_specs, check_vma=False,
    )
```

```python
import functools
import math

import jax
import jax.numpy as jnp
import numpy as np
from jax import lax
from jax.experimental import pallas as pl
from jax.experimental.pallas import tpu as pltpu
from jax.experimental.layout import Layout, with_layout_constraint
from jax.sharding import PartitionSpec as P

ITERS = 8
CH = 16
RIM = 8
LOW, HIGH = 1.0, 16.0
MID, HALF = (LOW + HIGH) / 2, (HIGH - LOW) / 2
BLOCK = 4
NOISE = 1.2e-7
TRUST = 1.0e-4
MESH = pl.DeviceIdType.MESH
F32 = jnp.float32


def trials():
    sub = lax.broadcasted_iota(jnp.int32, (16, 128), 0)
    lane = lanes((16, 128))
    tables = []
    for k in range(9):
        pair = jnp.minimum(sub, k) * 16 + jnp.maximum(sub, k)
        bits = pair * 1640531527 + lane * 668265263
        bits = (bits ^ lax.shift_right_logical(bits, 15)) * 739982445
        bits = bits ^ lax.shift_right_logical(bits, 13)
        sign = jnp.where((bits & 64) == 0, NOISE, -NOISE)
        tables.append(jnp.where((lane == 0) | (sub > 8), 0.0, sign))
    return tables


def row_kx(first, count, lat_total):
    row = (first + lax.broadcasted_iota(jnp.int32, (count, 128), 0)).astype(F32)
    phi = -math.pi / 2 + (row + 0.5) * (math.pi / lat_total)
    inside = (row >= 0.0) & (row < lat_total)
    cos = jnp.cos(phi)
    return jnp.where(inside, 0.5 / (cos * cos + 0.1), 0.0)


def lanes(shape):
    return lax.broadcasted_iota(jnp.int32, shape, len(shape) - 1)


def apply_a(vec):
    sub = lax.broadcasted_iota(jnp.int32, vec.shape, 0)
    up = pltpu.roll(vec, 1, 0)
    kept = jnp.where((sub == 0) | (sub == BLOCK), 0.0, vec)
    down = pltpu.roll(kept, 15, 0)
    return MID * vec + (HALF / 2) * (up + down)


def mat_vec(cols, vec, count):
    total = cols[0] * vec[0:1, :]
    for k in range(1, count):
        total = total + cols[k] * vec[k : k + 1, :]
    return total


def dot(a, b):
    return jnp.sum(a * b, axis=0, keepdims=True)


def gmres(cols):
    sub = lax.broadcasted_iota(jnp.int32, (16, 128), 0)
    first = jnp.sqrt(cols[0][0:1, :] + 1.0)
    basis = [jnp.where(sub == 0, 1.0, 0.0) / first]
    target = first
    targets = []
    columns = []
    turns = []
    for j in range(ITERS):
        w = apply_a(basis[j])
        u = mat_vec(cols, w, j + 2)
        h = [dot(v, u) for v in basis]
        for i in range(j + 1):
            w = w - h[i] * basis[i]
        norm = dot(w, mat_vec(cols, w, j + 2))
        below = jnp.sqrt(jnp.maximum(norm, 0.0) + 1.0)
        if j + 1 < ITERS:
            basis.append(w / below)
        col = list(h)
        for i, (c, s) in enumerate(turns):
            if i + 1 <= j:
                col[i], col[i + 1] = c * col[i] + s * col[i + 1], c * col[i + 1] - s * col[i]
        radius = jnp.sqrt(col[j] * col[j] + below * below)
        inv = 1.0 / radius
        c, s = col[j] * inv, below * inv
        turns.append((c, s))
        col[j] = radius
        columns.append((col, inv))
        targets.append(c * target)
        target = -s * target
    y = [None] * ITERS
    for j in reversed(range(ITERS)):
        y[j] = targets[j] * columns[j][1]
        for i in range(j):
            targets[i] = targets[i] - columns[j][0][i] * y[j]
    q = basis[0] * y[0]
    for j in range(1, ITERS):
        q = q + basis[j] * y[j]
    return q


def kernel(
    nx, ny, forc, damp, wlon, wlat, coup_hbm, outs, flag,
    *scratch,
):
    pwr, scratch = scratch[:ITERS], scratch[ITERS:]
    (ext, coef, main, wind, lon, pack, kxv, coup, made, rims, gx_slots, gy_slots,
     in_sem, lon_send, lon_recv, lat_send, lat_recv, cor_send, cor_recv,
     mid_send, mid_recv, gxs_send, gxs_recv, gys_send, gys_recv) = scratch
    gx, gy = lax.axis_index("gx"), lax.axis_index("gy")
    rows = forc.shape[1]
    top = RIM + rows
    total = rows + 2 * RIM
    groups = rows // 8
    east, west = lax.rem(gx + 1, nx), lax.rem(gx + nx - 1, nx)
    north, south = gy + 1, gy - 1
    has_n, has_s = gy < ny - 1, gy > 0
    no_n, no_s = jnp.logical_not(has_n), jnp.logical_not(has_s)

    core, place = lax.rem(gx, 2), gx // 2
    half_x = nx // 2
    team = half_x * ny
    hops = [(a, b) for a in range(half_x) for b in range(ny) if (a, b) != (0, 0)]
    hops.sort(key=lambda h: min(h[0], half_x - h[0]) + min(h[1], ny - h[1]))

    def mate(a, b):
        return (2 * lax.rem(place + a, half_x) + core, lax.rem(gy + b, ny))

    barrier = pltpu.get_barrier_semaphore()
    for peer in [(east, gy), (west, gy)] + [mate(a, b) for a, b in hops]:
        pl.semaphore_signal(barrier, 1, device_id=peer, device_id_type=MESH)

    loads = []
    for c in range(CH):
        for n, src in enumerate((forc, damp)):
            loads.append(pltpu.make_async_copy(
                src.at[c], ext.at[pl.ds(RIM, rows), CH * n + c, pl.ds(0, 256)],
                in_sem.at[CH * n + c]))
    for n, src in enumerate((wlon, wlat)):
        loads.append(pltpu.make_async_copy(
            src, wind.at[n, pl.ds(RIM, rows), pl.ds(0, 256)], in_sem.at[2 * CH + n]))
    loads.append(pltpu.make_async_copy(coup_hbm, coup, in_sem.at[2 * CH + 2]))
    for copy in loads:
        copy.start()

    kxv[...] = row_kx(gy * rows - RIM, total, rows * ny)
    for copy in loads:
        copy.wait()

    pl.semaphore_wait(barrier, team + 1)

    def strip(ref, src, dst, size, chan, sem, peer):
        return pltpu.make_async_remote_copy(
            ref.at[pl.ds(src, size), chan, pl.ds(0, 256)],
            ref.at[pl.ds(dst, size), chan, pl.ds(0, 256)],
            lat_send.at[sem], lat_recv.at[sem], device_id=(gx, peer), device_id_type=MESH)

    def breeze(src, dst, sem, peer):
        return pltpu.make_async_remote_copy(
            wind.at[:, pl.ds(src, 8), pl.ds(0, 256)], wind.at[:, pl.ds(dst, 8), pl.ds(0, 256)],
            lat_send.at[sem], lat_recv.at[sem], device_id=(gx, peer), device_id_type=MESH)

    vec, par = pl.ds(0, CH), pl.ds(CH, CH)
    near_s = [breeze(RIM, top, 0, south), strip(ext, RIM, top, 4, vec, 1, south),
              strip(ext, RIM, top, 4, par, 2, south)]
    far_s = [strip(ext, RIM + 4, top + 4, 4, vec, 3, south),
             strip(ext, RIM + 4, top + 4, 2, par, 4, south)]
    near_n = [breeze(rows, 0, 5, north), strip(ext, rows + 4, 4, 4, vec, 6, north),
              strip(ext, rows + 4, 4, 4, par, 7, north)]
    far_n = [strip(ext, rows, 0, 4, vec, 8, north), strip(ext, rows + 2, 2, 2, par, 9, north)]
    to_s, to_n = near_s + far_s, near_n + far_n

    def await_strips(from_s, from_n):
        @pl.when(has_s)
        def _():
            for copy in from_s:
                copy.wait_recv()

        @pl.when(has_n)
        def _():
            for copy in from_n:
                copy.wait_recv()

    def await_sent(gone_s, gone_n):
        @pl.when(has_s)
        def _():
            for copy in gone_s:
                copy.wait_send()

        @pl.when(has_n)
        def _():
            for copy in gone_n:
                copy.wait_send()

    @pl.when(has_s)
    def _():
        for copy in to_s:
            copy.start()

    @pl.when(has_n)
    def _():
        for copy in to_n:
            copy.start()

    for missing, row, slot in ((no_s, 0, 0), (no_n, top, groups + 1)):
        @pl.when(missing)
        def _():
            ext[row : row + RIM, 0 : 2 * CH, 0:256] = jnp.zeros((RIM, 2 * CH, 256), F32)
            wind[:, row : row + RIM, 0:256] = jnp.zeros((2, RIM, 256), F32)
            lon[:, slot] = jnp.zeros((2, 40, 128), F32)

    def turn(value, by):
        by = by % 128
        return pltpu.roll(value, by, value.ndim - 1) if by else value

    lane32, lane8 = lanes((2 * CH, 128)), lanes((8, 128))

    @pl.loop(0, groups)
    def _(g):
        for side in range(2):
            shift, cut = (0, pl.ds(0, 128)) if side == 0 else (16, pl.ds(128, 128))
            out = jnp.zeros((2 * CH, 128), F32)
            for j in range(8):
                here = (lane32 >= 16 * j) & (lane32 < 16 * j + 16)
                out = jnp.where(here, turn(ext[RIM + 8 * g + j, :, cut], 16 * j + shift), out)
            pack[side, g, 0 : 2 * CH, :] = out
            at = pl.ds(pl.multiple_of(RIM + 8 * g, 8), 8)
            a = turn(wind[0, at, cut], shift)
            b = turn(wind[1, at, cut], 16 + shift)
            pack[side, g, 2 * CH :, :] = jnp.where(lane8 < 16, a, b)

    go_west = pltpu.make_async_remote_copy(
        pack.at[0], lon.at[0, pl.ds(1, groups)], lon_send.at[0], lon_recv.at[0],
        device_id=(west, gy), device_id_type=MESH)
    go_east = pltpu.make_async_remote_copy(
        pack.at[1], lon.at[1, pl.ds(1, groups)], lon_send.at[1], lon_recv.at[1],
        device_id=(east, gy), device_id_type=MESH)
    go_west.start()
    go_east.start()

    go_west.wait_recv()
    go_east.wait_recv()
    cor_s = pltpu.make_async_remote_copy(
        lon.at[:, 1], lon.at[:, groups + 1], cor_send.at[0], cor_recv.at[0],
        device_id=(gx, south), device_id_type=MESH)
    cor_n = pltpu.make_async_remote_copy(
        lon.at[:, groups], lon.at[:, 0], cor_send.at[1], cor_recv.at[1],
        device_id=(gx, north), device_id_type=MESH)

    @pl.when(has_s)
    def _():
        cor_s.start()

    @pl.when(has_n)
    def _():
        cor_n.start()

    two = 2.0 / HALF
    kind = lax.broadcasted_iota(jnp.int32, (8, 128), 0)
    by_kx = jnp.where(kind < 2, -two, 0.0)
    by_one = jnp.where((kind == 3) | (kind == 4), -0.5 * two, 0.0)
    eight = two * 8.0 / 12.0
    by_lon = jnp.where(kind == 0, eight, 0.0) + jnp.where(kind == 1, -eight, 0.0)
    by_lon = by_lon + jnp.where(kind == 2, -two / 12.0, 0.0)
    by_lat = jnp.where(kind == 3, eight, 0.0) + jnp.where(kind == 4, -eight, 0.0)
    by_lat = by_lat + jnp.where(kind == 5, -two / 12.0, 0.0)

    def merge(from_e, from_w):
        at = lanes(from_e.shape)
        return jnp.where(at < 16, from_e, jnp.where(at >= 112, from_w, 0.0))

    def third(g):
        at = pl.ds(pl.multiple_of(8 * g, 8), 8)
        for j in range(8):
            ext[8 * g + j, 0 : 2 * CH, 256:384] = merge(
                turn(lon[0, g, 0 : 2 * CH, :], -16 * j), turn(lon[1, g, 0 : 2 * CH, :], 112 - 16 * j))
        for n in range(2):
            wind[n, at, 256:384] = merge(
                turn(lon[0, g, 2 * CH :, :], -16 * n), turn(lon[1, g, 2 * CH :, :], 112 - 16 * n))

    def prepare(g, some=range(8)):
        at = pl.ds(pl.multiple_of(8 * g, 8), 8)
        kx8 = kxv[at, :]
        in8 = jnp.where(kx8 > 0.0, 1.0, 0.0)
        for t in range(3):
            cut = pl.ds(128 * t, 128)
            lon8, lat8 = wind[0, at, cut], wind[1, at, cut]
            for j in some:
                one = slice(j, j + 1)
                coef[8 * g + j, :, cut] = (
                    kx8[one] * by_kx + in8[one] * by_one + by_lon * lon8[one] + by_lat * lat8[one])
                diag = ext[8 * g + j, CH : 2 * CH, cut]
                gain, base = two * in8[one], (two * (2.0 - MID)) * in8[one] + (2.0 * two) * kx8[one]
                main[8 * g + j, :, cut] = diag * gain + base

    @pl.loop(1, groups + 1)
    def _(g):
        third(g)
        prepare(g)

    cm = coup[...] * (0.25 * two)
    cm = jnp.concatenate([jnp.concatenate([cm] * 4, axis=1)] * 4, axis=0)
    r4 = lax.broadcasted_iota(jnp.int32, (64, 64), 0) // 16
    c4 = lax.broadcasted_iota(jnp.int32, (64, 64), 1) // 16
    cm = jnp.where(r4 == c4, cm, 0.0)
    cm_hi = cm.astype(jnp.bfloat16)
    cm_lo = (cm - cm_hi.astype(F32)).astype(jnp.bfloat16)
    weights = jnp.concatenate([cm_hi, cm_hi, cm_lo], axis=1)

    def power(k):
        return ext.at[:, pl.ds(0, CH), :] if k == 0 else pwr[k - 1]

    lane4 = lanes((4, CH, 128))

    def couple(src, r0):
        mids = [src[pl.ds(r0, 4), :, 128 * t : 128 * t + 128] for t in range(3)]
        flat = jnp.concatenate([m.reshape(64, 128) for m in mids], axis=1)
        hi = flat.astype(jnp.bfloat16)
        lo = (flat - hi.astype(F32)).astype(jnp.bfloat16)
        return jnp.dot(weights, jnp.concatenate([hi, lo, hi], axis=0), preferred_element_type=F32)

    def stencil(k, r0, mixed):
        src, dst = power(k), power(k + 1)
        prev = power(k - 1) if k % BLOCK else None
        mids = [src[pl.ds(r0, 4), :, 128 * t : 128 * t + 128] for t in range(3)]
        for t in range(3):
            cut = pl.ds(128 * t, 128)
            mid, nxt, prv = mids[t], mids[(t + 1) % 3], mids[(t + 2) % 3]
            e1 = pltpu.roll(jnp.where(lane4 < 1, nxt, mid), 127, 2)
            e2 = pltpu.roll(jnp.where(lane4 < 2, nxt, mid), 126, 2)
            w1 = pltpu.roll(jnp.where(lane4 >= 127, prv, mid), 1, 2)
            w2 = pltpu.roll(jnp.where(lane4 >= 126, prv, mid), 2, 2)
            n1 = src[pl.ds(r0 + 1, 4), :, cut]
            n2 = src[pl.ds(r0 + 2, 4), :, cut]
            s1 = src[pl.ds(r0 - 1, 4), :, cut]
            s2 = src[pl.ds(r0 - 2, 4), :, cut]
            cs = [coef[pl.ds(r0, 4), i : i + 1, cut] for i in range(6)]
            out = main[pl.ds(r0, 4), :, cut] * mid
            out = out + mixed[:, 128 * t : 128 * t + 128].reshape(4, CH, 128)
            out = out + cs[0] * e1 + cs[1] * w1 + cs[2] * (e2 - w2)
            out = out + cs[3] * n1 + cs[4] * s1 + cs[5] * (n2 - s2)
            if prev is not None:
                out = out - prev[pl.ds(r0, 4), :, cut]
            dst[pl.ds(r0, 4), :, cut] = out

    def inner(k):
        m = k % BLOCK + 1
        for r0 in range(RIM + 2 * m, top - 2 * m, 4):
            stencil(k, r0, couple(power(k), r0))

    def outer(k, far):
        m = k % BLOCK + 1
        for r0 in ((2 * m, top - 2 * m + 4) if far else (2 * m + 4, top - 2 * m)):
            stencil(k, r0, couple(power(k), r0))

    for k in range(BLOCK):
        inner(k)

    await_strips(near_n + [cor_n], near_s + [cor_s])
    third(0)
    third(groups + 1)
    prepare(0, range(4, 8))
    prepare(groups + 1, range(4))
    for k in range(BLOCK):
        outer(k, False)
    await_strips(far_n, far_s)
    prepare(0, range(2, 4))
    prepare(groups + 1, range(4, 6))
    for k in range(BLOCK):
        outer(k, True)

    half = power(BLOCK)
    lane16 = lanes((CH, 128))
    for side, row in ((0, RIM), (1, rows)):
        out = jnp.zeros((CH, 128), F32)
        for j in range(8):
            here = (lane16 >= 16 * j) & (lane16 < 16 * j + 16)
            out = jnp.where(here, turn(half[row + j, :, 256:384], 16 * j + 8), out)
        made[side] = out

    def again(src, dst, sem, peer):
        return pltpu.make_async_remote_copy(
            half.at[pl.ds(src, 4), :, pl.ds(0, 256)], half.at[pl.ds(dst, 4), :, pl.ds(0, 256)],
            mid_send.at[sem], mid_recv.at[sem], device_id=(gx, peer), device_id_type=MESH)

    def also(src, dst, sem, peer):
        return pltpu.make_async_remote_copy(
            made.at[src], rims.at[dst], mid_send.at[sem], mid_recv.at[sem],
            device_id=(gx, peer), device_id_type=MESH)

    near_s = [also(0, 1, 0, south), again(RIM, top, 1, south)]
    far_s2 = [again(RIM + 4, top + 4, 2, south)]
    near_n = [also(1, 0, 3, north), again(rows + 4, 4, 4, north)]
    far_n2 = [again(rows, 0, 5, north)]
    mid_s, mid_n = near_s + far_s2, near_n + far_n2

    @pl.when(has_s)
    def _():
        for copy in mid_s:
            copy.start()

    @pl.when(has_n)
    def _():
        for copy in mid_n:
            copy.start()

    for missing, row, slot in ((no_s, 0, 0), (no_n, top, 1)):
        @pl.when(missing)
        def _():
            half[row : row + RIM, :, 0:256] = jnp.zeros((RIM, CH, 256), F32)
            rims[slot] = jnp.zeros((CH, 128), F32)

    for k in range(BLOCK, ITERS):
        inner(k)

    pairs = [(i, k) for i in range(9) for k in range(i, 9)]

    def gram(r, sums):
        for o in range(2):
            for t in range(2):
                at = (r, pl.ds(8 * o, 8), pl.ds(128 * t, 128))
                vals = [power(k)[at] for k in range(9)]
                sums = [s + vals[i] * vals[k] for s, (i, k) in zip(sums, pairs)]
        return tuple(sums)

    sums = tuple(jnp.zeros((8, 128), F32) for _ in pairs)
    sums = lax.fori_loop(2 * RIM, top - RIM, gram, sums)
    await_strips(near_n, near_s)
    for side, row in ((0, 0), (1, top)):
        for j in range(8):
            half[row + j, :, 256:384] = turn(rims[side], -16 * j - 8)
    for k in range(BLOCK, ITERS):
        outer(k, False)
    sums = lax.fori_loop(
        0, 8, lambda g, acc: gram(RIM + 4 + g + (rows - 16) * (g // 4), acc), sums)
    await_strips(far_n2, far_s2)
    for k in range(BLOCK, ITERS):
        outer(k, True)
    sums = lax.fori_loop(0, 8, lambda g, acc: gram(RIM + g + (rows - 8) * (g // 4), acc), sums)

    sums = dict(zip(pairs, sums))
    folded = {p: jnp.sum(s, axis=0, keepdims=True) for p, s in sums.items()}
    sub8 = lax.broadcasted_iota(jnp.int32, (8, 128), 0)
    spread = jnp.zeros((8, 128), F32)
    for k in range(10):
        col = jnp.zeros((8, 128), F32)
        if k < 9:
            for i in range(8):
                col = jnp.where(sub8 == i, folded[min(i, k), max(i, k)], col)
        else:
            col = jnp.where(sub8 == 0, folded[8, 8], col)
        total_k = jnp.sum(col, axis=1, keepdims=True)
        spread = jnp.where(lane8 == 8 * k + sub8, total_k, spread)
    mine = jnp.sum(spread, axis=0, keepdims=True)

    me = place * ny + gy
    gx_slots[me] = mine
    for a, b in hops:
        copy = pltpu.make_async_remote_copy(
            gx_slots.at[me], gx_slots.at[me], gxs_send, gxs_recv,
            device_id=mate(a, b), device_id_type=MESH)
        copy.start()
    rest = pl.ds(0, team - 1)
    every = pltpu.make_async_remote_copy(
        gx_slots.at[rest], gx_slots.at[rest], gxs_send, gxs_recv,
        device_id=(east, gy), device_id_type=MESH)
    every.wait_recv()
    parts = [gx_slots[k] for k in range(team)]
    while len(parts) > 1:
        parts = [sum(parts[i : i + 2][1:], parts[i]) for i in range(0, len(parts), 2)]
    gy_slots[core] = parts[0]
    partner = gx + 1 - 2 * core
    pair = pltpu.make_async_remote_copy(
        gy_slots.at[core], gy_slots.at[core], gys_send, gys_recv,
        device_id=(partner, gy), device_id_type=MESH)
    pair.start()
    pair.wait_recv()
    value = gy_slots[0] + gy_slots[1]

    value = jnp.broadcast_to(value, (8, 128))
    picked = [jnp.where(lane8 == 8 * k + sub8, value, 0.0) for k in range(10)]
    upper = [jnp.broadcast_to(jnp.sum(p, axis=1, keepdims=True), (8, 128)) for p in picked]
    lower = [upper[8][k : k + 1, :] for k in range(8)] + [upper[9][0:1, :]]
    plain = [jnp.concatenate([u, jnp.where(sub8 == 0, w, 0.0)]) for u, w in zip(upper, lower)]
    sub = lax.broadcasted_iota(jnp.int32, (16, 128), 0)
    diag = jnp.zeros((16, 128), F32)
    for k in range(9):
        diag = jnp.where(sub == k, plain[k], diag)
    size = jnp.sqrt(diag)
    trial = trials()
    cols = [plain[k] + trial[k] * size * size[k : k + 1, :] for k in range(9)]
    q = gmres(cols)
    d = apply_a(q)
    q0 = jnp.broadcast_to(q[:, 0:1], (16, 128))
    d0 = jnp.broadcast_to(d[:, 0:1], (16, 128))
    left0 = jnp.where(sub == 0, 1.0, 0.0) - d0
    dq, dd = q - q0, d - d0
    bad_q = dot(dq, mat_vec(plain, dq, 8)) - TRUST**2 * dot(q0, mat_vec(plain, q0, 8))
    bad_d = dot(dd, mat_vec(plain, dd, 9)) - TRUST**2 * dot(left0, mat_vec(plain, left0, 9))
    fine = (bad_q <= 0.0) & (bad_d <= 0.0)
    flag[0, 0] = jnp.max(jnp.where(fine, 0.0, 1.0))

    qs = [q0[k : k + 1, :] for k in range(8)]
    ds = [left0[k : k + 1, :] for k in range(9)]

    @pl.loop(0, rows)
    def _(r):
        for t in range(2):
            cut = pl.ds(128 * t, 128)
            vals = [power(k)[r + RIM, :, cut] for k in range(9)]
            s = qs[0] * vals[0]
            e = ds[0] * vals[0]
            for k in range(1, 8):
                s = s + qs[k] * vals[k]
            for k in range(1, 9):
                e = e + ds[k] * vals[k]
            outs[0, r, :, cut] = s
            outs[1, r, :, cut] = e

    go_west.wait_send()
    go_east.wait_send()
    await_sent(to_s + [cor_s] + mid_s, to_n + [cor_n] + mid_n)
    every.wait_send()
    pair.wait_send()


def unfold(outs, sol, res, sem):
    copies = []
    for c in range(CH):
        for n, dst in enumerate((sol, res)):
            copies.append(pltpu.make_async_copy(outs.at[n, :, c, :], dst.at[c], sem.at[n, c]))
    for copy in copies:
        copy.start()
    for copy in copies:
        copy.wait()


def fused(nx, ny, forcing, damping, wind_lon, wind_lat, coup):
    rows = forcing.shape[1]
    total = rows + 2 * RIM
    vm = pl.BlockSpec(memory_space=pltpu.VMEM)
    hbm = pl.BlockSpec(memory_space=pltpu.HBM)
    dma = pltpu.SemaphoreType.DMA
    outs, flag = pl.pallas_call(
        functools.partial(kernel, nx, ny),
        out_shape=(jax.ShapeDtypeStruct((2, rows, CH, 256), F32), jax.ShapeDtypeStruct((1, 1), F32)),
        in_specs=[hbm] * 5,
        out_specs=(vm, pl.BlockSpec(memory_space=pltpu.SMEM)),
        scratch_shapes=[pltpu.VMEM((total, CH, 384), F32)] * ITERS + [
            pltpu.VMEM((total, 2 * CH, 384), F32),
            pltpu.VMEM((total, 8, 384), F32),
            pltpu.VMEM((total, CH, 384), F32),
            pltpu.VMEM((2, total, 384), F32),
            pltpu.VMEM((2, total // 8, 40, 128), F32),
            pltpu.VMEM((2, rows // 8, 40, 128), F32),
            pltpu.VMEM((total, 128), F32),
            pltpu.VMEM((CH, CH), F32),
            pltpu.VMEM((2, CH, 128), F32),
            pltpu.VMEM((2, CH, 128), F32),
            pltpu.VMEM((nx // 2 * ny, 1, 128), F32),
            pltpu.VMEM((2, 1, 128), F32),
            dma((2 * CH + 3,)), dma((2,)), dma((2,)), dma((10,)), dma((10,)),
            dma((2,)), dma((2,)), dma((6,)), dma((6,)), dma, dma, dma, dma,
        ],
        compiler_params=pltpu.CompilerParams(
            collective_id=0, has_side_effects=True, vmem_limit_bytes=48 * 1024 * 1024),
        name="krylov",
    )(forcing, damping, wind_lon, wind_lat, coup)
    field = jax.ShapeDtypeStruct(forcing.shape, F32)
    sol, res = pl.pallas_call(
        unfold,
        out_shape=(field, field),
        in_specs=[vm],
        out_specs=(hbm, hbm),
        scratch_shapes=[dma((2, CH))],
        compiler_params=pltpu.CompilerParams(vmem_limit_bytes=8 * 1024 * 1024),
        name="unfold",
    )(outs)
    return sol, res, flag


def shifted(cells, axis, dim, closed, width):
    count = lax.axis_size(axis)
    ends = count if closed else count - 1
    head = lax.slice_in_dim(cells, 0, width, axis=dim)
    tail = lax.slice_in_dim(cells, cells.shape[dim] - width, cells.shape[dim], axis=dim)
    return jnp.concatenate(
        [
            lax.ppermute(tail, axis, [(i, (i + 1) % count) for i in range(ends)]),
            cells,
            lax.ppermute(head, axis, [((i + 1) % count, i) for i in range(ends)]),
        ],
        axis=dim,
    )


def apply_plain(vec, damping, coupling, wind_lon, wind_lat, kx):
    wide = shifted(vec, "gx", 2, True, 2)
    tall = shifted(vec, "gy", 1, False, 2)
    e1, w1, e2, w2 = wide[:, :, 3:-1], wide[:, :, 1:-3], wide[:, :, 4:], wide[:, :, :-4]
    n1, s1, n2, s2 = tall[:, 3:-1], tall[:, 1:-3], tall[:, 4:], tall[:, :-4]
    mixed = jnp.einsum("ij,jab->iab", coupling, vec, precision=lax.Precision.HIGHEST)
    return (
        (1.0 + damping) * vec + 0.25 * mixed
        + kx * (2.0 * vec - e1 - w1) + 0.5 * (2.0 * vec - n1 - s1)
        + wind_lon * ((8.0 * (e1 - w1) - (e2 - w2)) / 12.0)
        + wind_lat * ((8.0 * (n1 - s1) - (n2 - s2)) / 12.0)
    )


def careful(forcing, damping, coupling, wind_lon, wind_lat):
    rows = forcing.shape[1]
    pos = (lax.axis_index("gy") * rows + jnp.arange(rows)).astype(F32)
    phi = -math.pi / 2 + (pos + 0.5) * (math.pi / (rows * lax.axis_size("gy")))
    kx = (0.5 / (jnp.cos(phi) ** 2 + 0.1))[:, None]
    operate = lambda v: apply_plain(v, damping, coupling, wind_lon, wind_lat, kx)
    every = ("gx", "gy")
    first = jnp.sqrt(lax.psum(jnp.sum(forcing * forcing), every) + 1.0)
    basis = jnp.zeros((ITERS,) + forcing.shape, F32).at[0].set(forcing / first)
    heights = jnp.zeros((ITERS + 1, ITERS), F32)

    def body(j, state):
        basis, heights = state
        w = operate(lax.dynamic_index_in_dim(basis, j, 0, keepdims=False))
        h = lax.psum(jnp.sum(basis * w[None], axis=(1, 2, 3)), every)
        w = w - jnp.sum(h[:, None, None, None] * basis, axis=0)
        below = jnp.sqrt(lax.psum(jnp.sum(w * w), every) + 1.0)
        col = jnp.concatenate([h, jnp.zeros((1,), F32)])
        col = jnp.where(jnp.arange(ITERS + 1) == j + 1, below, col)
        heights = lax.dynamic_update_slice(heights, col[:, None], (0, j))
        old = lax.dynamic_index_in_dim(basis, jnp.minimum(j + 1, ITERS - 1), 0, keepdims=False)
        new = jnp.where(j + 1 < ITERS, w / below, old)
        basis = lax.dynamic_update_index_in_dim(basis, new, jnp.minimum(j + 1, ITERS - 1), 0)
        return basis, heights

    basis, heights = lax.fori_loop(0, ITERS, body, (basis, heights))
    h = [[heights[i, j] for j in range(ITERS)] for i in range(ITERS + 1)]
    target = [first] + [jnp.zeros((), F32)] * ITERS
    turns = []
    for j in range(ITERS):
        for i in range(j):
            c, s = turns[i]
            h[i][j], h[i + 1][j] = c * h[i][j] + s * h[i + 1][j], c * h[i + 1][j] - s * h[i][j]
        radius = jnp.sqrt(h[j][j] * h[j][j] + h[j + 1][j] * h[j + 1][j])
        c, s = h[j][j] / radius, h[j + 1][j] / radius
        turns.append((c, s))
        h[j][j] = radius
        target[j], target[j + 1] = c * target[j] + s * target[j + 1], c * target[j + 1] - s * target[j]
    y = [None] * ITERS
    for j in reversed(range(ITERS)):
        part = target[j]
        for i in range(j + 1, ITERS):
            part = part - h[j][i] * y[i]
        y[j] = part / h[j][j]
    weights = jnp.stack(y)
    answer = jnp.sum(weights[:, None, None, None] * basis, axis=0)
    return answer, forcing - operate(answer)


def per_device(nx, ny, forcing, damping, coupling, wind_lon, wind_lat):
    sol, res, flag = fused(nx, ny, forcing, damping, wind_lon, wind_lat, coupling)

    pin = lambda x: with_layout_constraint(x, Layout(tuple(range(x.ndim))))

    def again(state):
        sol, res = careful(pin(forcing), pin(damping), coupling, wind_lon, wind_lat)
        return pin(sol), pin(res), jnp.zeros((), F32)

    done = lax.while_loop(lambda state: state[2] > 0.5, again, (sol, res, flag[0, 0]))
    return pin(done[0]), pin(done[1])


def solution(mesh):
    nx, ny = mesh.shape["gx"], mesh.shape["gy"]
    in_specs = (P(None, "gy", "gx"), P(None, "gy", "gx"), P(), P("gy", "gx"), P("gy", "gx"))
    out_specs = (P(None, "gy", "gx"), P(None, "gy", "gx"))
    return jax.shard_map(
        functools.partial(per_device, nx, ny),
        mesh=mesh, in_specs=in_specs, out_specs=out_specs, check_vma=False,
    )
```

```python
import functools
import math

import jax
import jax.numpy as jnp
import numpy as np
from jax import lax
from jax.experimental import pallas as pl
from jax.experimental.pallas import tpu as pltpu
from jax.experimental.layout import Layout, with_layout_constraint
from jax.sharding import PartitionSpec as P

ITERS = 8
CH = 16
RIM = 8
LOW, HIGH = 1.0, 16.0
MID, HALF = (LOW + HIGH) / 2, (HIGH - LOW) / 2
BLOCK = 4
NOISE = 1.2e-7
TRUST = 1.0e-4
MESH = pl.DeviceIdType.MESH
F32 = jnp.float32


def trials():
    sub = lax.broadcasted_iota(jnp.int32, (16, 128), 0)
    lane = lanes((16, 128))
    tables = []
    for k in range(9):
        pair = jnp.minimum(sub, k) * 16 + jnp.maximum(sub, k)
        bits = pair * 1640531527 + lane * 668265263
        bits = (bits ^ lax.shift_right_logical(bits, 15)) * 739982445
        bits = bits ^ lax.shift_right_logical(bits, 13)
        sign = jnp.where((bits & 64) == 0, NOISE, -NOISE)
        tables.append(jnp.where((lane == 0) | (sub > 8), 0.0, sign))
    return tables


def row_kx(first, count, lat_total):
    row = (first + lax.broadcasted_iota(jnp.int32, (count, 128), 0)).astype(F32)
    phi = -math.pi / 2 + (row + 0.5) * (math.pi / lat_total)
    inside = (row >= 0.0) & (row < lat_total)
    cos = jnp.cos(phi)
    return jnp.where(inside, 0.5 / (cos * cos + 0.1), 0.0)


def lanes(shape):
    return lax.broadcasted_iota(jnp.int32, shape, len(shape) - 1)


def apply_a(vec):
    sub = lax.broadcasted_iota(jnp.int32, vec.shape, 0)
    up = pltpu.roll(vec, 1, 0)
    kept = jnp.where((sub == 0) | (sub == BLOCK), 0.0, vec)
    down = pltpu.roll(kept, 15, 0)
    return MID * vec + (HALF / 2) * (up + down)


def mat_vec(cols, vec, count):
    total = cols[0] * vec[0:1, :]
    for k in range(1, count):
        total = total + cols[k] * vec[k : k + 1, :]
    return total


def dot(a, b):
    return jnp.sum(a * b, axis=0, keepdims=True)


def gmres(cols):
    sub = lax.broadcasted_iota(jnp.int32, (16, 128), 0)
    first = jnp.sqrt(cols[0][0:1, :] + 1.0)
    basis = [jnp.where(sub == 0, 1.0, 0.0) / first]
    target = first
    targets = []
    columns = []
    turns = []
    for j in range(ITERS):
        w = apply_a(basis[j])
        u = mat_vec(cols, w, j + 2)
        h = [dot(v, u) for v in basis]
        for i in range(j + 1):
            w = w - h[i] * basis[i]
        norm = dot(w, mat_vec(cols, w, j + 2))
        below = jnp.sqrt(jnp.maximum(norm, 0.0) + 1.0)
        if j + 1 < ITERS:
            basis.append(w / below)
        col = list(h)
        for i, (c, s) in enumerate(turns):
            if i + 1 <= j:
                col[i], col[i + 1] = c * col[i] + s * col[i + 1], c * col[i + 1] - s * col[i]
        radius = jnp.sqrt(col[j] * col[j] + below * below)
        inv = 1.0 / radius
        c, s = col[j] * inv, below * inv
        turns.append((c, s))
        col[j] = radius
        columns.append((col, inv))
        targets.append(c * target)
        target = -s * target
    y = [None] * ITERS
    for j in reversed(range(ITERS)):
        y[j] = targets[j] * columns[j][1]
        for i in range(j):
            targets[i] = targets[i] - columns[j][0][i] * y[j]
    q = basis[0] * y[0]
    for j in range(1, ITERS):
        q = q + basis[j] * y[j]
    return q


def kernel(
    nx, ny, forc, damp, wlon, wlat, coup_hbm, outs, flag,
    *scratch,
):
    pwr, scratch = scratch[:ITERS], scratch[ITERS:]
    (ext, coef, main, wind, lon, pack, kxv, coup, made, rims, gx_slots, gy_slots,
     in_sem, lon_send, lon_recv, lat_send, lat_recv, cor_send, cor_recv,
     mid_send, mid_recv, gxs_send, gxs_recv, gys_send, gys_recv) = scratch
    gx, gy = lax.axis_index("gx"), lax.axis_index("gy")
    rows = forc.shape[1]
    top = RIM + rows
    total = rows + 2 * RIM
    groups = rows // 8
    east, west = lax.rem(gx + 1, nx), lax.rem(gx + nx - 1, nx)
    north, south = gy + 1, gy - 1
    has_n, has_s = gy < ny - 1, gy > 0
    no_n, no_s = jnp.logical_not(has_n), jnp.logical_not(has_s)

    def reach(count):
        return sorted(range(1, count), key=lambda k: min(k, count - k))

    barrier = pltpu.get_barrier_semaphore()
    line_x = [(lax.rem(gx + k, nx), gy) for k in reach(nx)]
    line_y = [(gx, lax.rem(gy + k, ny)) for k in reach(ny)]

    def greet(some):
        for peer in some:
            pl.semaphore_signal(barrier, 1, device_id=peer, device_id_type=MESH)

    greet(line_x[:2] + line_y[:2])

    loads = []
    for c in range(CH):
        for n, src in enumerate((forc, damp)):
            loads.append(pltpu.make_async_copy(
                src.at[c], ext.at[pl.ds(RIM, rows), CH * n + c, pl.ds(0, 256)],
                in_sem.at[CH * n + c]))
    for n, src in enumerate((wlon, wlat)):
        loads.append(pltpu.make_async_copy(
            src, wind.at[n, pl.ds(RIM, rows), pl.ds(0, 256)], in_sem.at[2 * CH + n]))
    loads.append(pltpu.make_async_copy(coup_hbm, coup, in_sem.at[2 * CH + 2]))
    for copy in loads:
        copy.start()
    greet(line_x[2:] + line_y[2:])
    kxv[...] = row_kx(gy * rows - RIM, total, rows * ny)
    for copy in loads:
        copy.wait()

    def turn(value, by):
        by = by % 128
        return pltpu.roll(value, by, value.ndim - 1) if by else value

    lane32, lane8 = lanes((2 * CH, 128)), lanes((8, 128))

    @pl.loop(0, groups)
    def _(g):
        for side in range(2):
            shift, cut = (0, pl.ds(0, 128)) if side == 0 else (16, pl.ds(128, 128))
            out = jnp.zeros((2 * CH, 128), F32)
            for j in range(8):
                here = (lane32 >= 16 * j) & (lane32 < 16 * j + 16)
                out = jnp.where(here, turn(ext[RIM + 8 * g + j, :, cut], 16 * j + shift), out)
            pack[side, g, 0 : 2 * CH, :] = out
            at = pl.ds(pl.multiple_of(RIM + 8 * g, 8), 8)
            a = turn(wind[0, at, cut], shift)
            b = turn(wind[1, at, cut], 16 + shift)
            pack[side, g, 2 * CH :, :] = jnp.where(lane8 < 16, a, b)

    pl.semaphore_wait(barrier, nx + ny - 2)

    go_west = pltpu.make_async_remote_copy(
        pack.at[0], lon.at[0, pl.ds(1, groups)], lon_send.at[0], lon_recv.at[0],
        device_id=(west, gy), device_id_type=MESH)
    go_east = pltpu.make_async_remote_copy(
        pack.at[1], lon.at[1, pl.ds(1, groups)], lon_send.at[1], lon_recv.at[1],
        device_id=(east, gy), device_id_type=MESH)
    go_west.start()
    go_east.start()

    def strip(ref, src, dst, size, chan, sem, peer):
        return pltpu.make_async_remote_copy(
            ref.at[pl.ds(src, size), chan, pl.ds(0, 256)],
            ref.at[pl.ds(dst, size), chan, pl.ds(0, 256)],
            lat_send.at[sem], lat_recv.at[sem], device_id=(gx, peer), device_id_type=MESH)

    def breeze(src, dst, sem, peer):
        return pltpu.make_async_remote_copy(
            wind.at[:, pl.ds(src, 8), pl.ds(0, 256)], wind.at[:, pl.ds(dst, 8), pl.ds(0, 256)],
            lat_send.at[sem], lat_recv.at[sem], device_id=(gx, peer), device_id_type=MESH)

    vec, par = pl.ds(0, CH), pl.ds(CH, CH)
    near_s = [breeze(RIM, top, 0, south), strip(ext, RIM, top, 4, vec, 1, south),
              strip(ext, RIM, top, 4, par, 2, south)]
    far_s = [strip(ext, RIM + 4, top + 4, 4, vec, 3, south),
             strip(ext, RIM + 4, top + 4, 2, par, 4, south)]
    near_n = [breeze(rows, 0, 5, north), strip(ext, rows + 4, 4, 4, vec, 6, north),
              strip(ext, rows + 4, 4, 4, par, 7, north)]
    far_n = [strip(ext, rows, 0, 4, vec, 8, north), strip(ext, rows + 2, 2, 2, par, 9, north)]
    to_s, to_n = near_s + far_s, near_n + far_n

    def await_strips(from_s, from_n):
        @pl.when(has_s)
        def _():
            for copy in from_s:
                copy.wait_recv()

        @pl.when(has_n)
        def _():
            for copy in from_n:
                copy.wait_recv()

    def await_sent(gone_s, gone_n):
        @pl.when(has_s)
        def _():
            for copy in gone_s:
                copy.wait_send()

        @pl.when(has_n)
        def _():
            for copy in gone_n:
                copy.wait_send()

    @pl.when(has_s)
    def _():
        for copy in to_s:
            copy.start()

    @pl.when(has_n)
    def _():
        for copy in to_n:
            copy.start()

    for missing, row, slot in ((no_s, 0, 0), (no_n, top, groups + 1)):
        @pl.when(missing)
        def _():
            ext[row : row + RIM, 0 : 2 * CH, 0:256] = jnp.zeros((RIM, 2 * CH, 256), F32)
            wind[:, row : row + RIM, 0:256] = jnp.zeros((2, RIM, 256), F32)
            lon[:, slot] = jnp.zeros((2, 40, 128), F32)

    two = 2.0 / HALF
    kind = lax.broadcasted_iota(jnp.int32, (8, 128), 0)
    by_kx = jnp.where(kind < 2, -two, 0.0)
    by_one = jnp.where((kind == 3) | (kind == 4), -0.5 * two, 0.0)
    eight = two * 8.0 / 12.0
    by_lon = jnp.where(kind == 0, eight, 0.0) + jnp.where(kind == 1, -eight, 0.0)
    by_lon = by_lon + jnp.where(kind == 2, -two / 12.0, 0.0)
    by_lat = jnp.where(kind == 3, eight, 0.0) + jnp.where(kind == 4, -eight, 0.0)
    by_lat = by_lat + jnp.where(kind == 5, -two / 12.0, 0.0)

    def merge(from_e, from_w):
        at = lanes(from_e.shape)
        return jnp.where(at < 16, from_e, jnp.where(at >= 112, from_w, 0.0))

    def third(g):
        at = pl.ds(pl.multiple_of(8 * g, 8), 8)
        for j in range(8):
            ext[8 * g + j, 0 : 2 * CH, 256:384] = merge(
                turn(lon[0, g, 0 : 2 * CH, :], -16 * j), turn(lon[1, g, 0 : 2 * CH, :], 112 - 16 * j))
        for n in range(2):
            wind[n, at, 256:384] = merge(
                turn(lon[0, g, 2 * CH :, :], -16 * n), turn(lon[1, g, 2 * CH :, :], 112 - 16 * n))

    def prepare(g, some=range(8), tiles=range(3)):
        at = pl.ds(pl.multiple_of(8 * g, 8), 8)
        kx8 = kxv[at, :]
        in8 = jnp.where(kx8 > 0.0, 1.0, 0.0)
        for t in tiles:
            cut = pl.ds(128 * t, 128)
            lon8, lat8 = wind[0, at, cut], wind[1, at, cut]
            for j in some:
                one = slice(j, j + 1)
                coef[8 * g + j, :, cut] = (
                    kx8[one] * by_kx + in8[one] * by_one + by_lon * lon8[one] + by_lat * lat8[one])
                diag = ext[8 * g + j, CH : 2 * CH, cut]
                gain, base = two * in8[one], (two * (2.0 - MID)) * in8[one] + (2.0 * two) * kx8[one]
                main[8 * g + j, :, cut] = diag * gain + base

    @pl.loop(1, groups + 1)
    def _(g):
        prepare(g, tiles=range(2))

    go_west.wait_recv()
    go_east.wait_recv()
    cor_s = pltpu.make_async_remote_copy(
        lon.at[:, 1], lon.at[:, groups + 1], cor_send.at[0], cor_recv.at[0],
        device_id=(gx, south), device_id_type=MESH)
    cor_n = pltpu.make_async_remote_copy(
        lon.at[:, groups], lon.at[:, 0], cor_send.at[1], cor_recv.at[1],
        device_id=(gx, north), device_id_type=MESH)

    @pl.when(has_s)
    def _():
        cor_s.start()

    @pl.when(has_n)
    def _():
        cor_n.start()

    @pl.loop(1, groups + 1)
    def _(g):
        third(g)
        prepare(g, tiles=(2,))

    cm = coup[...] * (0.25 * two)
    cm = jnp.concatenate([jnp.concatenate([cm] * 4, axis=1)] * 4, axis=0)
    r4 = lax.broadcasted_iota(jnp.int32, (64, 64), 0) // 16
    c4 = lax.broadcasted_iota(jnp.int32, (64, 64), 1) // 16
    cm = jnp.where(r4 == c4, cm, 0.0)
    cm_hi = cm.astype(jnp.bfloat16)
    cm_lo = (cm - cm_hi.astype(F32)).astype(jnp.bfloat16)
    weights = jnp.concatenate([cm_hi, cm_hi, cm_lo], axis=1)

    def power(k):
        return ext.at[:, pl.ds(0, CH), :] if k == 0 else pwr[k - 1]

    lane4 = lanes((4, CH, 128))

    def couple(src, r0):
        mids = [src[pl.ds(r0, 4), :, 128 * t : 128 * t + 128] for t in range(3)]
        flat = jnp.concatenate([m.reshape(64, 128) for m in mids], axis=1)
        hi = flat.astype(jnp.bfloat16)
        lo = (flat - hi.astype(F32)).astype(jnp.bfloat16)
        return jnp.dot(weights, jnp.concatenate([hi, lo, hi], axis=0), preferred_element_type=F32)

    def stencil(k, r0, mixed):
        src, dst = power(k), power(k + 1)
        prev = power(k - 1) if k % BLOCK else None
        mids = [src[pl.ds(r0, 4), :, 128 * t : 128 * t + 128] for t in range(3)]
        for t in range(3):
            cut = pl.ds(128 * t, 128)
            mid, nxt, prv = mids[t], mids[(t + 1) % 3], mids[(t + 2) % 3]
            e1 = pltpu.roll(jnp.where(lane4 < 1, nxt, mid), 127, 2)
            e2 = pltpu.roll(jnp.where(lane4 < 2, nxt, mid), 126, 2)
            w1 = pltpu.roll(jnp.where(lane4 >= 127, prv, mid), 1, 2)
            w2 = pltpu.roll(jnp.where(lane4 >= 126, prv, mid), 2, 2)
            n1 = src[pl.ds(r0 + 1, 4), :, cut]
            n2 = src[pl.ds(r0 + 2, 4), :, cut]
            s1 = src[pl.ds(r0 - 1, 4), :, cut]
            s2 = src[pl.ds(r0 - 2, 4), :, cut]
            cs = [coef[pl.ds(r0, 4), i : i + 1, cut] for i in range(6)]
            out = main[pl.ds(r0, 4), :, cut] * mid
            out = out + mixed[:, 128 * t : 128 * t + 128].reshape(4, CH, 128)
            out = out + cs[0] * e1 + cs[1] * w1 + cs[2] * (e2 - w2)
            out = out + cs[3] * n1 + cs[4] * s1 + cs[5] * (n2 - s2)
            if prev is not None:
                out = out - prev[pl.ds(r0, 4), :, cut]
            dst[pl.ds(r0, 4), :, cut] = out

    def inner(k):
        m = k % BLOCK + 1
        for r0 in range(RIM + 2 * m, top - 2 * m, 4):
            stencil(k, r0, couple(power(k), r0))

    def outer(k, far):
        m = k % BLOCK + 1
        for r0 in ((2 * m, top - 2 * m + 4) if far else (2 * m + 4, top - 2 * m)):
            stencil(k, r0, couple(power(k), r0))

    for k in range(BLOCK):
        inner(k)

    await_strips(near_n + [cor_n], near_s + [cor_s])
    third(0)
    third(groups + 1)
    prepare(0, range(4, 8))
    prepare(groups + 1, range(4))
    for k in range(BLOCK):
        outer(k, False)
    await_strips(far_n, far_s)
    prepare(0, range(2, 4))
    prepare(groups + 1, range(4, 6))
    for k in range(BLOCK):
        outer(k, True)

    half = power(BLOCK)
    lane16 = lanes((CH, 128))
    for side, row in ((0, RIM), (1, rows)):
        out = jnp.zeros((CH, 128), F32)
        for j in range(8):
            here = (lane16 >= 16 * j) & (lane16 < 16 * j + 16)
            out = jnp.where(here, turn(half[row + j, :, 256:384], 16 * j + 8), out)
        made[side] = out

    def again(src, dst, sem, peer):
        return pltpu.make_async_remote_copy(
            half.at[pl.ds(src, 4), :, pl.ds(0, 256)], half.at[pl.ds(dst, 4), :, pl.ds(0, 256)],
            mid_send.at[sem], mid_recv.at[sem], device_id=(gx, peer), device_id_type=MESH)

    def also(src, dst, sem, peer):
        return pltpu.make_async_remote_copy(
            made.at[src], rims.at[dst], mid_send.at[sem], mid_recv.at[sem],
            device_id=(gx, peer), device_id_type=MESH)

    near_s = [also(0, 1, 0, south), again(RIM, top, 1, south)]
    far_s2 = [again(RIM + 4, top + 4, 2, south)]
    near_n = [also(1, 0, 3, north), again(rows + 4, 4, 4, north)]
    far_n2 = [again(rows, 0, 5, north)]
    mid_s, mid_n = near_s + far_s2, near_n + far_n2

    @pl.when(has_s)
    def _():
        for copy in mid_s:
            copy.start()

    @pl.when(has_n)
    def _():
        for copy in mid_n:
            copy.start()

    for missing, row, slot in ((no_s, 0, 0), (no_n, top, 1)):
        @pl.when(missing)
        def _():
            half[row : row + RIM, :, 0:256] = jnp.zeros((RIM, CH, 256), F32)
            rims[slot] = jnp.zeros((CH, 128), F32)

    for k in range(BLOCK, ITERS):
        inner(k)

    pairs = [(i, k) for i in range(9) for k in range(i, 9)]

    def gram(r, sums):
        for o in range(2):
            for t in range(2):
                at = (r, pl.ds(8 * o, 8), pl.ds(128 * t, 128))
                vals = [power(k)[at] for k in range(9)]
                sums = [s + vals[i] * vals[k] for s, (i, k) in zip(sums, pairs)]
        return tuple(sums)

    sums = tuple(jnp.zeros((8, 128), F32) for _ in pairs)
    sums = lax.fori_loop(2 * RIM, top - RIM, gram, sums)
    await_strips(near_n, near_s)
    for side, row in ((0, 0), (1, top)):
        for j in range(8):
            half[row + j, :, 256:384] = turn(rims[side], -16 * j - 8)
    for k in range(BLOCK, ITERS):
        outer(k, False)
    sums = lax.fori_loop(
        0, 8, lambda g, acc: gram(RIM + 4 + g + (rows - 16) * (g // 4), acc), sums)
    await_strips(far_n2, far_s2)
    for k in range(BLOCK, ITERS):
        outer(k, True)
    sums = lax.fori_loop(0, 8, lambda g, acc: gram(RIM + g + (rows - 8) * (g // 4), acc), sums)

    sums = dict(zip(pairs, sums))
    folded = {p: jnp.sum(s, axis=0, keepdims=True) for p, s in sums.items()}
    sub8 = lax.broadcasted_iota(jnp.int32, (8, 128), 0)
    spread = jnp.zeros((8, 128), F32)
    for k in range(10):
        col = jnp.zeros((8, 128), F32)
        if k < 9:
            for i in range(8):
                col = jnp.where(sub8 == i, folded[min(i, k), max(i, k)], col)
        else:
            col = jnp.where(sub8 == 0, folded[8, 8], col)
        total_k = jnp.sum(col, axis=1, keepdims=True)
        spread = jnp.where(lane8 == 8 * k + sub8, total_k, spread)
    mine = jnp.sum(spread, axis=0, keepdims=True)

    def reduce_over(value, slots, send, recv, me, count, device):
        slots[me] = value
        for k in reversed(reach(count)):
            pltpu.make_async_remote_copy(
                slots.at[me], slots.at[me], send, recv,
                device_id=device(lax.rem(me + k, count)), device_id_type=MESH).start()
        rest = slots.at[pl.ds(0, count - 1)]
        every = pltpu.make_async_remote_copy(
            rest, rest, send, recv,
            device_id=device(lax.rem(me + 1, count)), device_id_type=MESH)
        every.wait_recv()
        parts = [slots[k] for k in range(count)]
        while len(parts) > 1:
            parts = [sum(parts[i : i + 2][1:], parts[i]) for i in range(0, len(parts), 2)]
        return parts[0], every

    value, one_way = reduce_over(mine, gx_slots, gxs_send, gxs_recv, gx, nx, lambda p: (p, gy))
    value, other_way = reduce_over(value, gy_slots, gys_send, gys_recv, gy, ny, lambda p: (gx, p))
    value = jnp.broadcast_to(value, (8, 128))
    picked = [jnp.where(lane8 == 8 * k + sub8, value, 0.0) for k in range(10)]
    upper = [jnp.broadcast_to(jnp.sum(p, axis=1, keepdims=True), (8, 128)) for p in picked]
    lower = [upper[8][k : k + 1, :] for k in range(8)] + [upper[9][0:1, :]]
    plain = [jnp.concatenate([u, jnp.where(sub8 == 0, w, 0.0)]) for u, w in zip(upper, lower)]
    sub = lax.broadcasted_iota(jnp.int32, (16, 128), 0)
    diag = jnp.zeros((16, 128), F32)
    for k in range(9):
        diag = jnp.where(sub == k, plain[k], diag)
    size = jnp.sqrt(diag)
    trial = trials()
    cols = [plain[k] + trial[k] * size * size[k : k + 1, :] for k in range(9)]
    q = gmres(cols)
    d = apply_a(q)
    q0 = jnp.broadcast_to(q[:, 0:1], (16, 128))
    d0 = jnp.broadcast_to(d[:, 0:1], (16, 128))
    left0 = jnp.where(sub == 0, 1.0, 0.0) - d0
    dq, dd = q - q0, d - d0
    bad_q = dot(dq, mat_vec(plain, dq, 8)) - TRUST**2 * dot(q0, mat_vec(plain, q0, 8))
    bad_d = dot(dd, mat_vec(plain, dd, 9)) - TRUST**2 * dot(left0, mat_vec(plain, left0, 9))
    fine = (bad_q <= 0.0) & (bad_d <= 0.0)
    flag[0, 0] = jnp.max(jnp.where(fine, 0.0, 1.0))

    qs = [q0[k : k + 1, :] for k in range(8)]
    ds = [left0[k : k + 1, :] for k in range(9)]

    @pl.loop(0, rows)
    def _(r):
        for t in range(2):
            cut = pl.ds(128 * t, 128)
            vals = [power(k)[r + RIM, :, cut] for k in range(9)]
            s = qs[0] * vals[0]
            e = ds[0] * vals[0]
            for k in range(1, 8):
                s = s + qs[k] * vals[k]
            for k in range(1, 9):
                e = e + ds[k] * vals[k]
            outs[0, r, :, cut] = s
            outs[1, r, :, cut] = e

    go_west.wait_send()
    go_east.wait_send()
    await_sent(to_s + [cor_s] + mid_s, to_n + [cor_n] + mid_n)
    one_way.wait_send()
    other_way.wait_send()


def unfold(outs, sol, res, sem):
    copies = []
    for c in range(CH):
        for n, dst in enumerate((sol, res)):
            copies.append(pltpu.make_async_copy(outs.at[n, :, c, :], dst.at[c], sem.at[n, c]))
    for copy in copies:
        copy.start()
    for copy in copies:
        copy.wait()


def fused(nx, ny, forcing, damping, wind_lon, wind_lat, coup):
    rows = forcing.shape[1]
    total = rows + 2 * RIM
    vm = pl.BlockSpec(memory_space=pltpu.VMEM)
    hbm = pl.BlockSpec(memory_space=pltpu.HBM)
    dma = pltpu.SemaphoreType.DMA
    outs, flag = pl.pallas_call(
        functools.partial(kernel, nx, ny),
        out_shape=(jax.ShapeDtypeStruct((2, rows, CH, 256), F32), jax.ShapeDtypeStruct((1, 1), F32)),
        in_specs=[hbm] * 5,
        out_specs=(vm, pl.BlockSpec(memory_space=pltpu.SMEM)),
        scratch_shapes=[pltpu.VMEM((total, CH, 384), F32)] * ITERS + [
            pltpu.VMEM((total, 2 * CH, 384), F32),
            pltpu.VMEM((total, 8, 384), F32),
            pltpu.VMEM((total, CH, 384), F32),
            pltpu.VMEM((2, total, 384), F32),
            pltpu.VMEM((2, total // 8, 40, 128), F32),
            pltpu.VMEM((2, rows // 8, 40, 128), F32),
            pltpu.VMEM((total, 128), F32),
            pltpu.VMEM((CH, CH), F32),
            pltpu.VMEM((2, CH, 128), F32),
            pltpu.VMEM((2, CH, 128), F32),
            pltpu.VMEM((nx, 1, 128), F32),
            pltpu.VMEM((ny, 1, 128), F32),
            dma((2 * CH + 3,)), dma((2,)), dma((2,)), dma((10,)), dma((10,)),
            dma((2,)), dma((2,)), dma((6,)), dma((6,)), dma, dma, dma, dma,
        ],
        compiler_params=pltpu.CompilerParams(
            collective_id=0, has_side_effects=True, vmem_limit_bytes=48 * 1024 * 1024),
        name="krylov",
    )(forcing, damping, wind_lon, wind_lat, coup)
    field = jax.ShapeDtypeStruct(forcing.shape, F32)
    sol, res = pl.pallas_call(
        unfold,
        out_shape=(field, field),
        in_specs=[vm],
        out_specs=(hbm, hbm),
        scratch_shapes=[dma((2, CH))],
        compiler_params=pltpu.CompilerParams(vmem_limit_bytes=8 * 1024 * 1024),
        name="unfold",
    )(outs)
    return sol, res, flag


def shifted(cells, axis, dim, closed, width):
    count = lax.axis_size(axis)
    ends = count if closed else count - 1
    head = lax.slice_in_dim(cells, 0, width, axis=dim)
    tail = lax.slice_in_dim(cells, cells.shape[dim] - width, cells.shape[dim], axis=dim)
    return jnp.concatenate(
        [
            lax.ppermute(tail, axis, [(i, (i + 1) % count) for i in range(ends)]),
            cells,
            lax.ppermute(head, axis, [((i + 1) % count, i) for i in range(ends)]),
        ],
        axis=dim,
    )


def apply_plain(vec, damping, coupling, wind_lon, wind_lat, kx):
    wide = shifted(vec, "gx", 2, True, 2)
    tall = shifted(vec, "gy", 1, False, 2)
    e1, w1, e2, w2 = wide[:, :, 3:-1], wide[:, :, 1:-3], wide[:, :, 4:], wide[:, :, :-4]
    n1, s1, n2, s2 = tall[:, 3:-1], tall[:, 1:-3], tall[:, 4:], tall[:, :-4]
    mixed = jnp.einsum("ij,jab->iab", coupling, vec, precision=lax.Precision.HIGHEST)
    return (
        (1.0 + damping) * vec + 0.25 * mixed
        + kx * (2.0 * vec - e1 - w1) + 0.5 * (2.0 * vec - n1 - s1)
        + wind_lon * ((8.0 * (e1 - w1) - (e2 - w2)) / 12.0)
        + wind_lat * ((8.0 * (n1 - s1) - (n2 - s2)) / 12.0)
    )


def careful(forcing, damping, coupling, wind_lon, wind_lat):
    rows = forcing.shape[1]
    pos = (lax.axis_index("gy") * rows + jnp.arange(rows)).astype(F32)
    phi = -math.pi / 2 + (pos + 0.5) * (math.pi / (rows * lax.axis_size("gy")))
    kx = (0.5 / (jnp.cos(phi) ** 2 + 0.1))[:, None]
    operate = lambda v: apply_plain(v, damping, coupling, wind_lon, wind_lat, kx)
    every = ("gx", "gy")
    first = jnp.sqrt(lax.psum(jnp.sum(forcing * forcing), every) + 1.0)
    basis = jnp.zeros((ITERS,) + forcing.shape, F32).at[0].set(forcing / first)
    heights = jnp.zeros((ITERS + 1, ITERS), F32)

    def body(j, state):
        basis, heights = state
        w = operate(lax.dynamic_index_in_dim(basis, j, 0, keepdims=False))
        h = lax.psum(jnp.sum(basis * w[None], axis=(1, 2, 3)), every)
        w = w - jnp.sum(h[:, None, None, None] * basis, axis=0)
        below = jnp.sqrt(lax.psum(jnp.sum(w * w), every) + 1.0)
        col = jnp.concatenate([h, jnp.zeros((1,), F32)])
        col = jnp.where(jnp.arange(ITERS + 1) == j + 1, below, col)
        heights = lax.dynamic_update_slice(heights, col[:, None], (0, j))
        old = lax.dynamic_index_in_dim(basis, jnp.minimum(j + 1, ITERS - 1), 0, keepdims=False)
        new = jnp.where(j + 1 < ITERS, w / below, old)
        basis = lax.dynamic_update_index_in_dim(basis, new, jnp.minimum(j + 1, ITERS - 1), 0)
        return basis, heights

    basis, heights = lax.fori_loop(0, ITERS, body, (basis, heights))
    h = [[heights[i, j] for j in range(ITERS)] for i in range(ITERS + 1)]
    target = [first] + [jnp.zeros((), F32)] * ITERS
    turns = []
    for j in range(ITERS):
        for i in range(j):
            c, s = turns[i]
            h[i][j], h[i + 1][j] = c * h[i][j] + s * h[i + 1][j], c * h[i + 1][j] - s * h[i][j]
        radius = jnp.sqrt(h[j][j] * h[j][j] + h[j + 1][j] * h[j + 1][j])
        c, s = h[j][j] / radius, h[j + 1][j] / radius
        turns.append((c, s))
        h[j][j] = radius
        target[j], target[j + 1] = c * target[j] + s * target[j + 1], c * target[j + 1] - s * target[j]
    y = [None] * ITERS
    for j in reversed(range(ITERS)):
        part = target[j]
        for i in range(j + 1, ITERS):
            part = part - h[j][i] * y[i]
        y[j] = part / h[j][j]
    weights = jnp.stack(y)
    answer = jnp.sum(weights[:, None, None, None] * basis, axis=0)
    return answer, forcing - operate(answer)


def per_device(nx, ny, forcing, damping, coupling, wind_lon, wind_lat):
    sol, res, flag = fused(nx, ny, forcing, damping, wind_lon, wind_lat, coupling)

    pin = lambda x: with_layout_constraint(x, Layout(tuple(range(x.ndim))))

    def again(state):
        sol, res = careful(pin(forcing), pin(damping), coupling, wind_lon, wind_lat)
        return pin(sol), pin(res), jnp.zeros((), F32)

    done = lax.while_loop(lambda state: state[2] > 0.5, again, (sol, res, flag[0, 0]))
    return pin(done[0]), pin(done[1])


def solution(mesh):
    nx, ny = mesh.shape["gx"], mesh.shape["gy"]
    in_specs = (P(None, "gy", "gx"), P(None, "gy", "gx"), P(), P("gy", "gx"), P("gy", "gx"))
    out_specs = (P(None, "gy", "gx"), P(None, "gy", "gx"))
    return jax.shard_map(
        functools.partial(per_device, nx, ny),
        mesh=mesh, in_specs=in_specs, out_specs=out_specs, check_vma=False,
    )
```

```python
import functools
import math

import jax
import jax.numpy as jnp
import numpy as np
from jax import lax
from jax.experimental import pallas as pl
from jax.experimental.pallas import tpu as pltpu
from jax.experimental.layout import Layout, with_layout_constraint
from jax.sharding import PartitionSpec as P

ITERS = 8
CH = 16
RIM = 8
LOW, HIGH = 1.0, 16.0
MID, HALF = (LOW + HIGH) / 2, (HIGH - LOW) / 2
BLOCK = 4
NOISE = 1.2e-7
TRUST = 1.0e-4
MESH = pl.DeviceIdType.MESH
F32 = jnp.float32


def trials():
    sub = lax.broadcasted_iota(jnp.int32, (16, 128), 0)
    lane = lanes((16, 128))
    tables = []
    for k in range(9):
        pair = jnp.minimum(sub, k) * 16 + jnp.maximum(sub, k)
        bits = pair * 1640531527 + lane * 668265263
        bits = (bits ^ lax.shift_right_logical(bits, 15)) * 739982445
        bits = bits ^ lax.shift_right_logical(bits, 13)
        sign = jnp.where((bits & 64) == 0, NOISE, -NOISE)
        tables.append(jnp.where((lane == 0) | (sub > 8), 0.0, sign))
    return tables


def row_kx(first, count, lat_total):
    row = (first + lax.broadcasted_iota(jnp.int32, (count, 128), 0)).astype(F32)
    phi = -math.pi / 2 + (row + 0.5) * (math.pi / lat_total)
    inside = (row >= 0.0) & (row < lat_total)
    cos = jnp.cos(phi)
    return jnp.where(inside, 0.5 / (cos * cos + 0.1), 0.0)


def lanes(shape):
    return lax.broadcasted_iota(jnp.int32, shape, len(shape) - 1)


def apply_a(vec):
    sub = lax.broadcasted_iota(jnp.int32, vec.shape, 0)
    up = pltpu.roll(vec, 1, 0)
    kept = jnp.where((sub == 0) | (sub == BLOCK), 0.0, vec)
    down = pltpu.roll(kept, 15, 0)
    return MID * vec + (HALF / 2) * (up + down)


def mat_vec(cols, vec, count):
    total = cols[0] * vec[0:1, :]
    for k in range(1, count):
        total = total + cols[k] * vec[k : k + 1, :]
    return total


def dot(a, b):
    return jnp.sum(a * b, axis=0, keepdims=True)


def gmres(cols):
    sub = lax.broadcasted_iota(jnp.int32, (16, 128), 0)
    first = jnp.sqrt(cols[0][0:1, :] + 1.0)
    basis = [jnp.where(sub == 0, 1.0, 0.0) / first]
    target = first
    targets = []
    columns = []
    turns = []
    for j in range(ITERS):
        w = apply_a(basis[j])
        u = mat_vec(cols, w, j + 2)
        h = [dot(v, u) for v in basis]
        for i in range(j + 1):
            w = w - h[i] * basis[i]
        norm = dot(w, mat_vec(cols, w, j + 2))
        below = jnp.sqrt(jnp.maximum(norm, 0.0) + 1.0)
        if j + 1 < ITERS:
            basis.append(w / below)
        col = list(h)
        for i, (c, s) in enumerate(turns):
            if i + 1 <= j:
                col[i], col[i + 1] = c * col[i] + s * col[i + 1], c * col[i + 1] - s * col[i]
        radius = jnp.sqrt(col[j] * col[j] + below * below)
        inv = 1.0 / radius
        c, s = col[j] * inv, below * inv
        turns.append((c, s))
        col[j] = radius
        columns.append((col, inv))
        targets.append(c * target)
        target = -s * target
    y = [None] * ITERS
    for j in reversed(range(ITERS)):
        y[j] = targets[j] * columns[j][1]
        for i in range(j):
            targets[i] = targets[i] - columns[j][0][i] * y[j]
    q = basis[0] * y[0]
    for j in range(1, ITERS):
        q = q + basis[j] * y[j]
    return q


def kernel(
    nx, ny, forc, damp, wlon, wlat, coup_hbm, outs, flag,
    *scratch,
):
    pwr, scratch = scratch[:ITERS], scratch[ITERS:]
    (ext, coef, main, wind, lon, pack, kxv, coup, made, rims, gx_slots, gy_slots,
     in_sem, lon_send, lon_recv, lat_send, lat_recv, cor_send, cor_recv,
     mid_send, mid_recv, gxs_send, gxs_recv, gys_send, gys_recv) = scratch
    gx, gy = lax.axis_index("gx"), lax.axis_index("gy")
    rows = forc.shape[1]
    top = RIM + rows
    total = rows + 2 * RIM
    groups = rows // 8
    east, west = lax.rem(gx + 1, nx), lax.rem(gx + nx - 1, nx)
    north, south = gy + 1, gy - 1
    has_n, has_s = gy < ny - 1, gy > 0
    no_n, no_s = jnp.logical_not(has_n), jnp.logical_not(has_s)

    def reach(count):
        return sorted(range(1, count), key=lambda k: min(k, count - k))

    barrier = pltpu.get_barrier_semaphore()
    line_x = [(lax.rem(gx + k, nx), gy) for k in reach(nx)]
    line_y = [(gx, lax.rem(gy + k, ny)) for k in reach(ny)]

    def greet(some):
        for peer in some:
            pl.semaphore_signal(barrier, 1, device_id=peer, device_id_type=MESH)

    greet(line_x[:2] + line_y[:2])

    loads = []
    for c in range(CH):
        for n, src in enumerate((forc, damp)):
            loads.append(pltpu.make_async_copy(
                src.at[c], ext.at[pl.ds(RIM, rows), CH * n + c, pl.ds(0, 256)],
                in_sem.at[CH * n + c]))
    for n, src in enumerate((wlon, wlat)):
        loads.append(pltpu.make_async_copy(
            src, wind.at[n, pl.ds(RIM, rows), pl.ds(0, 256)], in_sem.at[2 * CH + n]))
    loads.append(pltpu.make_async_copy(coup_hbm, coup, in_sem.at[2 * CH + 2]))
    for copy in loads:
        copy.start()
    greet(line_x[2:] + line_y[2:])
    kxv[...] = row_kx(gy * rows - RIM, total, rows * ny)
    for copy in loads:
        copy.wait()

    def turn(value, by):
        by = by % 128
        return pltpu.roll(value, by, value.ndim - 1) if by else value

    lane32, lane8 = lanes((2 * CH, 128)), lanes((8, 128))

    for g in range(groups):
        for side in range(2):
            shift, cut = (0, pl.ds(0, 128)) if side == 0 else (16, pl.ds(128, 128))
            out = jnp.zeros((2 * CH, 128), F32)
            for j in range(8):
                here = (lane32 >= 16 * j) & (lane32 < 16 * j + 16)
                out = jnp.where(here, turn(ext[RIM + 8 * g + j, :, cut], 16 * j + shift), out)
            pack[side, g, 0 : 2 * CH, :] = out
            at = pl.ds(RIM + 8 * g, 8)
            a = turn(wind[0, at, cut], shift)
            b = turn(wind[1, at, cut], 16 + shift)
            pack[side, g, 2 * CH :, :] = jnp.where(lane8 < 16, a, b)

    pl.semaphore_wait(barrier, nx + ny - 2)

    go_west = pltpu.make_async_remote_copy(
        pack.at[0], lon.at[0, pl.ds(1, groups)], lon_send.at[0], lon_recv.at[0],
        device_id=(west, gy), device_id_type=MESH)
    go_east = pltpu.make_async_remote_copy(
        pack.at[1], lon.at[1, pl.ds(1, groups)], lon_send.at[1], lon_recv.at[1],
        device_id=(east, gy), device_id_type=MESH)
    go_west.start()
    go_east.start()

    def strip(ref, src, dst, size, chan, sem, peer):
        return pltpu.make_async_remote_copy(
            ref.at[pl.ds(src, size), chan, pl.ds(0, 256)],
            ref.at[pl.ds(dst, size), chan, pl.ds(0, 256)],
            lat_send.at[sem], lat_recv.at[sem], device_id=(gx, peer), device_id_type=MESH)

    def breeze(src, dst, sem, peer):
        return pltpu.make_async_remote_copy(
            wind.at[:, pl.ds(src, 8), pl.ds(0, 256)], wind.at[:, pl.ds(dst, 8), pl.ds(0, 256)],
            lat_send.at[sem], lat_recv.at[sem], device_id=(gx, peer), device_id_type=MESH)

    vec, par = pl.ds(0, CH), pl.ds(CH, CH)
    near_s = [breeze(RIM, top, 0, south), strip(ext, RIM, top, 4, vec, 1, south),
              strip(ext, RIM, top, 4, par, 2, south)]
    far_s = [strip(ext, RIM + 4, top + 4, 4, vec, 3, south),
             strip(ext, RIM + 4, top + 4, 2, par, 4, south)]
    near_n = [breeze(rows, 0, 5, north), strip(ext, rows + 4, 4, 4, vec, 6, north),
              strip(ext, rows + 4, 4, 4, par, 7, north)]
    far_n = [strip(ext, rows, 0, 4, vec, 8, north), strip(ext, rows + 2, 2, 2, par, 9, north)]
    to_s, to_n = near_s + far_s, near_n + far_n

    def await_strips(from_s, from_n):
        @pl.when(has_s)
        def _():
            for copy in from_s:
                copy.wait_recv()

        @pl.when(has_n)
        def _():
            for copy in from_n:
                copy.wait_recv()

    def await_sent(gone_s, gone_n):
        @pl.when(has_s)
        def _():
            for copy in gone_s:
                copy.wait_send()

        @pl.when(has_n)
        def _():
            for copy in gone_n:
                copy.wait_send()

    @pl.when(has_s)
    def _():
        for copy in to_s:
            copy.start()

    @pl.when(has_n)
    def _():
        for copy in to_n:
            copy.start()

    for missing, row, slot in ((no_s, 0, 0), (no_n, top, groups + 1)):
        @pl.when(missing)
        def _():
            ext[row : row + RIM, 0 : 2 * CH, 0:256] = jnp.zeros((RIM, 2 * CH, 256), F32)
            wind[:, row : row + RIM, 0:256] = jnp.zeros((2, RIM, 256), F32)
            lon[:, slot] = jnp.zeros((2, 40, 128), F32)

    two = 2.0 / HALF
    kind = lax.broadcasted_iota(jnp.int32, (8, 128), 0)
    by_kx = jnp.where(kind < 2, -two, 0.0)
    by_one = jnp.where((kind == 3) | (kind == 4), -0.5 * two, 0.0)
    eight = two * 8.0 / 12.0
    by_lon = jnp.where(kind == 0, eight, 0.0) + jnp.where(kind == 1, -eight, 0.0)
    by_lon = by_lon + jnp.where(kind == 2, -two / 12.0, 0.0)
    by_lat = jnp.where(kind == 3, eight, 0.0) + jnp.where(kind == 4, -eight, 0.0)
    by_lat = by_lat + jnp.where(kind == 5, -two / 12.0, 0.0)

    def merge(from_e, from_w):
        at = lanes(from_e.shape)
        return jnp.where(at < 16, from_e, jnp.where(at >= 112, from_w, 0.0))

    def third(g):
        at = pl.ds(pl.multiple_of(8 * g, 8), 8)
        for j in range(8):
            ext[8 * g + j, 0 : 2 * CH, 256:384] = merge(
                turn(lon[0, g, 0 : 2 * CH, :], -16 * j), turn(lon[1, g, 0 : 2 * CH, :], 112 - 16 * j))
        for n in range(2):
            wind[n, at, 256:384] = merge(
                turn(lon[0, g, 2 * CH :, :], -16 * n), turn(lon[1, g, 2 * CH :, :], 112 - 16 * n))

    def prepare(g, some=range(8), tiles=range(3)):
        at = pl.ds(pl.multiple_of(8 * g, 8), 8)
        kx8 = kxv[at, :]
        in8 = jnp.where(kx8 > 0.0, 1.0, 0.0)
        for t in tiles:
            cut = pl.ds(128 * t, 128)
            lon8, lat8 = wind[0, at, cut], wind[1, at, cut]
            for j in some:
                one = slice(j, j + 1)
                coef[8 * g + j, :, cut] = (
                    kx8[one] * by_kx + in8[one] * by_one + by_lon * lon8[one] + by_lat * lat8[one])
                diag = ext[8 * g + j, CH : 2 * CH, cut]
                gain, base = two * in8[one], (two * (2.0 - MID)) * in8[one] + (2.0 * two) * kx8[one]
                main[8 * g + j, :, cut] = diag * gain + base

    @pl.loop(1, groups + 1)
    def _(g):
        prepare(g, tiles=range(2))

    go_west.wait_recv()
    go_east.wait_recv()
    cor_s = pltpu.make_async_remote_copy(
        lon.at[:, 1], lon.at[:, groups + 1], cor_send.at[0], cor_recv.at[0],
        device_id=(gx, south), device_id_type=MESH)
    cor_n = pltpu.make_async_remote_copy(
        lon.at[:, groups], lon.at[:, 0], cor_send.at[1], cor_recv.at[1],
        device_id=(gx, north), device_id_type=MESH)

    @pl.when(has_s)
    def _():
        cor_s.start()

    @pl.when(has_n)
    def _():
        cor_n.start()

    for g in range(1, groups + 1):
        third(g)
        prepare(g, tiles=(2,))

    cm = coup[...] * (0.25 * two)
    cm = jnp.concatenate([jnp.concatenate([cm] * 4, axis=1)] * 4, axis=0)
    r4 = lax.broadcasted_iota(jnp.int32, (64, 64), 0) // 16
    c4 = lax.broadcasted_iota(jnp.int32, (64, 64), 1) // 16
    cm = jnp.where(r4 == c4, cm, 0.0)
    cm_hi = cm.astype(jnp.bfloat16)
    cm_lo = (cm - cm_hi.astype(F32)).astype(jnp.bfloat16)
    weights = jnp.concatenate([cm_hi, cm_hi, cm_lo], axis=1)

    def power(k):
        return ext.at[:, pl.ds(0, CH), :] if k == 0 else pwr[k - 1]

    lane4 = lanes((4, CH, 128))

    def couple(src, r0, tiles):
        mids = [src[pl.ds(r0, 4), :, 128 * t : 128 * t + 128] for t in range(tiles)]
        flat = jnp.concatenate([m.reshape(64, 128) for m in mids], axis=1)
        hi = flat.astype(jnp.bfloat16)
        lo = (flat - hi.astype(F32)).astype(jnp.bfloat16)
        return jnp.dot(weights, jnp.concatenate([hi, lo, hi], axis=0), preferred_element_type=F32)

    def stencil(k, r0):
        src, dst = power(k), power(k + 1)
        tiles = 3 if k + 1 < ITERS else 2
        mixed = couple(src, r0, tiles)
        prev = power(k - 1) if k % BLOCK else None
        mids = [src[pl.ds(r0, 4), :, 128 * t : 128 * t + 128] for t in range(3)]
        for t in range(tiles):
            cut = pl.ds(128 * t, 128)
            mid, nxt, prv = mids[t], mids[(t + 1) % 3], mids[(t + 2) % 3]
            e1 = pltpu.roll(jnp.where(lane4 < 1, nxt, mid), 127, 2)
            e2 = pltpu.roll(jnp.where(lane4 < 2, nxt, mid), 126, 2)
            w1 = pltpu.roll(jnp.where(lane4 >= 127, prv, mid), 1, 2)
            w2 = pltpu.roll(jnp.where(lane4 >= 126, prv, mid), 2, 2)
            n1 = src[pl.ds(r0 + 1, 4), :, cut]
            n2 = src[pl.ds(r0 + 2, 4), :, cut]
            s1 = src[pl.ds(r0 - 1, 4), :, cut]
            s2 = src[pl.ds(r0 - 2, 4), :, cut]
            cs = [coef[pl.ds(r0, 4), i : i + 1, cut] for i in range(6)]
            out = main[pl.ds(r0, 4), :, cut] * mid
            out = out + mixed[:, 128 * t : 128 * t + 128].reshape(4, CH, 128)
            out = out + cs[0] * e1 + cs[1] * w1 + cs[2] * (e2 - w2)
            out = out + cs[3] * n1 + cs[4] * s1 + cs[5] * (n2 - s2)
            if prev is not None:
                out = out - prev[pl.ds(r0, 4), :, cut]
            dst[pl.ds(r0, 4), :, cut] = out

    def inner(k):
        m = k % BLOCK + 1
        for r0 in range(RIM + 2 * m, top - 2 * m, 4):
            stencil(k, r0)

    def outer(k, far):
        m = k % BLOCK + 1
        for r0 in ((2 * m, top - 2 * m + 4) if far else (2 * m + 4, top - 2 * m)):
            stencil(k, r0)

    for k in range(BLOCK):
        inner(k)

    await_strips(near_n + [cor_n], near_s + [cor_s])
    third(0)
    third(groups + 1)
    prepare(0, range(4, 8))
    prepare(groups + 1, range(4))
    for k in range(BLOCK):
        outer(k, False)
    await_strips(far_n, far_s)
    prepare(0, range(2, 4))
    prepare(groups + 1, range(4, 6))
    for k in range(BLOCK):
        outer(k, True)

    half = power(BLOCK)
    lane16 = lanes((CH, 128))
    for side, row in ((0, RIM), (1, rows)):
        out = jnp.zeros((CH, 128), F32)
        for j in range(8):
            here = (lane16 >= 16 * j) & (lane16 < 16 * j + 16)
            out = jnp.where(here, turn(half[row + j, :, 256:384], 16 * j + 8), out)
        made[side] = out

    def again(src, dst, sem, peer):
        return pltpu.make_async_remote_copy(
            half.at[pl.ds(src, 4), :, pl.ds(0, 256)], half.at[pl.ds(dst, 4), :, pl.ds(0, 256)],
            mid_send.at[sem], mid_recv.at[sem], device_id=(gx, peer), device_id_type=MESH)

    def also(src, dst, sem, peer):
        return pltpu.make_async_remote_copy(
            made.at[src], rims.at[dst], mid_send.at[sem], mid_recv.at[sem],
            device_id=(gx, peer), device_id_type=MESH)

    near_s = [also(0, 1, 0, south), again(RIM, top, 1, south)]
    far_s2 = [again(RIM + 4, top + 4, 2, south)]
    near_n = [also(1, 0, 3, north), again(rows + 4, 4, 4, north)]
    far_n2 = [again(rows, 0, 5, north)]
    mid_s, mid_n = near_s + far_s2, near_n + far_n2

    @pl.when(has_s)
    def _():
        for copy in mid_s:
            copy.start()

    @pl.when(has_n)
    def _():
        for copy in mid_n:
            copy.start()

    for missing, row, slot in ((no_s, 0, 0), (no_n, top, 1)):
        @pl.when(missing)
        def _():
            half[row : row + RIM, :, 0:256] = jnp.zeros((RIM, CH, 256), F32)
            rims[slot] = jnp.zeros((CH, 128), F32)

    for k in range(BLOCK, ITERS):
        inner(k)

    pairs = [(i, k) for i in range(9) for k in range(i, 9)]

    def gram(r, sums):
        for o in range(2):
            for t in range(2):
                at = (r, pl.ds(8 * o, 8), pl.ds(128 * t, 128))
                vals = [power(k)[at] for k in range(9)]
                sums = [s + vals[i] * vals[k] for s, (i, k) in zip(sums, pairs)]
        return tuple(sums)

    sums = tuple(jnp.zeros((8, 128), F32) for _ in pairs)
    sums = lax.fori_loop(2 * RIM, top - RIM, gram, sums)
    await_strips(near_n, near_s)
    for side, row in ((0, 0), (1, top)):
        for j in range(8):
            half[row + j, :, 256:384] = turn(rims[side], -16 * j - 8)
    for k in range(BLOCK, ITERS):
        outer(k, False)
    sums = lax.fori_loop(
        0, 8, lambda g, acc: gram(RIM + 4 + g + (rows - 16) * (g // 4), acc), sums)
    await_strips(far_n2, far_s2)
    for k in range(BLOCK, ITERS):
        outer(k, True)
    sums = lax.fori_loop(0, 8, lambda g, acc: gram(RIM + g + (rows - 8) * (g // 4), acc), sums)

    sums = dict(zip(pairs, sums))
    folded = {p: jnp.sum(s, axis=0, keepdims=True) for p, s in sums.items()}
    sub8 = lax.broadcasted_iota(jnp.int32, (8, 128), 0)
    spread = jnp.zeros((8, 128), F32)
    for k in range(10):
        col = jnp.zeros((8, 128), F32)
        if k < 9:
            for i in range(8):
                col = jnp.where(sub8 == i, folded[min(i, k), max(i, k)], col)
        else:
            col = jnp.where(sub8 == 0, folded[8, 8], col)
        total_k = jnp.sum(col, axis=1, keepdims=True)
        spread = jnp.where(lane8 == 8 * k + sub8, total_k, spread)
    mine = jnp.sum(spread, axis=0, keepdims=True)

    def reduce_over(value, slots, send, recv, me, count, device):
        slots[me] = value
        for k in reversed(reach(count)):
            pltpu.make_async_remote_copy(
                slots.at[me], slots.at[me], send, recv,
                device_id=device(lax.rem(me + k, count)), device_id_type=MESH).start()
        rest = slots.at[pl.ds(0, count - 1)]
        every = pltpu.make_async_remote_copy(
            rest, rest, send, recv,
            device_id=device(lax.rem(me + 1, count)), device_id_type=MESH)
        every.wait_recv()
        parts = [slots[k] for k in range(count)]
        while len(parts) > 1:
            parts = [sum(parts[i : i + 2][1:], parts[i]) for i in range(0, len(parts), 2)]
        return parts[0], every

    value, one_way = reduce_over(mine, gx_slots, gxs_send, gxs_recv, gx, nx, lambda p: (p, gy))
    value, other_way = reduce_over(value, gy_slots, gys_send, gys_recv, gy, ny, lambda p: (gx, p))
    value = jnp.broadcast_to(value, (8, 128))
    picked = [jnp.where(lane8 == 8 * k + sub8, value, 0.0) for k in range(10)]
    upper = [jnp.broadcast_to(jnp.sum(p, axis=1, keepdims=True), (8, 128)) for p in picked]
    lower = [upper[8][k : k + 1, :] for k in range(8)] + [upper[9][0:1, :]]
    plain = [jnp.concatenate([u, jnp.where(sub8 == 0, w, 0.0)]) for u, w in zip(upper, lower)]
    sub = lax.broadcasted_iota(jnp.int32, (16, 128), 0)
    diag = jnp.zeros((16, 128), F32)
    for k in range(9):
        diag = jnp.where(sub == k, plain[k], diag)
    size = jnp.sqrt(diag)
    trial = trials()
    cols = [plain[k] + trial[k] * size * size[k : k + 1, :] for k in range(9)]
    q = gmres(cols)
    d = apply_a(q)
    q0 = jnp.broadcast_to(q[:, 0:1], (16, 128))
    d0 = jnp.broadcast_to(d[:, 0:1], (16, 128))
    left0 = jnp.where(sub == 0, 1.0, 0.0) - d0
    dq, dd = q - q0, d - d0
    bad_q = dot(dq, mat_vec(plain, dq, 8)) - TRUST**2 * dot(q0, mat_vec(plain, q0, 8))
    bad_d = dot(dd, mat_vec(plain, dd, 9)) - TRUST**2 * dot(left0, mat_vec(plain, left0, 9))
    fine = (bad_q <= 0.0) & (bad_d <= 0.0)
    flag[0, 0] = jnp.max(jnp.where(fine, 0.0, 1.0))

    qs = [q0[k : k + 1, :] for k in range(8)]
    ds = [left0[k : k + 1, :] for k in range(9)]

    @pl.loop(0, rows, unroll=4)
    def _(r):
        for t in range(2):
            cut = pl.ds(128 * t, 128)
            vals = [power(k)[r + RIM, :, cut] for k in range(9)]
            s = qs[0] * vals[0]
            e = ds[0] * vals[0]
            for k in range(1, 8):
                s = s + qs[k] * vals[k]
            for k in range(1, 9):
                e = e + ds[k] * vals[k]
            outs[0, r, :, cut] = s
            outs[1, r, :, cut] = e

    go_west.wait_send()
    go_east.wait_send()
    await_sent(to_s + [cor_s] + mid_s, to_n + [cor_n] + mid_n)
    one_way.wait_send()
    other_way.wait_send()


def unfold(outs, sol, res, sem):
    copies = []
    for c in range(CH):
        for n, dst in enumerate((sol, res)):
            copies.append(pltpu.make_async_copy(outs.at[n, :, c, :], dst.at[c], sem.at[n, c]))
    for copy in copies:
        copy.start()
    for copy in copies:
        copy.wait()


def fused(nx, ny, forcing, damping, wind_lon, wind_lat, coup):
    rows = forcing.shape[1]
    total = rows + 2 * RIM
    vm = pl.BlockSpec(memory_space=pltpu.VMEM)
    hbm = pl.BlockSpec(memory_space=pltpu.HBM)
    dma = pltpu.SemaphoreType.DMA
    outs, flag = pl.pallas_call(
        functools.partial(kernel, nx, ny),
        out_shape=(jax.ShapeDtypeStruct((2, rows, CH, 256), F32), jax.ShapeDtypeStruct((1, 1), F32)),
        in_specs=[hbm] * 5,
        out_specs=(vm, pl.BlockSpec(memory_space=pltpu.SMEM)),
        scratch_shapes=[pltpu.VMEM((total, CH, 384), F32)] * ITERS + [
            pltpu.VMEM((total, 2 * CH, 384), F32),
            pltpu.VMEM((total, 8, 384), F32),
            pltpu.VMEM((total, CH, 384), F32),
            pltpu.VMEM((2, total, 384), F32),
            pltpu.VMEM((2, total // 8, 40, 128), F32),
            pltpu.VMEM((2, rows // 8, 40, 128), F32),
            pltpu.VMEM((total, 128), F32),
            pltpu.VMEM((CH, CH), F32),
            pltpu.VMEM((2, CH, 128), F32),
            pltpu.VMEM((2, CH, 128), F32),
            pltpu.VMEM((nx, 1, 128), F32),
            pltpu.VMEM((ny, 1, 128), F32),
            dma((2 * CH + 3,)), dma((2,)), dma((2,)), dma((10,)), dma((10,)),
            dma((2,)), dma((2,)), dma((6,)), dma((6,)), dma, dma, dma, dma,
        ],
        compiler_params=pltpu.CompilerParams(
            collective_id=0, has_side_effects=True, vmem_limit_bytes=48 * 1024 * 1024),
        name="krylov",
    )(forcing, damping, wind_lon, wind_lat, coup)
    field = jax.ShapeDtypeStruct(forcing.shape, F32)
    sol, res = pl.pallas_call(
        unfold,
        out_shape=(field, field),
        in_specs=[vm],
        out_specs=(hbm, hbm),
        scratch_shapes=[dma((2, CH))],
        compiler_params=pltpu.CompilerParams(vmem_limit_bytes=8 * 1024 * 1024),
        name="unfold",
    )(outs)
    return sol, res, flag


def shifted(cells, axis, dim, closed, width):
    count = lax.axis_size(axis)
    ends = count if closed else count - 1
    head = lax.slice_in_dim(cells, 0, width, axis=dim)
    tail = lax.slice_in_dim(cells, cells.shape[dim] - width, cells.shape[dim], axis=dim)
    return jnp.concatenate(
        [
            lax.ppermute(tail, axis, [(i, (i + 1) % count) for i in range(ends)]),
            cells,
            lax.ppermute(head, axis, [((i + 1) % count, i) for i in range(ends)]),
        ],
        axis=dim,
    )


def apply_plain(vec, damping, coupling, wind_lon, wind_lat, kx):
    wide = shifted(vec, "gx", 2, True, 2)
    tall = shifted(vec, "gy", 1, False, 2)
    e1, w1, e2, w2 = wide[:, :, 3:-1], wide[:, :, 1:-3], wide[:, :, 4:], wide[:, :, :-4]
    n1, s1, n2, s2 = tall[:, 3:-1], tall[:, 1:-3], tall[:, 4:], tall[:, :-4]
    mixed = jnp.einsum("ij,jab->iab", coupling, vec, precision=lax.Precision.HIGHEST)
    return (
        (1.0 + damping) * vec + 0.25 * mixed
        + kx * (2.0 * vec - e1 - w1) + 0.5 * (2.0 * vec - n1 - s1)
        + wind_lon * ((8.0 * (e1 - w1) - (e2 - w2)) / 12.0)
        + wind_lat * ((8.0 * (n1 - s1) - (n2 - s2)) / 12.0)
    )


def careful(forcing, damping, coupling, wind_lon, wind_lat):
    rows = forcing.shape[1]
    pos = (lax.axis_index("gy") * rows + jnp.arange(rows)).astype(F32)
    phi = -math.pi / 2 + (pos + 0.5) * (math.pi / (rows * lax.axis_size("gy")))
    kx = (0.5 / (jnp.cos(phi) ** 2 + 0.1))[:, None]
    operate = lambda v: apply_plain(v, damping, coupling, wind_lon, wind_lat, kx)
    every = ("gx", "gy")
    first = jnp.sqrt(lax.psum(jnp.sum(forcing * forcing), every) + 1.0)
    basis = jnp.zeros((ITERS,) + forcing.shape, F32).at[0].set(forcing / first)
    heights = jnp.zeros((ITERS + 1, ITERS), F32)

    def body(j, state):
        basis, heights = state
        w = operate(lax.dynamic_index_in_dim(basis, j, 0, keepdims=False))
        h = lax.psum(jnp.sum(basis * w[None], axis=(1, 2, 3)), every)
        w = w - jnp.sum(h[:, None, None, None] * basis, axis=0)
        below = jnp.sqrt(lax.psum(jnp.sum(w * w), every) + 1.0)
        col = jnp.concatenate([h, jnp.zeros((1,), F32)])
        col = jnp.where(jnp.arange(ITERS + 1) == j + 1, below, col)
        heights = lax.dynamic_update_slice(heights, col[:, None], (0, j))
        old = lax.dynamic_index_in_dim(basis, jnp.minimum(j + 1, ITERS - 1), 0, keepdims=False)
        new = jnp.where(j + 1 < ITERS, w / below, old)
        basis = lax.dynamic_update_index_in_dim(basis, new, jnp.minimum(j + 1, ITERS - 1), 0)
        return basis, heights

    basis, heights = lax.fori_loop(0, ITERS, body, (basis, heights))
    h = [[heights[i, j] for j in range(ITERS)] for i in range(ITERS + 1)]
    target = [first] + [jnp.zeros((), F32)] * ITERS
    turns = []
    for j in range(ITERS):
        for i in range(j):
            c, s = turns[i]
            h[i][j], h[i + 1][j] = c * h[i][j] + s * h[i + 1][j], c * h[i + 1][j] - s * h[i][j]
        radius = jnp.sqrt(h[j][j] * h[j][j] + h[j + 1][j] * h[j + 1][j])
        c, s = h[j][j] / radius, h[j + 1][j] / radius
        turns.append((c, s))
        h[j][j] = radius
        target[j], target[j + 1] = c * target[j] + s * target[j + 1], c * target[j + 1] - s * target[j]
    y = [None] * ITERS
    for j in reversed(range(ITERS)):
        part = target[j]
        for i in range(j + 1, ITERS):
            part = part - h[j][i] * y[i]
        y[j] = part / h[j][j]
    weights = jnp.stack(y)
    answer = jnp.sum(weights[:, None, None, None] * basis, axis=0)
    return answer, forcing - operate(answer)


def per_device(nx, ny, forcing, damping, coupling, wind_lon, wind_lat):
    sol, res, flag = fused(nx, ny, forcing, damping, wind_lon, wind_lat, coupling)

    pin = lambda x: with_layout_constraint(x, Layout(tuple(range(x.ndim))))

    def again(state):
        sol, res = careful(pin(forcing), pin(damping), coupling, wind_lon, wind_lat)
        return pin(sol), pin(res), jnp.zeros((), F32)

    done = lax.while_loop(lambda state: state[2] > 0.5, again, (sol, res, flag[0, 0]))
    return pin(done[0]), pin(done[1])


def solution(mesh):
    nx, ny = mesh.shape["gx"], mesh.shape["gy"]
    in_specs = (P(None, "gy", "gx"), P(None, "gy", "gx"), P(), P("gy", "gx"), P("gy", "gx"))
    out_specs = (P(None, "gy", "gx"), P(None, "gy", "gx"))
    return jax.shard_map(
        functools.partial(per_device, nx, ny),
        mesh=mesh, in_specs=in_specs, out_specs=out_specs, check_vma=False,
    )
```

```python
import functools
import math

import jax
import jax.numpy as jnp
import numpy as np
from jax import lax
from jax.experimental import pallas as pl
from jax.experimental.pallas import tpu as pltpu
from jax.experimental.layout import Layout, with_layout_constraint
from jax.sharding import PartitionSpec as P

ITERS = 8
CH = 16
RIM = 8
LOW, HIGH = 1.0, 16.0
MID, HALF = (LOW + HIGH) / 2, (HIGH - LOW) / 2
BLOCK = 4
NOISE = 1.2e-7
TRUST = 1.0e-4
MESH = pl.DeviceIdType.MESH
F32 = jnp.float32


def trials():
    sub = lax.broadcasted_iota(jnp.int32, (16, 128), 0)
    lane = lanes((16, 128))
    tables = []
    for k in range(9):
        pair = jnp.minimum(sub, k) * 16 + jnp.maximum(sub, k)
        bits = pair * 1640531527 + lane * 668265263
        bits = (bits ^ lax.shift_right_logical(bits, 15)) * 739982445
        bits = bits ^ lax.shift_right_logical(bits, 13)
        sign = jnp.where((bits & 64) == 0, NOISE, -NOISE)
        tables.append(jnp.where((lane == 0) | (sub > 8), 0.0, sign))
    return tables


def row_kx(first, count, lat_total):
    row = (first + lax.broadcasted_iota(jnp.int32, (count, 128), 0)).astype(F32)
    phi = -math.pi / 2 + (row + 0.5) * (math.pi / lat_total)
    inside = (row >= 0.0) & (row < lat_total)
    cos = jnp.cos(phi)
    return jnp.where(inside, 0.5 / (cos * cos + 0.1), 0.0)


def lanes(shape):
    return lax.broadcasted_iota(jnp.int32, shape, len(shape) - 1)


def apply_a(vec):
    sub = lax.broadcasted_iota(jnp.int32, vec.shape, 0)
    up = pltpu.roll(vec, 1, 0)
    kept = jnp.where((sub == 0) | (sub == BLOCK), 0.0, vec)
    down = pltpu.roll(kept, 15, 0)
    return MID * vec + (HALF / 2) * (up + down)


def mat_vec(cols, vec, count):
    total = cols[0] * vec[0:1, :]
    for k in range(1, count):
        total = total + cols[k] * vec[k : k + 1, :]
    return total


def dot(a, b):
    return jnp.sum(a * b, axis=0, keepdims=True)


def gmres(cols):
    sub = lax.broadcasted_iota(jnp.int32, (16, 128), 0)
    first = jnp.sqrt(cols[0][0:1, :] + 1.0)
    basis = [jnp.where(sub == 0, 1.0, 0.0) / first]
    target = first
    targets = []
    columns = []
    turns = []
    for j in range(ITERS):
        w = apply_a(basis[j])
        u = mat_vec(cols, w, j + 2)
        h = [dot(v, u) for v in basis]
        for i in range(j + 1):
            w = w - h[i] * basis[i]
        norm = dot(w, mat_vec(cols, w, j + 2))
        below = jnp.sqrt(jnp.maximum(norm, 0.0) + 1.0)
        if j + 1 < ITERS:
            basis.append(w / below)
        col = list(h)
        for i, (c, s) in enumerate(turns):
            if i + 1 <= j:
                col[i], col[i + 1] = c * col[i] + s * col[i + 1], c * col[i + 1] - s * col[i]
        radius = jnp.sqrt(col[j] * col[j] + below * below)
        inv = 1.0 / radius
        c, s = col[j] * inv, below * inv
        turns.append((c, s))
        col[j] = radius
        columns.append((col, inv))
        targets.append(c * target)
        target = -s * target
    y = [None] * ITERS
    for j in reversed(range(ITERS)):
        y[j] = targets[j] * columns[j][1]
        for i in range(j):
            targets[i] = targets[i] - columns[j][0][i] * y[j]
    q = basis[0] * y[0]
    for j in range(1, ITERS):
        q = q + basis[j] * y[j]
    return q


def kernel(
    nx, ny, forc, damp, wlon, wlat, coup_hbm, outs, flag,
    *scratch,
):
    pwr, scratch = scratch[:ITERS], scratch[ITERS:]
    (ext, coef, main, wind, lon, pack, kxv, coup, made, rims, gx_slots, gy_slots,
     in_sem, lon_send, lon_recv, lat_send, lat_recv, cor_send, cor_recv,
     mid_send, mid_recv, gxs_send, gxs_recv, gys_send, gys_recv) = scratch
    gx, gy = lax.axis_index("gx"), lax.axis_index("gy")
    rows = forc.shape[1]
    top = RIM + rows
    total = rows + 2 * RIM
    groups = rows // 8
    east, west = lax.rem(gx + 1, nx), lax.rem(gx + nx - 1, nx)
    north, south = gy + 1, gy - 1
    has_n, has_s = gy < ny - 1, gy > 0
    no_n, no_s = jnp.logical_not(has_n), jnp.logical_not(has_s)

    def reach(count):
        return sorted(range(1, count), key=lambda k: min(k, count - k))

    barrier = pltpu.get_barrier_semaphore()
    line_x = [(lax.rem(gx + k, nx), gy) for k in reach(nx)]
    line_y = [(gx, lax.rem(gy + k, ny)) for k in reach(ny)]

    def greet(some):
        for peer in some:
            pl.semaphore_signal(barrier, 1, device_id=peer, device_id_type=MESH)

    greet(line_x[:2] + line_y[:2])

    loads = []
    for c in range(CH):
        for n, src in enumerate((forc, damp)):
            loads.append(pltpu.make_async_copy(
                src.at[c], ext.at[pl.ds(RIM, rows), CH * n + c, pl.ds(0, 256)],
                in_sem.at[CH * n + c]))
    for n, src in enumerate((wlon, wlat)):
        loads.append(pltpu.make_async_copy(
            src, wind.at[n, pl.ds(RIM, rows), pl.ds(0, 256)], in_sem.at[2 * CH + n]))
    loads.append(pltpu.make_async_copy(coup_hbm, coup, in_sem.at[2 * CH + 2]))
    for copy in loads:
        copy.start()
    greet(line_x[2:] + line_y[2:])
    kxv[...] = row_kx(gy * rows - RIM, total, rows * ny)
    for copy in loads:
        copy.wait()

    def turn(value, by):
        by = by % 128
        return pltpu.roll(value, by, value.ndim - 1) if by else value

    lane32, lane8 = lanes((2 * CH, 128)), lanes((8, 128))

    for g in range(groups):
        for side in range(2):
            shift, cut = (0, pl.ds(0, 128)) if side == 0 else (16, pl.ds(128, 128))
            out = jnp.zeros((2 * CH, 128), F32)
            for j in range(8):
                here = (lane32 >= 16 * j) & (lane32 < 16 * j + 16)
                out = jnp.where(here, turn(ext[RIM + 8 * g + j, :, cut], 16 * j + shift), out)
            pack[side, g, 0 : 2 * CH, :] = out
            at = pl.ds(RIM + 8 * g, 8)
            a = turn(wind[0, at, cut], shift)
            b = turn(wind[1, at, cut], 16 + shift)
            pack[side, g, 2 * CH :, :] = jnp.where(lane8 < 16, a, b)

    pl.semaphore_wait(barrier, nx + ny - 2)

    go_west = pltpu.make_async_remote_copy(
        pack.at[0], lon.at[0, pl.ds(1, groups)], lon_send.at[0], lon_recv.at[0],
        device_id=(west, gy), device_id_type=MESH)
    go_east = pltpu.make_async_remote_copy(
        pack.at[1], lon.at[1, pl.ds(1, groups)], lon_send.at[1], lon_recv.at[1],
        device_id=(east, gy), device_id_type=MESH)
    go_west.start()
    go_east.start()

    def strip(ref, src, dst, size, chan, sem, peer):
        return pltpu.make_async_remote_copy(
            ref.at[pl.ds(src, size), chan, pl.ds(0, 256)],
            ref.at[pl.ds(dst, size), chan, pl.ds(0, 256)],
            lat_send.at[sem], lat_recv.at[sem], device_id=(gx, peer), device_id_type=MESH)

    def breeze(src, dst, sem, peer):
        return pltpu.make_async_remote_copy(
            wind.at[:, pl.ds(src, 8), pl.ds(0, 256)], wind.at[:, pl.ds(dst, 8), pl.ds(0, 256)],
            lat_send.at[sem], lat_recv.at[sem], device_id=(gx, peer), device_id_type=MESH)

    vec, par = pl.ds(0, CH), pl.ds(CH, CH)
    near_s = [breeze(RIM, top, 0, south), strip(ext, RIM, top, 4, vec, 1, south),
              strip(ext, RIM, top, 4, par, 2, south)]
    far_s = [strip(ext, RIM + 4, top + 4, 4, vec, 3, south),
             strip(ext, RIM + 4, top + 4, 2, par, 4, south)]
    near_n = [breeze(rows, 0, 5, north), strip(ext, rows + 4, 4, 4, vec, 6, north),
              strip(ext, rows + 4, 4, 4, par, 7, north)]
    far_n = [strip(ext, rows, 0, 4, vec, 8, north), strip(ext, rows + 2, 2, 2, par, 9, north)]
    to_s, to_n = near_s + far_s, near_n + far_n

    def await_strips(from_s, from_n):
        @pl.when(has_s)
        def _():
            for copy in from_s:
                copy.wait_recv()

        @pl.when(has_n)
        def _():
            for copy in from_n:
                copy.wait_recv()

    def await_sent(gone_s, gone_n):
        @pl.when(has_s)
        def _():
            for copy in gone_s:
                copy.wait_send()

        @pl.when(has_n)
        def _():
            for copy in gone_n:
                copy.wait_send()

    @pl.when(has_s)
    def _():
        for copy in to_s:
            copy.start()

    @pl.when(has_n)
    def _():
        for copy in to_n:
            copy.start()

    for missing, row, slot in ((no_s, 0, 0), (no_n, top, groups + 1)):
        @pl.when(missing)
        def _():
            ext[row : row + RIM, 0 : 2 * CH, 0:256] = jnp.zeros((RIM, 2 * CH, 256), F32)
            wind[:, row : row + RIM, 0:256] = jnp.zeros((2, RIM, 256), F32)
            lon[:, slot] = jnp.zeros((2, 40, 128), F32)

    two = 2.0 / HALF
    kind = lax.broadcasted_iota(jnp.int32, (8, 128), 0)
    by_kx = jnp.where(kind < 2, -two, 0.0)
    by_one = jnp.where((kind == 3) | (kind == 4), -0.5 * two, 0.0)
    eight = two * 8.0 / 12.0
    by_lon = jnp.where(kind == 0, eight, 0.0) + jnp.where(kind == 1, -eight, 0.0)
    by_lon = by_lon + jnp.where(kind == 2, -two / 12.0, 0.0)
    by_lat = jnp.where(kind == 3, eight, 0.0) + jnp.where(kind == 4, -eight, 0.0)
    by_lat = by_lat + jnp.where(kind == 5, -two / 12.0, 0.0)

    def merge(from_e, from_w):
        at = lanes(from_e.shape)
        return jnp.where(at < 16, from_e, jnp.where(at >= 112, from_w, 0.0))

    def third(g):
        at = pl.ds(pl.multiple_of(8 * g, 8), 8)
        for j in range(8):
            ext[8 * g + j, 0 : 2 * CH, 256:384] = merge(
                turn(lon[0, g, 0 : 2 * CH, :], -16 * j), turn(lon[1, g, 0 : 2 * CH, :], 112 - 16 * j))
        for n in range(2):
            wind[n, at, 256:384] = merge(
                turn(lon[0, g, 2 * CH :, :], -16 * n), turn(lon[1, g, 2 * CH :, :], 112 - 16 * n))

    def prepare(g, some=range(8), tiles=range(3)):
        at = pl.ds(pl.multiple_of(8 * g, 8), 8)
        kx8 = kxv[at, :]
        in8 = jnp.where(kx8 > 0.0, 1.0, 0.0)
        for t in tiles:
            cut = pl.ds(128 * t, 128)
            lon8, lat8 = wind[0, at, cut], wind[1, at, cut]
            for j in some:
                one = slice(j, j + 1)
                coef[8 * g + j, :, cut] = (
                    kx8[one] * by_kx + in8[one] * by_one + by_lon * lon8[one] + by_lat * lat8[one])
                diag = ext[8 * g + j, CH : 2 * CH, cut]
                gain, base = two * in8[one], (two * (2.0 - MID)) * in8[one] + (2.0 * two) * kx8[one]
                main[8 * g + j, :, cut] = diag * gain + base

    @pl.loop(1, groups + 1)
    def _(g):
        prepare(g, tiles=range(2))

    go_west.wait_recv()
    go_east.wait_recv()
    cor_s = pltpu.make_async_remote_copy(
        lon.at[:, 1], lon.at[:, groups + 1], cor_send.at[0], cor_recv.at[0],
        device_id=(gx, south), device_id_type=MESH)
    cor_n = pltpu.make_async_remote_copy(
        lon.at[:, groups], lon.at[:, 0], cor_send.at[1], cor_recv.at[1],
        device_id=(gx, north), device_id_type=MESH)

    @pl.when(has_s)
    def _():
        cor_s.start()

    @pl.when(has_n)
    def _():
        cor_n.start()

    for g in range(1, groups + 1):
        third(g)
        prepare(g, tiles=(2,))

    cm = coup[...] * (0.25 * two)
    cm = jnp.concatenate([jnp.concatenate([cm] * 4, axis=1)] * 4, axis=0)
    r4 = lax.broadcasted_iota(jnp.int32, (64, 64), 0) // 16
    c4 = lax.broadcasted_iota(jnp.int32, (64, 64), 1) // 16
    cm = jnp.where(r4 == c4, cm, 0.0)
    cm_hi = cm.astype(jnp.bfloat16)
    cm_lo = (cm - cm_hi.astype(F32)).astype(jnp.bfloat16)
    weights = jnp.concatenate([cm_hi, cm_hi, cm_lo], axis=1)

    def power(k):
        return ext.at[:, pl.ds(0, CH), :] if k == 0 else pwr[k - 1]

    lane4 = lanes((4, CH, 128))

    def couple(src, r0, tiles):
        mids = [src[pl.ds(r0, 4), :, 128 * t : 128 * t + 128] for t in range(tiles)]
        flat = jnp.concatenate([m.reshape(64, 128) for m in mids], axis=1)
        hi = flat.astype(jnp.bfloat16)
        lo = (flat - hi.astype(F32)).astype(jnp.bfloat16)
        return jnp.dot(weights, jnp.concatenate([hi, lo, hi], axis=0), preferred_element_type=F32)

    def stencil(k, r0):
        src, dst = power(k), power(k + 1)
        tiles = 3 if k + 1 < ITERS else 2
        mixed = couple(src, r0, tiles)
        prev = power(k - 1) if k % BLOCK else None
        mids = [src[pl.ds(r0, 4), :, 128 * t : 128 * t + 128] for t in range(3)]
        for t in range(tiles):
            cut = pl.ds(128 * t, 128)
            mid, nxt, prv = mids[t], mids[(t + 1) % 3], mids[(t + 2) % 3]
            e1 = pltpu.roll(jnp.where(lane4 < 1, nxt, mid), 127, 2)
            e2 = pltpu.roll(jnp.where(lane4 < 2, nxt, mid), 126, 2)
            w1 = pltpu.roll(jnp.where(lane4 >= 127, prv, mid), 1, 2)
            w2 = pltpu.roll(jnp.where(lane4 >= 126, prv, mid), 2, 2)
            n1 = src[pl.ds(r0 + 1, 4), :, cut]
            n2 = src[pl.ds(r0 + 2, 4), :, cut]
            s1 = src[pl.ds(r0 - 1, 4), :, cut]
            s2 = src[pl.ds(r0 - 2, 4), :, cut]
            cs = [coef[pl.ds(r0, 4), i : i + 1, cut] for i in range(6)]
            out = main[pl.ds(r0, 4), :, cut] * mid
            out = out + mixed[:, 128 * t : 128 * t + 128].reshape(4, CH, 128)
            out = out + cs[0] * e1 + cs[1] * w1 + cs[2] * (e2 - w2)
            out = out + cs[3] * n1 + cs[4] * s1 + cs[5] * (n2 - s2)
            if prev is not None:
                out = out - prev[pl.ds(r0, 4), :, cut]
            dst[pl.ds(r0, 4), :, cut] = out

    def inner(k):
        m = k % BLOCK + 1
        for r0 in range(RIM + 2 * m, top - 2 * m, 4):
            stencil(k, r0)

    def outer(k, far):
        m = k % BLOCK + 1
        for r0 in ((2 * m, top - 2 * m + 4) if far else (2 * m + 4, top - 2 * m)):
            stencil(k, r0)

    for k in range(BLOCK):
        inner(k)

    await_strips(near_n + [cor_n], near_s + [cor_s])
    third(0)
    third(groups + 1)
    prepare(0, range(4, 8))
    prepare(groups + 1, range(4))
    for k in range(BLOCK):
        outer(k, False)
    await_strips(far_n, far_s)
    prepare(0, range(2, 4))
    prepare(groups + 1, range(4, 6))
    for k in range(BLOCK):
        outer(k, True)

    half = power(BLOCK)
    lane16 = lanes((CH, 128))
    for side, row in ((0, RIM), (1, rows)):
        out = jnp.zeros((CH, 128), F32)
        for j in range(8):
            here = (lane16 >= 16 * j) & (lane16 < 16 * j + 16)
            out = jnp.where(here, turn(half[row + j, :, 256:384], 16 * j + 8), out)
        made[side] = out

    def again(src, dst, sem, peer):
        return pltpu.make_async_remote_copy(
            half.at[pl.ds(src, 4), :, pl.ds(0, 256)], half.at[pl.ds(dst, 4), :, pl.ds(0, 256)],
            mid_send.at[sem], mid_recv.at[sem], device_id=(gx, peer), device_id_type=MESH)

    def also(src, dst, sem, peer):
        return pltpu.make_async_remote_copy(
            made.at[src], rims.at[dst], mid_send.at[sem], mid_recv.at[sem],
            device_id=(gx, peer), device_id_type=MESH)

    near_s = [also(0, 1, 0, south), again(RIM, top, 1, south)]
    far_s2 = [again(RIM + 4, top + 4, 2, south)]
    near_n = [also(1, 0, 3, north), again(rows + 4, 4, 4, north)]
    far_n2 = [again(rows, 0, 5, north)]
    mid_s, mid_n = near_s + far_s2, near_n + far_n2

    @pl.when(has_s)
    def _():
        for copy in mid_s:
            copy.start()

    @pl.when(has_n)
    def _():
        for copy in mid_n:
            copy.start()

    for missing, row, slot in ((no_s, 0, 0), (no_n, top, 1)):
        @pl.when(missing)
        def _():
            half[row : row + RIM, :, 0:256] = jnp.zeros((RIM, CH, 256), F32)
            rims[slot] = jnp.zeros((CH, 128), F32)

    for k in range(BLOCK, ITERS):
        inner(k)

    pairs = [(i, k) for i in range(9) for k in range(i, 9)]

    def gram(r, sums):
        for o in range(2):
            for t in range(2):
                at = (r, pl.ds(8 * o, 8), pl.ds(128 * t, 128))
                vals = [power(k)[at] for k in range(9)]
                sums = [s + vals[i] * vals[k] for s, (i, k) in zip(sums, pairs)]
        return tuple(sums)

    sums = tuple(jnp.zeros((8, 128), F32) for _ in pairs)
    sums = lax.fori_loop(2 * RIM, top - RIM, gram, sums)
    await_strips(near_n, near_s)
    for side, row in ((0, 0), (1, top)):
        for j in range(8):
            half[row + j, :, 256:384] = turn(rims[side], -16 * j - 8)
    for k in range(BLOCK, ITERS):
        outer(k, False)
    sums = lax.fori_loop(RIM + 4, 2 * RIM, gram, sums)
    sums = lax.fori_loop(top - RIM, top - 4, gram, sums)
    await_strips(far_n2, far_s2)
    for k in range(BLOCK, ITERS):
        outer(k, True)
    sums = lax.fori_loop(RIM, RIM + 4, gram, sums)
    sums = lax.fori_loop(top - 4, top, gram, sums)

    sums = dict(zip(pairs, sums))
    folded = {p: jnp.sum(s, axis=0, keepdims=True) for p, s in sums.items()}
    sub8 = lax.broadcasted_iota(jnp.int32, (8, 128), 0)
    spread = jnp.zeros((8, 128), F32)
    for k in range(10):
        col = jnp.zeros((8, 128), F32)
        if k < 9:
            for i in range(8):
                col = jnp.where(sub8 == i, folded[min(i, k), max(i, k)], col)
        else:
            col = jnp.where(sub8 == 0, folded[8, 8], col)
        total_k = jnp.sum(col, axis=1, keepdims=True)
        spread = jnp.where(lane8 == 8 * k + sub8, total_k, spread)
    mine = jnp.sum(spread, axis=0, keepdims=True)

    def reduce_over(value, slots, send, recv, me, count, device):
        slots[me] = value
        for k in reversed(reach(count)):
            pltpu.make_async_remote_copy(
                slots.at[me], slots.at[me], send, recv,
                device_id=device(lax.rem(me + k, count)), device_id_type=MESH).start()
        rest = slots.at[pl.ds(0, count - 1)]
        every = pltpu.make_async_remote_copy(
            rest, rest, send, recv,
            device_id=device(lax.rem(me + 1, count)), device_id_type=MESH)
        every.wait_recv()
        parts = [slots[k] for k in range(count)]
        while len(parts) > 1:
            parts = [sum(parts[i : i + 2][1:], parts[i]) for i in range(0, len(parts), 2)]
        return parts[0], every

    value, one_way = reduce_over(mine, gx_slots, gxs_send, gxs_recv, gx, nx, lambda p: (p, gy))
    value, other_way = reduce_over(value, gy_slots, gys_send, gys_recv, gy, ny, lambda p: (gx, p))
    value = jnp.broadcast_to(value, (8, 128))
    picked = [jnp.where(lane8 == 8 * k + sub8, value, 0.0) for k in range(10)]
    upper = [jnp.broadcast_to(jnp.sum(p, axis=1, keepdims=True), (8, 128)) for p in picked]
    lower = [upper[8][k : k + 1, :] for k in range(8)] + [upper[9][0:1, :]]
    plain = [jnp.concatenate([u, jnp.where(sub8 == 0, w, 0.0)]) for u, w in zip(upper, lower)]
    sub = lax.broadcasted_iota(jnp.int32, (16, 128), 0)
    diag = jnp.zeros((16, 128), F32)
    for k in range(9):
        diag = jnp.where(sub == k, plain[k], diag)
    size = jnp.sqrt(diag)
    trial = trials()
    cols = [plain[k] + trial[k] * size * size[k : k + 1, :] for k in range(9)]
    q = gmres(cols)
    d = apply_a(q)
    q0 = jnp.broadcast_to(q[:, 0:1], (16, 128))
    d0 = jnp.broadcast_to(d[:, 0:1], (16, 128))
    left0 = jnp.where(sub == 0, 1.0, 0.0) - d0
    dq, dd = q - q0, d - d0
    bad_q = dot(dq, mat_vec(plain, dq, 8)) - TRUST**2 * dot(q0, mat_vec(plain, q0, 8))
    bad_d = dot(dd, mat_vec(plain, dd, 9)) - TRUST**2 * dot(left0, mat_vec(plain, left0, 9))
    fine = (bad_q <= 0.0) & (bad_d <= 0.0)
    flag[0, 0] = jnp.max(jnp.where(fine, 0.0, 1.0))

    qs = [q0[k : k + 1, :] for k in range(8)]
    ds = [left0[k : k + 1, :] for k in range(9)]

    @pl.loop(0, rows, unroll=4)
    def _(r):
        for t in range(2):
            cut = pl.ds(128 * t, 128)
            vals = [power(k)[r + RIM, :, cut] for k in range(9)]
            s = qs[0] * vals[0]
            e = ds[0] * vals[0]
            for k in range(1, 8):
                s = s + qs[k] * vals[k]
            for k in range(1, 9):
                e = e + ds[k] * vals[k]
            outs[0, r, :, cut] = s
            outs[1, r, :, cut] = e

    go_west.wait_send()
    go_east.wait_send()
    await_sent(to_s + [cor_s] + mid_s, to_n + [cor_n] + mid_n)
    one_way.wait_send()
    other_way.wait_send()


def unfold(outs, sol, res, sem):
    copies = []
    for c in range(CH):
        for n, dst in enumerate((sol, res)):
            copies.append(pltpu.make_async_copy(outs.at[n, :, c, :], dst.at[c], sem.at[n, c]))
    for copy in copies:
        copy.start()
    for copy in copies:
        copy.wait()


def fused(nx, ny, forcing, damping, wind_lon, wind_lat, coup):
    rows = forcing.shape[1]
    total = rows + 2 * RIM
    vm = pl.BlockSpec(memory_space=pltpu.VMEM)
    hbm = pl.BlockSpec(memory_space=pltpu.HBM)
    dma = pltpu.SemaphoreType.DMA
    outs, flag = pl.pallas_call(
        functools.partial(kernel, nx, ny),
        out_shape=(jax.ShapeDtypeStruct((2, rows, CH, 256), F32), jax.ShapeDtypeStruct((1, 1), F32)),
        in_specs=[hbm] * 5,
        out_specs=(vm, pl.BlockSpec(memory_space=pltpu.SMEM)),
        scratch_shapes=[pltpu.VMEM((total, CH, 384), F32)] * ITERS + [
            pltpu.VMEM((total, 2 * CH, 384), F32),
            pltpu.VMEM((total, 8, 384), F32),
            pltpu.VMEM((total, CH, 384), F32),
            pltpu.VMEM((2, total, 384), F32),
            pltpu.VMEM((2, total // 8, 40, 128), F32),
            pltpu.VMEM((2, rows // 8, 40, 128), F32),
            pltpu.VMEM((total, 128), F32),
            pltpu.VMEM((CH, CH), F32),
            pltpu.VMEM((2, CH, 128), F32),
            pltpu.VMEM((2, CH, 128), F32),
            pltpu.VMEM((nx, 1, 128), F32),
            pltpu.VMEM((ny, 1, 128), F32),
            dma((2 * CH + 3,)), dma((2,)), dma((2,)), dma((10,)), dma((10,)),
            dma((2,)), dma((2,)), dma((6,)), dma((6,)), dma, dma, dma, dma,
        ],
        compiler_params=pltpu.CompilerParams(
            collective_id=0, has_side_effects=True, vmem_limit_bytes=48 * 1024 * 1024),
        name="krylov",
    )(forcing, damping, wind_lon, wind_lat, coup)
    field = jax.ShapeDtypeStruct(forcing.shape, F32)
    sol, res = pl.pallas_call(
        unfold,
        out_shape=(field, field),
        in_specs=[vm],
        out_specs=(hbm, hbm),
        scratch_shapes=[dma((2, CH))],
        compiler_params=pltpu.CompilerParams(vmem_limit_bytes=8 * 1024 * 1024),
        name="unfold",
    )(outs)
    return sol, res, flag


def shifted(cells, axis, dim, closed, width):
    count = lax.axis_size(axis)
    ends = count if closed else count - 1
    head = lax.slice_in_dim(cells, 0, width, axis=dim)
    tail = lax.slice_in_dim(cells, cells.shape[dim] - width, cells.shape[dim], axis=dim)
    return jnp.concatenate(
        [
            lax.ppermute(tail, axis, [(i, (i + 1) % count) for i in range(ends)]),
            cells,
            lax.ppermute(head, axis, [((i + 1) % count, i) for i in range(ends)]),
        ],
        axis=dim,
    )


def apply_plain(vec, damping, coupling, wind_lon, wind_lat, kx):
    wide = shifted(vec, "gx", 2, True, 2)
    tall = shifted(vec, "gy", 1, False, 2)
    e1, w1, e2, w2 = wide[:, :, 3:-1], wide[:, :, 1:-3], wide[:, :, 4:], wide[:, :, :-4]
    n1, s1, n2, s2 = tall[:, 3:-1], tall[:, 1:-3], tall[:, 4:], tall[:, :-4]
    mixed = jnp.einsum("ij,jab->iab", coupling, vec, precision=lax.Precision.HIGHEST)
    return (
        (1.0 + damping) * vec + 0.25 * mixed
        + kx * (2.0 * vec - e1 - w1) + 0.5 * (2.0 * vec - n1 - s1)
        + wind_lon * ((8.0 * (e1 - w1) - (e2 - w2)) / 12.0)
        + wind_lat * ((8.0 * (n1 - s1) - (n2 - s2)) / 12.0)
    )


def careful(forcing, damping, coupling, wind_lon, wind_lat):
    rows = forcing.shape[1]
    pos = (lax.axis_index("gy") * rows + jnp.arange(rows)).astype(F32)
    phi = -math.pi / 2 + (pos + 0.5) * (math.pi / (rows * lax.axis_size("gy")))
    kx = (0.5 / (jnp.cos(phi) ** 2 + 0.1))[:, None]
    operate = lambda v: apply_plain(v, damping, coupling, wind_lon, wind_lat, kx)
    every = ("gx", "gy")
    first = jnp.sqrt(lax.psum(jnp.sum(forcing * forcing), every) + 1.0)
    basis = jnp.zeros((ITERS,) + forcing.shape, F32).at[0].set(forcing / first)
    heights = jnp.zeros((ITERS + 1, ITERS), F32)

    def body(j, state):
        basis, heights = state
        w = operate(lax.dynamic_index_in_dim(basis, j, 0, keepdims=False))
        h = lax.psum(jnp.sum(basis * w[None], axis=(1, 2, 3)), every)
        w = w - jnp.sum(h[:, None, None, None] * basis, axis=0)
        below = jnp.sqrt(lax.psum(jnp.sum(w * w), every) + 1.0)
        col = jnp.concatenate([h, jnp.zeros((1,), F32)])
        col = jnp.where(jnp.arange(ITERS + 1) == j + 1, below, col)
        heights = lax.dynamic_update_slice(heights, col[:, None], (0, j))
        old = lax.dynamic_index_in_dim(basis, jnp.minimum(j + 1, ITERS - 1), 0, keepdims=False)
        new = jnp.where(j + 1 < ITERS, w / below, old)
        basis = lax.dynamic_update_index_in_dim(basis, new, jnp.minimum(j + 1, ITERS - 1), 0)
        return basis, heights

    basis, heights = lax.fori_loop(0, ITERS, body, (basis, heights))
    h = [[heights[i, j] for j in range(ITERS)] for i in range(ITERS + 1)]
    target = [first] + [jnp.zeros((), F32)] * ITERS
    turns = []
    for j in range(ITERS):
        for i in range(j):
            c, s = turns[i]
            h[i][j], h[i + 1][j] = c * h[i][j] + s * h[i + 1][j], c * h[i + 1][j] - s * h[i][j]
        radius = jnp.sqrt(h[j][j] * h[j][j] + h[j + 1][j] * h[j + 1][j])
        c, s = h[j][j] / radius, h[j + 1][j] / radius
        turns.append((c, s))
        h[j][j] = radius
        target[j], target[j + 1] = c * target[j] + s * target[j + 1], c * target[j + 1] - s * target[j]
    y = [None] * ITERS
    for j in reversed(range(ITERS)):
        part = target[j]
        for i in range(j + 1, ITERS):
            part = part - h[j][i] * y[i]
        y[j] = part / h[j][j]
    weights = jnp.stack(y)
    answer = jnp.sum(weights[:, None, None, None] * basis, axis=0)
    return answer, forcing - operate(answer)


def per_device(nx, ny, forcing, damping, coupling, wind_lon, wind_lat):
    sol, res, flag = fused(nx, ny, forcing, damping, wind_lon, wind_lat, coupling)

    pin = lambda x: with_layout_constraint(x, Layout(tuple(range(x.ndim))))

    def again(state):
        sol, res = careful(pin(forcing), pin(damping), coupling, wind_lon, wind_lat)
        return pin(sol), pin(res), jnp.zeros((), F32)

    done = lax.while_loop(lambda state: state[2] > 0.5, again, (sol, res, flag[0, 0]))
    return pin(done[0]), pin(done[1])


def solution(mesh):
    nx, ny = mesh.shape["gx"], mesh.shape["gy"]
    in_specs = (P(None, "gy", "gx"), P(None, "gy", "gx"), P(), P("gy", "gx"), P("gy", "gx"))
    out_specs = (P(None, "gy", "gx"), P(None, "gy", "gx"))
    return jax.shard_map(
        functools.partial(per_device, nx, ny),
        mesh=mesh, in_specs=in_specs, out_specs=out_specs, check_vma=False,
    )
```
